32 devices in a mesh: dp: 8 (over y, x, core), tensor: 4 (over z).
Axes of the slice: x: 2, y: 2, z: 4, core: 2. Of those that a mesh axis runs over, the one named last changes fastest.
Arguments:
- inputs: bfloat16 [12288, 768], P(('dp', 'tensor')), may hold values from -6 to 6
- segments: int32 [24, 512], P('dp'), may hold values from 0 to 3, never falling along the last dimension, each value on 1 to 256 neighbouring positions
- labels: int32 [24], P('dp'), may hold values from 0 to 2
- qkv_weight: bfloat16 [3, 768, 768], P(None, None, 'tensor'), may hold values from -0.21875 to 0.21875
- qv_bias: float32 [2, 768], P(None, 'tensor'), may hold values from -3 to 3
- out_weight: bfloat16 [768, 768], P('tensor'), may hold values from -0.875 to 0.875
- out_bias: float32 [768], replicated, may hold values from -3 to 3
- norm1_gain: float32 [768], replicated, may hold values from 0.5 to 1.5
- norm1_bias: float32 [768], replicated, may hold values from -3 to 3
- up_weight: bfloat16 [768, 3072], P(None, 'tensor'), may hold values from -0.21875 to 0.21875
- up_bias: float32 [3072], P('tensor'), may hold values from -3 to 3
- down_weight: bfloat16 [3072, 768], P('tensor'), may hold values from -0.109375 to 0.109375
- down_bias: float32 [768], replicated, may hold values from -3 to 3
- norm2_gain: float32 [768], replicated, may hold values from 0.5 to 1.5
- norm2_bias: float32 [768], replicated, may hold values from -3 to 3
- pool_weight: bfloat16 [768, 768], replicated, may hold values from -0.21875 to 0.21875
- pool_bias: float32 [768], replicated, may hold values from -3 to 3
- class_weight: bfloat16 [768, 3], replicated, may hold values from -0.4375 to 0.4375
- class_bias: float32 [3], replicated, may hold values from -4 to 4
- cotangent: bfloat16 [12288, 768], P(('dp', 'tensor')), may hold values from -6 to 6
Outputs:
- hidden: bfloat16 [12288, 768], P(('dp', 'tensor'))
- input_grad: bfloat16 [12288, 768], P(('dp', 'tensor'))
- qkv_weight_grad: float32 [3, 768, 768], P(None, 'dp', 'tensor')
- qv_bias_grad: float32 [2, 768], P(None, 'tensor')
- out_weight_grad: float32 [768, 768], P('tensor', 'dp')
- out_bias_grad: float32 [768], replicated
- norm1_gain_grad: float32 [768], replicated
- norm1_bias_grad: float32 [768], replicated
- up_weight_grad: float32 [768, 3072], P('dp', 'tensor')
- up_bias_grad: float32 [3072], P('tensor')
- down_weight_grad: float32 [3072, 768], P('tensor', 'dp')
- down_bias_grad: float32 [768], replicated
- norm2_gain_grad: float32 [768], replicated
- norm2_bias_grad: float32 [768], replicated
- pool_weight_grad: float32 [768, 768], replicated
- pool_bias_grad: float32 [768], replicated
- class_weight_grad: float32 [768, 3], replicated
- class_bias_grad: float32 [3], replicated
The draws below stay inside these ranges and needn't reach their ends.
Inputs may be any that keep to these rules, and one draw needn't show every extreme that they name: `segments`: along each packed row of 512 tokens the ids never fall; a document holds at most half of 512 tokens.
All inputs are finite; a program needn't handle non-finite values.
Results may differ from the reference program's by a relative error of at most 0.017.
The reference program's roundings to bfloat16 on the way count: a program that leaves them out, or rounds other values in their place, can miss the bound.
Values may be sent and summed in bfloat16 or wider, within the bound.
A program may use at most 128 MiB of HBM per device.

```python
import math
import jax
import jax.numpy as jnp
import numpy as np
from jax import lax

D = 768
HEADS = 12
HEAD = 64
FF = 3072
CLASSES = 3
SEQ = 512
SEGS = 4
SEQ_DEV = 3
TOK_DEV = 1536
ROWS = 24
TOKENS = 12288
N_DP = 8


def place_ends(drawn, own_key, least, high):
    spot = [jax.random.randint(jax.random.fold_in(own_key, axis), (), 0, length) for axis, length in enumerate(drawn.shape)]
    widest = drawn.shape.index(max(drawn.shape))
    neighbour = spot[:widest] + [(spot[widest] + 1) % drawn.shape[widest]] + spot[widest + 1:]
    return drawn.at[tuple(spot)].set(least).at[tuple(neighbour)].set(high)


def raised(values, key, source, target, shards_of, factor):
    owner, partner = [(jnp.arange(values.shape[position]) // (values.shape[position] // shards_of)).reshape([-1 if axis == position else 1 for axis in range(values.ndim)]) for position in (source, target)]
    chosen = jax.random.permutation(key, shards_of)[partner]
    strong = (owner == chosen) | (owner == (partner + shards_of // 2) % shards_of)
    return jnp.where(strong, factor * values, values)


def block_levels(stream_key, extent, cuts, least, top_value):
    def one(dim, blocks):
        heights = jax.random.uniform(jax.random.fold_in(jax.random.fold_in(stream_key, 6), dim), (blocks,), jnp.float32, least / len(cuts), top_value / len(cuts))
        return jnp.repeat(jnp.exp(heights), extent[dim] // blocks).reshape((-1,) + (1,) * (len(extent) - dim - 1))

    factor_of = one(*cuts[0])
    for cut in cuts[1:]:
        factor_of = factor_of * one(*cut)
    return factor_of


def profile(count, total, reach, skew):
    weights = [(1 << 20) // math.isqrt(grade ** skew) + 1 for grade in range(2, count + 1)]
    surplus, holding = total - reach - (count - 1), [1] * (count - 1)
    while surplus > 0:
        movable = [i for i in range(count - 1) if holding[i] < reach]
        whole, budget = sum([weights[i] for i in movable]), surplus
        for i in movable:
            addition = min(reach - holding[i], max(1, budget * weights[i] // whole), surplus)
            holding[i] = holding[i] + addition
            surplus = surplus - addition
    return np.array([reach] + holding)


def uneven(own_key, count, total, bound, slope):
    if count == 2:
        one = jax.random.randint(own_key, (), max(1, total - bound), min(bound, total - 1) + 1)
        return jnp.stack([one, total - one])
    lengths = jnp.asarray(profile(count, total, bound, slope), jnp.int32)
    couples = (count - 1) // 2
    giver, sink = lengths[1:1 + 2 * couples:2], lengths[2:2 + 2 * couples:2]
    room = jnp.minimum(giver - 1, bound - sink)
    passed = jax.random.randint(jax.random.fold_in(own_key, 1), (couples,), 0, 1 << 20) % (room + 1)
    lengths = lengths.at[1:1 + 2 * couples:2].set(giver - passed).at[2:2 + 2 * couples:2].set(sink + passed)
    return lengths[jax.random.permutation(jax.random.fold_in(own_key, 2), count)]


def noise(stream_key, shape, scale, limit, cuts=(), kind=jnp.bfloat16):
    array = jax.random.normal(stream_key, shape, jnp.float32) * scale
    if len(cuts) > 0:
        array = block_levels(stream_key, shape, cuts, -0.22, 0.18) * array
    return jnp.clip(array, min=-limit, max=limit).astype(kind)


def noise_with(stream_key, shape, deviation, limit, split, heavy, kind=jnp.bfloat16):
    result = deviation * jax.random.normal(stream_key, shape, jnp.float32)
    if split:
        result = result * block_levels(stream_key, shape, split, -0.22, 0.18)
    return jnp.clip(raised(result, jax.random.fold_in(stream_key, 3), *heavy), -limit, limit).astype(kind)


def setup_inputs(seed: int = 0) -> dict:
    splits = jax.random.split(jax.random.key(seed), 21)
    return {
        "inputs": noise_with(splits[0], (TOKENS, D), 1.0, 6.0, ((0, 32),), (0, 1, 32, 2.75)),
        "segments": jax.vmap(lambda own: jnp.searchsorted(jnp.cumsum(uneven(own, SEGS, SEQ, SEQ // 2, 0)), jnp.arange(SEQ), side="right"))(jax.random.split(splits[1], ROWS)).reshape((ROWS, SEQ)).astype(jnp.int32),
        "labels": place_ends(jax.random.randint(splits[2], (ROWS,), 0, CLASSES), jax.random.fold_in(splits[2], 1), 0, CLASSES - 1).astype(jnp.int32),
        "qkv_weight": noise(splits[3], (3, D, D), D ** -0.5, 0.21875, ((2, 4),)),
        "qv_bias": noise(splits[4], (2, D), 0.5, 3.0, ((1, 4),), jnp.float32),
        "out_weight": noise(splits[5], (D, D), (D // 16) ** -0.5, 0.875, ((0, 4),)),
        "out_bias": noise(splits[6], (D,), 0.5, 3.0, (), jnp.float32),
        "norm1_gain": jnp.clip(jax.random.uniform(splits[7], (D,), jnp.float32, 0.5, 1.5), 0.5, 1.5),
        "norm1_bias": noise(splits[8], (D,), 0.5, 3.0, (), jnp.float32),
        "up_weight": noise(splits[9], (D, FF), D ** -0.5, 0.21875, ((1, 4),)),
        "up_bias": noise(splits[10], (FF,), 0.5, 3.0, ((0, 4),), jnp.float32),
        "down_weight": noise(splits[11], (FF, D), FF ** -0.5, 0.109375, ((0, 4),)),
        "down_bias": noise(splits[12], (D,), 0.5, 3.0, (), jnp.float32),
        "norm2_gain": jnp.clip(jax.random.uniform(splits[13], (D,), jnp.float32, 0.5, 1.5), 0.5, 1.5),
        "norm2_bias": noise(splits[14], (D,), 0.5, 3.0, (), jnp.float32),
        "pool_weight": noise(splits[15], (D, D), D ** -0.5, 0.21875),
        "pool_bias": noise(splits[16], (D,), 0.5, 3.0, (), jnp.float32),
        "class_weight": noise(splits[17], (D, CLASSES), (D // 4) ** -0.5, 0.4375),
        "class_bias": noise(splits[18], (CLASSES,), 1.0, 4.0, (), jnp.float32),
        "cotangent": noise_with(splits[19], (TOKENS, D), 1.0, 6.0, ((0, 32),), (0, 1, 32, 2.75)),
    }


@jax.custom_vjp
def low(v):
    return lax.optimization_barrier(v.astype(jnp.bfloat16)).astype(jnp.float32)

@jax.custom_vjp
def low_back(v):
    return v

def low_keep(v):
    return (low(v), None)

def low_pass(kept, grad):
    return (grad,)

def back_keep(v):
    return (v, None)

def back_low(kept, grad):
    return (low(grad),)
low.defvjp(low_keep, low_pass)
low_back.defvjp(back_keep, back_low)
highest = lax.Precision.HIGHEST
epsilon = 1e-12
masked_value = -1e+30

def product(left, right):
    return jnp.dot(left, right, precision=highest)

def layer_norm(values, norm_gain, norm_shift):
    centre = values - lax.optimization_barrier(jnp.mean(values, axis=-1, keepdims=True))
    variance = lax.optimization_barrier(jnp.mean(centre * centre, axis=-1, keepdims=True))
    return centre * lax.rsqrt(variance + epsilon) * norm_gain + norm_shift

def forward(parameters, inputs, segment_rows, label_rows):
    qkv_weight, qv_bias, out_weight, out_bias, norm1_gain, norm1_bias, up_weight, up_bias, down_weight, down_bias, norm2_gain, norm2_bias, pool_weight, pool_bias, class_weight, class_bias = parameters
    row_count = segment_rows.shape[0]
    score_scale = HEAD ** (-0.5)
    projected = jnp.einsum('td,kde->kte', inputs, qkv_weight, precision=highest)
    queries = low(low_back(projected[0] + qv_bias[0]))
    key_rows = low(low_back(projected[1]))
    value_rows = low(low_back(projected[2] + qv_bias[1]))
    head_shape = (row_count, SEQ, HEADS, HEAD)
    scores = jnp.einsum('rqhe,rkhe->rhqk', queries.reshape(head_shape), key_rows.reshape(head_shape), precision=highest)
    scores = low_back(scores * score_scale)
    allowed = segment_rows[:, None, :, None] == segment_rows[:, None, None, :]
    soft_probs = jax.nn.softmax(jnp.where(allowed, scores, masked_value), axis=-1)
    context = jnp.einsum('rhqk,rkhe->rqhe', low(soft_probs), value_rows.reshape(head_shape), precision=highest)
    context = low(low_back(context.reshape(row_count * SEQ, D)))
    attended = low_back(product(context, out_weight) + out_bias)
    first_norm = layer_norm(inputs + attended, norm1_gain, norm1_bias)
    up_pre = low_back(product(low(first_norm), up_weight) + up_bias)
    active = low(jax.nn.gelu(up_pre, approximate=False))
    ffn_out = low_back(product(active, down_weight) + down_bias)
    final_norm = layer_norm(first_norm + ffn_out, norm2_gain, norm2_bias)
    leading = low(final_norm.reshape(row_count, SEQ, D)[:, 0])
    pooled = low(jnp.tanh(low_back(product(leading, pool_weight) + pool_bias)))
    logits = low_back(product(pooled, class_weight) + class_bias)
    chosen = (label_rows[:, None] == jnp.arange(CLASSES, dtype=jnp.int32)[None, :]).astype(jnp.float32)
    total_loss = jnp.sum(jax.nn.logsumexp(logits, axis=-1) - lax.optimization_barrier(jnp.sum(logits * chosen, axis=-1)))
    return (final_norm, total_loss)

def reference(inputs, segments, labels, qkv_weight, qv_bias, out_weight, out_bias, norm1_gain, norm1_bias, up_weight, up_bias, down_weight, down_bias, norm2_gain, norm2_bias, pool_weight, pool_bias, class_weight, class_bias, cotangent):
    parameters = tuple((member.astype(jnp.float32) for member in (qkv_weight, qv_bias, out_weight, out_bias, norm1_gain, norm1_bias, up_weight, up_bias, down_weight, down_bias, norm2_gain, norm2_bias, pool_weight, pool_bias, class_weight, class_bias)))
    token_blocks = inputs.astype(jnp.float32).reshape(N_DP, TOK_DEV, D)
    cot_blocks = cotangent.astype(jnp.float32).reshape(N_DP, TOK_DEV, D)
    seg_blocks = segments.reshape(N_DP, SEQ_DEV, SEQ)
    label_blocks = labels.reshape(N_DP, SEQ_DEV)
    zero_grads = tuple((jnp.zeros(member.shape, jnp.float32) for member in parameters))

    def scan_step(totals, block_rows):
        token_rows, cot_rows, seg_rows, label_rows = block_rows

        def closed(params_in, tokens_in):
            return forward(params_in, tokens_in, seg_rows, label_rows)
        outputs, pullback = jax.vjp(closed, parameters, token_rows)
        param_grads, token_grads = pullback((cot_rows, jnp.ones((), jnp.float32)))
        totals = tuple((left + right for left, right in zip(totals, param_grads)))
        return (totals, (outputs[0].astype(jnp.bfloat16), token_grads.astype(jnp.bfloat16)))
    totals, (hidden, input_grad) = lax.scan(scan_step, zero_grads, (token_blocks, cot_blocks, seg_blocks, label_blocks))
    return (hidden.reshape(TOKENS, D), input_grad.reshape(TOKENS, D), totals[0], totals[1], totals[2], totals[3], totals[4], totals[5], totals[6], totals[7], totals[8], totals[9], totals[10], totals[11], totals[12], totals[13], totals[14], totals[15])
```

```python
from functools import partial

import jax
import jax.numpy as jnp
from jax import lax
from jax.sharding import PartitionSpec as P

HEAD = 64


epsilon = 1e-12
masked_value = -1e30


def norm_forward(values, norm_gain, norm_shift):
    centre = values - jnp.mean(values, axis=-1, keepdims=True)
    inverse = lax.rsqrt(jnp.mean(centre * centre, axis=-1, keepdims=True) + epsilon)
    normed = centre * inverse
    return (normed * norm_gain + norm_shift, normed, inverse)


def norm_backward(grad_out, normed, inverse, norm_gain):
    scaled = grad_out * norm_gain
    grad_in = inverse * (
        scaled
        - jnp.mean(scaled, axis=-1, keepdims=True)
        - normed * jnp.mean(scaled * normed, axis=-1, keepdims=True)
    )
    return (grad_in, jnp.sum(grad_out * normed, axis=0), jnp.sum(grad_out, axis=0))


def split_heads(rows, seq_count):
    return rows.reshape(seq_count, rows.shape[0] // seq_count, rows.shape[1] // HEAD, HEAD)


def masked_scores(query_heads, key_heads, segments):
    raw_scores = jnp.einsum(
        "rqhe,rkhe->rhqk", query_heads, key_heads, preferred_element_type=jnp.float32
    ) * HEAD ** (-0.5)
    allowed = segments[:, None, :, None] == segments[:, None, None, :]
    return (jnp.where(allowed, raw_scores, masked_value), allowed)


def attend_forward(queries, key_rows, value_rows, segments):
    seq_count = segments.shape[0]
    scores, allowed = masked_scores(
        split_heads(queries, seq_count), split_heads(key_rows, seq_count), segments
    )
    largest = jnp.max(scores, axis=-1, keepdims=True)
    exponent = jnp.exp(scores - largest)
    row_total = jnp.sum(exponent, axis=-1, keepdims=True)
    soft_low = (exponent / row_total).astype(jnp.bfloat16)
    context = jnp.einsum(
        "rhqk,rkhe->rqhe",
        soft_low,
        split_heads(value_rows, seq_count),
        preferred_element_type=jnp.float32,
    )
    context = context.reshape(queries.shape).astype(jnp.bfloat16)
    return (context, largest + jnp.log(row_total))


def attend_backward(queries, key_rows, value_rows, segments, log_total, grad_context):
    seq_count = segments.shape[0]
    query_heads = split_heads(queries, seq_count)
    key_heads = split_heads(key_rows, seq_count)
    value_heads = split_heads(value_rows, seq_count)
    grad_heads = split_heads(grad_context, seq_count)
    scores, allowed = masked_scores(query_heads, key_heads, segments)
    soft_probs = jnp.exp(scores - log_total)
    grad_values = jnp.einsum(
        "rhqk,rqhe->rkhe",
        soft_probs.astype(jnp.bfloat16),
        grad_heads,
        preferred_element_type=jnp.float32,
    )
    grad_soft = jnp.einsum(
        "rqhe,rkhe->rhqk", grad_heads, value_heads, preferred_element_type=jnp.float32
    )
    grad_scores = soft_probs * (grad_soft - jnp.sum(soft_probs * grad_soft, axis=-1, keepdims=True))
    grad_low = jnp.where(allowed, grad_scores, 0.0).astype(jnp.bfloat16)
    score_scale = HEAD ** (-0.5)
    grad_queries = (
        jnp.einsum("rhqk,rkhe->rqhe", grad_low, key_heads, preferred_element_type=jnp.float32)
        * score_scale
    )
    grad_keys = (
        jnp.einsum("rhqk,rqhe->rkhe", grad_low, query_heads, preferred_element_type=jnp.float32)
        * score_scale
    )
    full_shape = queries.shape
    return (
        grad_queries.reshape(full_shape).astype(jnp.bfloat16),
        grad_keys.reshape(full_shape).astype(jnp.bfloat16),
        grad_values.reshape(full_shape).astype(jnp.bfloat16),
    )


def to_blocks(array, axis, count):
    shape = array.shape
    split = shape[:axis] + (count, shape[axis] // count) + shape[axis + 1 :]
    return jnp.moveaxis(array.reshape(split), axis, 0).reshape(count, -1)


def from_block(flat, shape, axis, count):
    local = shape[:axis] + (shape[axis] // count,) + shape[axis + 1 :]
    return flat.reshape(local)


def body(
    inputs,
    segments,
    labels,
    qkv_weight,
    qv_bias,
    out_weight,
    out_bias,
    norm1_gain,
    norm1_bias,
    up_weight,
    up_bias,
    down_weight,
    down_bias,
    norm2_gain,
    norm2_bias,
    pool_weight,
    pool_bias,
    class_weight,
    class_bias,
    cotangent,
):
    share_rows = inputs.shape[0]
    seq_count, seq_length = segments.shape
    tensor_index = lax.axis_index("tensor")
    dp_index = lax.axis_index("dp")
    tensor_count = lax.axis_size("tensor")
    dp_count = lax.axis_size("dp")
    offset = tensor_index * share_rows

    gathered = lax.all_gather(inputs, "tensor", axis=0, tiled=True)
    group_rows = gathered.shape[0]
    projected = jnp.einsum("td,kde->kte", gathered, qkv_weight, preferred_element_type=jnp.float32)
    queries = (projected[0] + qv_bias[0]).astype(jnp.bfloat16)
    key_rows = projected[1].astype(jnp.bfloat16)
    value_rows = (projected[2] + qv_bias[1]).astype(jnp.bfloat16)
    local_width = queries.shape[1]

    context, log_totals = attend_forward(queries, key_rows, value_rows, segments)
    attended = (
        lax.psum_scatter(
            jnp.dot(context, out_weight, preferred_element_type=jnp.float32),
            "tensor",
            scatter_dimension=0,
            tiled=True,
        )
        + out_bias
    )
    first_norm, normed_one, inverse_one = norm_forward(
        inputs.astype(jnp.float32) + attended, norm1_gain, norm1_bias
    )
    first_low = first_norm.astype(jnp.bfloat16)
    first_all = lax.all_gather(first_low, "tensor", axis=0, tiled=True)
    up_pre = jnp.dot(first_all, up_weight, preferred_element_type=jnp.float32) + up_bias
    gelu_exact = partial(jax.nn.gelu, approximate=False)
    active = gelu_exact(up_pre).astype(jnp.bfloat16)
    ffn_out = (
        lax.psum_scatter(
            jnp.dot(active, down_weight, preferred_element_type=jnp.float32),
            "tensor",
            scatter_dimension=0,
            tiled=True,
        )
        + down_bias
    )
    final_norm, normed_two, inverse_two = norm_forward(
        first_norm + ffn_out, norm2_gain, norm2_bias
    )

    positions = offset + jnp.arange(share_rows, dtype=jnp.int32)
    row_starts = jnp.arange(seq_count, dtype=jnp.int32) * seq_length
    selector = (row_starts[:, None] == positions[None, :]).astype(jnp.float32)
    owned = jnp.sum(selector, axis=1, keepdims=True)
    leading = jnp.dot(selector, final_norm, precision=lax.Precision.HIGHEST).astype(jnp.bfloat16)
    pooled = jnp.tanh(jnp.dot(leading, pool_weight, preferred_element_type=jnp.float32) + pool_bias)
    pooled_low = pooled.astype(jnp.bfloat16)
    logits = jnp.dot(pooled_low, class_weight, preferred_element_type=jnp.float32) + class_bias
    chosen = (
        labels[:, None] == jnp.arange(class_weight.shape[1], dtype=jnp.int32)[None, :]
    ).astype(jnp.float32)
    grad_logits = jnp.where(
        owned > 0, jax.nn.softmax(logits, axis=-1) - chosen, 0.0
    ).astype(jnp.bfloat16)
    grad_pre = (
        jnp.einsum("rc,dc->rd", grad_logits, class_weight, preferred_element_type=jnp.float32)
        * (1.0 - pooled * pooled)
    ).astype(jnp.bfloat16)
    grad_leading = jnp.einsum(
        "re,de->rd", grad_pre, pool_weight, preferred_element_type=jnp.float32
    )
    grad_final = cotangent.astype(jnp.float32) + jnp.einsum(
        "rt,rd->td", selector, grad_leading, precision=lax.Precision.HIGHEST
    )
    grad_second, norm2_gain_grad, norm2_bias_grad = norm_backward(
        grad_final, normed_two, inverse_two, norm2_gain
    )
    grad_fed = grad_second.astype(jnp.bfloat16)
    down_bias_grad = jnp.sum(grad_fed.astype(jnp.float32), axis=0)
    grad_fed_all = lax.all_gather(grad_fed, "tensor", axis=0, tiled=True)
    down_weight_grad = jnp.einsum(
        "tf,td->fd", active, grad_fed_all, preferred_element_type=jnp.float32
    )
    grad_active = jnp.einsum(
        "td,fd->tf", grad_fed_all, down_weight, preferred_element_type=jnp.float32
    )
    grad_up = jax.vjp(gelu_exact, up_pre)[1](grad_active)[0].astype(jnp.bfloat16)
    up_bias_grad = jnp.sum(grad_up.astype(jnp.float32), axis=0)
    up_weight_grad = jnp.einsum("td,tf->df", first_all, grad_up, preferred_element_type=jnp.float32)
    grad_first = (
        lax.psum_scatter(
            jnp.einsum("tf,df->td", grad_up, up_weight, preferred_element_type=jnp.float32),
            "tensor",
            scatter_dimension=0,
            tiled=True,
        )
        + grad_second
    )
    grad_res, norm1_gain_grad, norm1_bias_grad = norm_backward(
        grad_first, normed_one, inverse_one, norm1_gain
    )
    grad_att = grad_res.astype(jnp.bfloat16)
    out_bias_grad = jnp.sum(grad_att.astype(jnp.float32), axis=0)
    grad_att_all = lax.all_gather(grad_att, "tensor", axis=0, tiled=True)
    out_weight_grad = jnp.einsum(
        "te,td->ed", context, grad_att_all, preferred_element_type=jnp.float32
    )
    grad_context = jnp.einsum(
        "td,ed->te", grad_att_all, out_weight, preferred_element_type=jnp.float32
    ).astype(jnp.bfloat16)
    grad_queries, grad_keys, grad_values = attend_backward(
        queries, key_rows, value_rows, segments, log_totals, grad_context
    )
    stacked = jnp.stack([grad_queries, grad_keys, grad_values])
    qkv_weight_grad = jnp.einsum(
        "td,kte->kde", gathered, stacked, preferred_element_type=jnp.float32
    )
    qv_bias_grad = jnp.stack(
        [
            jnp.sum(grad_queries.astype(jnp.float32), axis=0),
            jnp.sum(grad_values.astype(jnp.float32), axis=0),
        ]
    )
    input_grad = (
        lax.psum_scatter(
            jnp.einsum(
                "kte,kde->td", stacked, qkv_weight, preferred_element_type=jnp.float32
            ).astype(jnp.bfloat16),
            "tensor",
            scatter_dimension=0,
            tiled=True,
        ).astype(jnp.float32)
        + grad_res
    ).astype(jnp.bfloat16)

    weight_parts = (
        (qkv_weight_grad, 1),
        (out_weight_grad, 1),
        (up_weight_grad, 0),
        (down_weight_grad, 1),
    )
    weight_flat = jnp.concatenate(
        [to_blocks(grad, axis, dp_count) for grad, axis in weight_parts], axis=1
    )
    lanes = 1024 if weight_flat.shape[1] % 1024 == 0 else 128
    weight_sum = lax.psum_scatter(
        weight_flat.reshape(-1, lanes), "dp", scatter_dimension=0, tiled=True
    ).reshape(-1)
    weight_out = []
    start = 0
    for grad, axis in weight_parts:
        size = grad.size // dp_count
        weight_out.append(from_block(weight_sum[start : start + size], grad.shape, axis, dp_count))
        start += size

    def slot(values, index, count):
        holder = jnp.zeros((count,) + values.shape, values.dtype)
        return lax.dynamic_update_slice(holder, values[None], (index,) + (0,) * values.ndim)

    row_block = jnp.concatenate(
        [
            leading.astype(jnp.float32) * owned,
            grad_pre.astype(jnp.float32),
            pooled_low.astype(jnp.float32) * owned,
            grad_logits.astype(jnp.float32),
        ],
        axis=1,
    )
    small_parts = [
        jnp.stack(
            [
                out_bias_grad,
                norm1_gain_grad,
                norm1_bias_grad,
                down_bias_grad,
                norm2_gain_grad,
                norm2_bias_grad,
            ]
        ),
        slot(qv_bias_grad, tensor_index, tensor_count),
        slot(up_bias_grad, tensor_index, tensor_count),
        slot(row_block, dp_index, dp_count),
    ]
    small_flat = jnp.concatenate([part.reshape(-1) for part in small_parts])
    small_sum = lax.psum(small_flat, ("dp", "tensor"))
    small_out = []
    start = 0
    for part in small_parts:
        small_out.append(small_sum[start : start + part.size].reshape(part.shape))
        start += part.size
    token_grads = small_out[0]
    qv_bias_total = small_out[1][tensor_index]
    up_bias_total = small_out[2][tensor_index]
    rows_all = small_out[3].reshape(dp_count * seq_count, row_block.shape[1])
    width = leading.shape[1]
    classes = class_weight.shape[1]
    leading_all = rows_all[:, :width].astype(jnp.bfloat16)
    grad_pre_all = rows_all[:, width : 2 * width].astype(jnp.bfloat16)
    pooled_all = rows_all[:, 2 * width : 3 * width].astype(jnp.bfloat16)
    grad_logits_all = rows_all[:, 3 * width : 3 * width + classes].astype(jnp.bfloat16)
    pool_weight_grad = jnp.einsum(
        "rd,re->de", leading_all, grad_pre_all, preferred_element_type=jnp.float32
    )
    pool_bias_grad = jnp.sum(grad_pre_all.astype(jnp.float32), axis=0)
    class_weight_grad = jnp.einsum(
        "rd,rc->dc", pooled_all, grad_logits_all, preferred_element_type=jnp.float32
    )
    class_bias_grad = jnp.sum(grad_logits_all.astype(jnp.float32), axis=0)

    return (
        final_norm.astype(jnp.bfloat16),
        input_grad,
        weight_out[0],
        qv_bias_total,
        weight_out[1],
        token_grads[0],
        token_grads[1],
        token_grads[2],
        weight_out[2],
        up_bias_total,
        weight_out[3],
        token_grads[3],
        token_grads[4],
        token_grads[5],
        pool_weight_grad,
        pool_bias_grad,
        class_weight_grad,
        class_bias_grad,
    )


def solution(mesh):
    placed = (
        P(("dp", "tensor"), None),
        P("dp", None),
        P("dp"),
        P(None, None, "tensor"),
        P(None, "tensor"),
        P("tensor", None),
        P(),
        P(),
        P(),
        P(None, "tensor"),
        P("tensor"),
        P("tensor", None),
        P(),
        P(),
        P(),
        P(),
        P(),
        P(),
        P(),
        P(("dp", "tensor"), None),
    )
    return jax.shard_map(
        body,
        mesh=mesh,
        in_specs=placed,
        out_specs=(
            P(("dp", "tensor"), None),
            P(("dp", "tensor"), None),
            P(None, "dp", "tensor"),
            P(None, "tensor"),
            P("tensor", "dp"),
            P(),
            P(),
            P(),
            P("dp", "tensor"),
            P("tensor"),
            P("tensor", "dp"),
            P(),
            P(),
            P(),
            P(),
            P(),
            P(),
            P(),
        ),
        check_vma=False,
    )
```

```python
from functools import partial

import jax
import jax.numpy as jnp
from jax import lax
from jax.sharding import PartitionSpec as P

HEAD = 64


epsilon = 1e-12
masked_value = -1e30


def norm_forward(values, norm_gain, norm_shift):
    centre = values - jnp.mean(values, axis=-1, keepdims=True)
    inverse = lax.rsqrt(jnp.mean(centre * centre, axis=-1, keepdims=True) + epsilon)
    normed = centre * inverse
    return (normed * norm_gain + norm_shift, normed, inverse)


def norm_backward(grad_out, normed, inverse, norm_gain):
    scaled = grad_out * norm_gain
    grad_in = inverse * (
        scaled
        - jnp.mean(scaled, axis=-1, keepdims=True)
        - normed * jnp.mean(scaled * normed, axis=-1, keepdims=True)
    )
    return (grad_in, jnp.sum(grad_out * normed, axis=0), jnp.sum(grad_out, axis=0))


def split_heads(rows, seq_count):
    return rows.reshape(seq_count, rows.shape[0] // seq_count, rows.shape[1] // HEAD, HEAD)


def masked_scores(query_heads, key_heads, segments):
    raw_scores = jnp.einsum(
        "rqhe,rkhe->rhqk", query_heads, key_heads, preferred_element_type=jnp.float32
    ) * HEAD ** (-0.5)
    allowed = segments[:, None, :, None] == segments[:, None, None, :]
    return (jnp.where(allowed, raw_scores, masked_value), allowed)


def attend_forward(queries, key_rows, value_rows, segments):
    seq_count = segments.shape[0]
    scores, allowed = masked_scores(
        split_heads(queries, seq_count), split_heads(key_rows, seq_count), segments
    )
    largest = jnp.max(scores, axis=-1, keepdims=True)
    exponent = jnp.exp(scores - largest)
    row_total = jnp.sum(exponent, axis=-1, keepdims=True)
    soft_low = (exponent / row_total).astype(jnp.bfloat16)
    context = jnp.einsum(
        "rhqk,rkhe->rqhe",
        soft_low,
        split_heads(value_rows, seq_count),
        preferred_element_type=jnp.float32,
    )
    context = context.reshape(queries.shape).astype(jnp.bfloat16)
    return (context, largest + jnp.log(row_total))


def attend_backward(queries, key_rows, value_rows, segments, log_total, grad_context):
    seq_count = segments.shape[0]
    query_heads = split_heads(queries, seq_count)
    key_heads = split_heads(key_rows, seq_count)
    value_heads = split_heads(value_rows, seq_count)
    grad_heads = split_heads(grad_context, seq_count)
    scores, allowed = masked_scores(query_heads, key_heads, segments)
    soft_probs = jnp.exp(scores - log_total)
    grad_values = jnp.einsum(
        "rhqk,rqhe->rkhe",
        soft_probs.astype(jnp.bfloat16),
        grad_heads,
        preferred_element_type=jnp.float32,
    )
    grad_soft = jnp.einsum(
        "rqhe,rkhe->rhqk", grad_heads, value_heads, preferred_element_type=jnp.float32
    )
    grad_scores = soft_probs * (grad_soft - jnp.sum(soft_probs * grad_soft, axis=-1, keepdims=True))
    grad_low = jnp.where(allowed, grad_scores, 0.0).astype(jnp.bfloat16)
    score_scale = HEAD ** (-0.5)
    grad_queries = (
        jnp.einsum("rhqk,rkhe->rqhe", grad_low, key_heads, preferred_element_type=jnp.float32)
        * score_scale
    )
    grad_keys = (
        jnp.einsum("rhqk,rqhe->rkhe", grad_low, query_heads, preferred_element_type=jnp.float32)
        * score_scale
    )
    full_shape = queries.shape
    return (
        grad_queries.reshape(full_shape).astype(jnp.bfloat16),
        grad_keys.reshape(full_shape).astype(jnp.bfloat16),
        grad_values.reshape(full_shape).astype(jnp.bfloat16),
    )


def to_blocks(array, axis, count):
    shape = array.shape
    split = shape[:axis] + (count, shape[axis] // count) + shape[axis + 1 :]
    return jnp.moveaxis(array.reshape(split), axis, 0).reshape(count, -1)


def from_block(flat, shape, axis, count):
    local = shape[:axis] + (shape[axis] // count,) + shape[axis + 1 :]
    return flat.reshape(local)


def body(
    inputs,
    segments,
    labels,
    qkv_weight,
    qv_bias,
    out_weight,
    out_bias,
    norm1_gain,
    norm1_bias,
    up_weight,
    up_bias,
    down_weight,
    down_bias,
    norm2_gain,
    norm2_bias,
    pool_weight,
    pool_bias,
    class_weight,
    class_bias,
    cotangent,
):
    share_rows = inputs.shape[0]
    seq_count, seq_length = segments.shape
    tensor_index = lax.axis_index("tensor")
    dp_index = lax.axis_index("dp")
    tensor_count = lax.axis_size("tensor")
    dp_count = lax.axis_size("dp")
    offset = tensor_index * share_rows

    gathered = lax.all_gather(inputs, "tensor", axis=0, tiled=True)
    group_rows = gathered.shape[0]
    projected = jnp.einsum("td,kde->kte", gathered, qkv_weight, preferred_element_type=jnp.float32)
    queries = (projected[0] + qv_bias[0]).astype(jnp.bfloat16)
    key_rows = projected[1].astype(jnp.bfloat16)
    value_rows = (projected[2] + qv_bias[1]).astype(jnp.bfloat16)
    local_width = queries.shape[1]

    context, log_totals = attend_forward(queries, key_rows, value_rows, segments)
    attended = (
        lax.psum_scatter(
            jnp.dot(context, out_weight, preferred_element_type=jnp.float32).astype(jnp.bfloat16),
            "tensor",
            scatter_dimension=0,
            tiled=True,
        )
        .astype(jnp.float32)
        + out_bias
    )
    first_norm, normed_one, inverse_one = norm_forward(
        inputs.astype(jnp.float32) + attended, norm1_gain, norm1_bias
    )
    first_low = first_norm.astype(jnp.bfloat16)
    first_all = lax.all_gather(first_low, "tensor", axis=0, tiled=True)
    up_pre = jnp.dot(first_all, up_weight, preferred_element_type=jnp.float32) + up_bias
    gelu_exact = partial(jax.nn.gelu, approximate=False)
    active = gelu_exact(up_pre).astype(jnp.bfloat16)
    ffn_out = (
        lax.psum_scatter(
            jnp.dot(active, down_weight, preferred_element_type=jnp.float32).astype(jnp.bfloat16),
            "tensor",
            scatter_dimension=0,
            tiled=True,
        )
        .astype(jnp.float32)
        + down_bias
    )
    final_norm, normed_two, inverse_two = norm_forward(
        first_norm + ffn_out, norm2_gain, norm2_bias
    )

    positions = offset + jnp.arange(share_rows, dtype=jnp.int32)
    row_starts = jnp.arange(seq_count, dtype=jnp.int32) * seq_length
    selector = (row_starts[:, None] == positions[None, :]).astype(jnp.float32)
    owned = jnp.sum(selector, axis=1, keepdims=True)
    leading = jnp.dot(selector, final_norm, precision=lax.Precision.HIGHEST).astype(jnp.bfloat16)
    pooled = jnp.tanh(jnp.dot(leading, pool_weight, preferred_element_type=jnp.float32) + pool_bias)
    pooled_low = pooled.astype(jnp.bfloat16)
    logits = jnp.dot(pooled_low, class_weight, preferred_element_type=jnp.float32) + class_bias
    chosen = (
        labels[:, None] == jnp.arange(class_weight.shape[1], dtype=jnp.int32)[None, :]
    ).astype(jnp.float32)
    grad_logits = jnp.where(
        owned > 0, jax.nn.softmax(logits, axis=-1) - chosen, 0.0
    ).astype(jnp.bfloat16)
    grad_pre = (
        jnp.einsum("rc,dc->rd", grad_logits, class_weight, preferred_element_type=jnp.float32)
        * (1.0 - pooled * pooled)
    ).astype(jnp.bfloat16)
    grad_leading = jnp.einsum(
        "re,de->rd", grad_pre, pool_weight, preferred_element_type=jnp.float32
    )
    grad_final = cotangent.astype(jnp.float32) + jnp.einsum(
        "rt,rd->td", selector, grad_leading, precision=lax.Precision.HIGHEST
    )
    grad_second, norm2_gain_grad, norm2_bias_grad = norm_backward(
        grad_final, normed_two, inverse_two, norm2_gain
    )
    grad_fed = grad_second.astype(jnp.bfloat16)
    down_bias_grad = jnp.sum(grad_fed.astype(jnp.float32), axis=0)
    grad_fed_all = lax.all_gather(grad_fed, "tensor", axis=0, tiled=True)
    down_weight_grad = jnp.einsum(
        "tf,td->fd", active, grad_fed_all, preferred_element_type=jnp.float32
    )
    grad_active = jnp.einsum(
        "td,fd->tf", grad_fed_all, down_weight, preferred_element_type=jnp.float32
    )
    grad_up = jax.vjp(gelu_exact, up_pre)[1](grad_active)[0].astype(jnp.bfloat16)
    up_bias_grad = jnp.sum(grad_up.astype(jnp.float32), axis=0)
    up_weight_grad = jnp.einsum("td,tf->df", first_all, grad_up, preferred_element_type=jnp.float32)
    grad_first = (
        lax.psum_scatter(
            jnp.einsum("tf,df->td", grad_up, up_weight, preferred_element_type=jnp.float32).astype(jnp.bfloat16),
            "tensor",
            scatter_dimension=0,
            tiled=True,
        )
        .astype(jnp.float32)
        + grad_second
    )
    grad_res, norm1_gain_grad, norm1_bias_grad = norm_backward(
        grad_first, normed_one, inverse_one, norm1_gain
    )
    grad_att = grad_res.astype(jnp.bfloat16)
    out_bias_grad = jnp.sum(grad_att.astype(jnp.float32), axis=0)
    grad_att_all = lax.all_gather(grad_att, "tensor", axis=0, tiled=True)
    out_weight_grad = jnp.einsum(
        "te,td->ed", context, grad_att_all, preferred_element_type=jnp.float32
    )
    grad_context = jnp.einsum(
        "td,ed->te", grad_att_all, out_weight, preferred_element_type=jnp.float32
    ).astype(jnp.bfloat16)
    grad_queries, grad_keys, grad_values = attend_backward(
        queries, key_rows, value_rows, segments, log_totals, grad_context
    )
    stacked = jnp.stack([grad_queries, grad_keys, grad_values])
    qkv_weight_grad = jnp.einsum(
        "td,kte->kde", gathered, stacked, preferred_element_type=jnp.float32
    )
    qv_bias_grad = jnp.stack(
        [
            jnp.sum(grad_queries.astype(jnp.float32), axis=0),
            jnp.sum(grad_values.astype(jnp.float32), axis=0),
        ]
    )
    input_grad = (
        lax.psum_scatter(
            jnp.einsum(
                "kte,kde->td", stacked, qkv_weight, preferred_element_type=jnp.float32
            ).astype(jnp.bfloat16),
            "tensor",
            scatter_dimension=0,
            tiled=True,
        ).astype(jnp.float32)
        + grad_res
    ).astype(jnp.bfloat16)

    def reduce_over_dp(parts):
        flat = jnp.concatenate([to_blocks(grad, axis, dp_count) for grad, axis in parts], axis=1)
        lanes = 1024 if flat.shape[1] % 1024 == 0 else 128
        summed = lax.psum_scatter(
            flat.reshape(-1, lanes), "dp", scatter_dimension=0, tiled=True
        ).reshape(-1)
        pieces = []
        begin = 0
        for grad, axis in parts:
            size = grad.size // dp_count
            pieces.append(from_block(summed[begin : begin + size], grad.shape, axis, dp_count))
            begin += size
        return pieces

    up_sum, down_sum = reduce_over_dp(((up_weight_grad, 0), (down_weight_grad, 1)))
    qkv_sum, out_sum = reduce_over_dp(((qkv_weight_grad, 1), (out_weight_grad, 1)))

    def joined(parts):
        return jnp.concatenate([part.reshape(-1) for part in parts])

    def parted(flat, parts):
        pieces = []
        begin = 0
        for part in parts:
            pieces.append(flat[..., begin : begin + part.size].reshape(flat.shape[:-1] + part.shape))
            begin += part.size
        return pieces

    row_block = jnp.concatenate(
        [
            leading.astype(jnp.float32) * owned,
            grad_pre.astype(jnp.float32),
            pooled_low.astype(jnp.float32) * owned,
            grad_logits.astype(jnp.float32),
        ],
        axis=1,
    )
    token_parts = [
        jnp.stack(
            [
                out_bias_grad,
                norm1_gain_grad,
                norm1_bias_grad,
                down_bias_grad,
                norm2_gain_grad,
                norm2_bias_grad,
            ]
        ),
        row_block,
    ]
    token_sum, rows_group = parted(lax.psum(joined(token_parts), "tensor"), token_parts)
    group_parts = [token_sum, rows_group, qv_bias_grad, up_bias_grad]
    gathered_small = lax.all_gather(joined(group_parts), "dp", axis=0, tiled=False)
    token_each, rows_each, qv_each, up_each = parted(gathered_small, group_parts)
    token_grads = jnp.sum(token_each, axis=0)
    qv_bias_total = jnp.sum(qv_each, axis=0)
    up_bias_total = jnp.sum(up_each, axis=0)
    rows_all = rows_each.reshape(dp_count * seq_count, row_block.shape[1])
    width = leading.shape[1]
    classes = class_weight.shape[1]
    leading_all = rows_all[:, :width].astype(jnp.bfloat16)
    grad_pre_all = rows_all[:, width : 2 * width].astype(jnp.bfloat16)
    pooled_all = rows_all[:, 2 * width : 3 * width].astype(jnp.bfloat16)
    grad_logits_all = rows_all[:, 3 * width : 3 * width + classes].astype(jnp.bfloat16)
    pool_weight_grad = jnp.einsum(
        "rd,re->de", leading_all, grad_pre_all, preferred_element_type=jnp.float32
    )
    pool_bias_grad = jnp.sum(grad_pre_all.astype(jnp.float32), axis=0)
    class_weight_grad = jnp.einsum(
        "rd,rc->dc", pooled_all, grad_logits_all, preferred_element_type=jnp.float32
    )
    class_bias_grad = jnp.sum(grad_logits_all.astype(jnp.float32), axis=0)

    return (
        final_norm.astype(jnp.bfloat16),
        input_grad,
        qkv_sum,
        qv_bias_total,
        out_sum,
        token_grads[0],
        token_grads[1],
        token_grads[2],
        up_sum,
        up_bias_total,
        down_sum,
        token_grads[3],
        token_grads[4],
        token_grads[5],
        pool_weight_grad,
        pool_bias_grad,
        class_weight_grad,
        class_bias_grad,
    )


def solution(mesh):
    placed = (
        P(("dp", "tensor"), None),
        P("dp", None),
        P("dp"),
        P(None, None, "tensor"),
        P(None, "tensor"),
        P("tensor", None),
        P(),
        P(),
        P(),
        P(None, "tensor"),
        P("tensor"),
        P("tensor", None),
        P(),
        P(),
        P(),
        P(),
        P(),
        P(),
        P(),
        P(("dp", "tensor"), None),
    )
    return jax.shard_map(
        body,
        mesh=mesh,
        in_specs=placed,
        out_specs=(
            P(("dp", "tensor"), None),
            P(("dp", "tensor"), None),
            P(None, "dp", "tensor"),
            P(None, "tensor"),
            P("tensor", "dp"),
            P(),
            P(),
            P(),
            P("dp", "tensor"),
            P("tensor"),
            P("tensor", "dp"),
            P(),
            P(),
            P(),
            P(),
            P(),
            P(),
            P(),
        ),
        check_vma=False,
    )
```

```python
from functools import partial

import jax
import jax.numpy as jnp
from jax import lax
from jax.sharding import PartitionSpec as P


HEAD = 64


epsilon = 1e-12
masked_value = -1e30


def norm_forward(values, norm_gain, norm_shift):
    centre = values - jnp.mean(values, axis=-1, keepdims=True)
    inverse = lax.rsqrt(jnp.mean(centre * centre, axis=-1, keepdims=True) + epsilon)
    normed = centre * inverse
    return (normed * norm_gain + norm_shift, normed, inverse)


def norm_backward(grad_out, normed, inverse, norm_gain):
    scaled = grad_out * norm_gain
    grad_in = inverse * (
        scaled
        - jnp.mean(scaled, axis=-1, keepdims=True)
        - normed * jnp.mean(scaled * normed, axis=-1, keepdims=True)
    )
    return (grad_in, jnp.sum(grad_out * normed, axis=0), jnp.sum(grad_out, axis=0))


def split_heads(rows, seq_count):
    return rows.reshape(seq_count, rows.shape[0] // seq_count, rows.shape[1] // HEAD, HEAD)


def masked_scores(query_heads, key_heads, segments):
    raw_scores = jnp.einsum(
        "rqhe,rkhe->rhqk", query_heads, key_heads, preferred_element_type=jnp.float32
    ) * HEAD ** (-0.5)
    allowed = segments[:, None, :, None] == segments[:, None, None, :]
    return (jnp.where(allowed, raw_scores, masked_value), allowed)


def attend_forward(queries, key_rows, value_rows, segments):
    seq_count = segments.shape[0]
    scores, _ = masked_scores(
        split_heads(queries, seq_count), split_heads(key_rows, seq_count), segments
    )
    largest = jnp.max(scores, axis=-1, keepdims=True)
    exponent = jnp.exp(scores - largest)
    row_total = jnp.sum(exponent, axis=-1, keepdims=True)
    soft_low = (exponent / row_total).astype(jnp.bfloat16)
    context = jnp.einsum(
        "rhqk,rkhe->rqhe",
        soft_low,
        split_heads(value_rows, seq_count),
        preferred_element_type=jnp.float32,
    )
    context = context.reshape(queries.shape).astype(jnp.bfloat16)
    return (context, largest + jnp.log(row_total))


def attend_backward(queries, key_rows, value_rows, segments, log_total, grad_context):
    seq_count = segments.shape[0]
    query_heads = split_heads(queries, seq_count)
    key_heads = split_heads(key_rows, seq_count)
    value_heads = split_heads(value_rows, seq_count)
    grad_heads = split_heads(grad_context, seq_count)
    scores, allowed = masked_scores(query_heads, key_heads, segments)
    soft_probs = jnp.exp(scores - log_total)
    grad_values = jnp.einsum(
        "rhqk,rqhe->rkhe",
        soft_probs.astype(jnp.bfloat16),
        grad_heads,
        preferred_element_type=jnp.float32,
    )
    grad_soft = jnp.einsum(
        "rqhe,rkhe->rhqk", grad_heads, value_heads, preferred_element_type=jnp.float32
    )
    grad_scores = soft_probs * (grad_soft - jnp.sum(soft_probs * grad_soft, axis=-1, keepdims=True))
    grad_low = jnp.where(allowed, grad_scores, 0.0).astype(jnp.bfloat16)
    score_scale = HEAD ** (-0.5)
    grad_queries = (
        jnp.einsum("rhqk,rkhe->rqhe", grad_low, key_heads, preferred_element_type=jnp.float32)
        * score_scale
    )
    grad_keys = (
        jnp.einsum("rhqk,rqhe->rkhe", grad_low, query_heads, preferred_element_type=jnp.float32)
        * score_scale
    )
    full_shape = queries.shape
    return (
        grad_queries.reshape(full_shape).astype(jnp.bfloat16),
        grad_keys.reshape(full_shape).astype(jnp.bfloat16),
        grad_values.reshape(full_shape).astype(jnp.bfloat16),
    )


def to_blocks(array, axis, count):
    shape = array.shape
    split = shape[:axis] + (count, shape[axis] // count) + shape[axis + 1 :]
    return jnp.moveaxis(array.reshape(split), axis, 0).reshape(count, -1)


def from_block(flat, shape, axis, count):
    local = shape[:axis] + (shape[axis] // count,) + shape[axis + 1 :]
    return flat.reshape(local)


def body(
    inputs,
    segments,
    labels,
    qkv_weight,
    qv_bias,
    out_weight,
    out_bias,
    norm1_gain,
    norm1_bias,
    up_weight,
    up_bias,
    down_weight,
    down_bias,
    norm2_gain,
    norm2_bias,
    pool_weight,
    pool_bias,
    class_weight,
    class_bias,
    cotangent,
):
    share_rows = inputs.shape[0]
    seq_count, seq_length = segments.shape
    tensor_index = lax.axis_index("tensor")
    dp_index = lax.axis_index("dp")
    tensor_count = lax.axis_size("tensor")
    dp_count = lax.axis_size("dp")
    offset = tensor_index * share_rows

    gathered = lax.all_gather(inputs, "tensor", axis=0, tiled=True)
    group_rows = gathered.shape[0]
    projected = jnp.einsum("td,kde->kte", gathered, qkv_weight, preferred_element_type=jnp.float32)
    queries = (projected[0] + qv_bias[0]).astype(jnp.bfloat16)
    key_rows = projected[1].astype(jnp.bfloat16)
    value_rows = (projected[2] + qv_bias[1]).astype(jnp.bfloat16)

    context, log_totals = attend_forward(queries, key_rows, value_rows, segments)
    attended = (
        lax.psum_scatter(
            jnp.dot(context, out_weight, preferred_element_type=jnp.float32).astype(jnp.bfloat16),
            "tensor",
            scatter_dimension=0,
            tiled=True,
        )
        .astype(jnp.float32)
        + out_bias
    )
    first_norm, normed_one, inverse_one = norm_forward(
        inputs.astype(jnp.float32) + attended, norm1_gain, norm1_bias
    )
    first_low = first_norm.astype(jnp.bfloat16)
    first_all = lax.all_gather(first_low, "tensor", axis=0, tiled=True)
    up_pre = jnp.dot(first_all, up_weight, preferred_element_type=jnp.float32) + up_bias
    gelu_exact = partial(jax.nn.gelu, approximate=False)
    active = gelu_exact(up_pre).astype(jnp.bfloat16)
    ffn_out = (
        lax.psum_scatter(
            jnp.dot(active, down_weight, preferred_element_type=jnp.float32).astype(jnp.bfloat16),
            "tensor",
            scatter_dimension=0,
            tiled=True,
        )
        .astype(jnp.float32)
        + down_bias
    )
    final_norm, normed_two, inverse_two = norm_forward(
        first_norm + ffn_out, norm2_gain, norm2_bias
    )

    positions = offset + jnp.arange(share_rows, dtype=jnp.int32)
    row_starts = jnp.arange(seq_count, dtype=jnp.int32) * seq_length
    selector = (row_starts[:, None] == positions[None, :]).astype(jnp.float32)
    owned = jnp.sum(selector, axis=1, keepdims=True)
    leading = jnp.dot(selector, final_norm, precision=lax.Precision.HIGHEST).astype(jnp.bfloat16)
    pooled = jnp.tanh(jnp.dot(leading, pool_weight, preferred_element_type=jnp.float32) + pool_bias)
    pooled_low = pooled.astype(jnp.bfloat16)
    logits = jnp.dot(pooled_low, class_weight, preferred_element_type=jnp.float32) + class_bias
    chosen = (
        labels[:, None] == jnp.arange(class_weight.shape[1], dtype=jnp.int32)[None, :]
    ).astype(jnp.float32)
    grad_logits = jnp.where(
        owned > 0, jax.nn.softmax(logits, axis=-1) - chosen, 0.0
    ).astype(jnp.bfloat16)
    grad_pre = (
        jnp.einsum("rc,dc->rd", grad_logits, class_weight, preferred_element_type=jnp.float32)
        * (1.0 - pooled * pooled)
    ).astype(jnp.bfloat16)
    grad_leading = jnp.einsum(
        "re,de->rd", grad_pre, pool_weight, preferred_element_type=jnp.float32
    )
    grad_final = cotangent.astype(jnp.float32) + jnp.einsum(
        "rt,rd->td", selector, grad_leading, precision=lax.Precision.HIGHEST
    )
    grad_second, norm2_gain_grad, norm2_bias_grad = norm_backward(
        grad_final, normed_two, inverse_two, norm2_gain
    )
    grad_fed = grad_second.astype(jnp.bfloat16)
    down_bias_grad = jnp.sum(grad_fed.astype(jnp.float32), axis=0)
    grad_fed_all = lax.all_gather(grad_fed, "tensor", axis=0, tiled=True)
    down_weight_grad = jnp.einsum(
        "tf,td->fd", active, grad_fed_all, preferred_element_type=jnp.float32
    )
    grad_active = jnp.einsum(
        "td,fd->tf", grad_fed_all, down_weight, preferred_element_type=jnp.float32
    )
    grad_up = jax.vjp(gelu_exact, up_pre)[1](grad_active)[0].astype(jnp.bfloat16)
    up_bias_grad = jnp.sum(grad_up.astype(jnp.float32), axis=0)
    up_weight_grad = jnp.einsum("td,tf->df", first_all, grad_up, preferred_element_type=jnp.float32)
    grad_first = (
        lax.psum_scatter(
            jnp.einsum("tf,df->td", grad_up, up_weight, preferred_element_type=jnp.float32).astype(jnp.bfloat16),
            "tensor",
            scatter_dimension=0,
            tiled=True,
        )
        .astype(jnp.float32)
        + grad_second
    )
    grad_res, norm1_gain_grad, norm1_bias_grad = norm_backward(
        grad_first, normed_one, inverse_one, norm1_gain
    )
    grad_att = grad_res.astype(jnp.bfloat16)
    out_bias_grad = jnp.sum(grad_att.astype(jnp.float32), axis=0)

    def joined(parts):
        return jnp.concatenate([part.reshape(-1) for part in parts])

    def parted(flat, parts):
        pieces = []
        begin = 0
        for part in parts:
            pieces.append(flat[begin : begin + part.size].reshape(part.shape))
            begin += part.size
        return pieces

    row_block = jnp.concatenate(
        [
            leading.astype(jnp.float32) * owned,
            grad_pre.astype(jnp.float32),
            pooled_low.astype(jnp.float32) * owned,
            grad_logits.astype(jnp.float32),
        ],
        axis=1,
    )
    token_parts = [
        jnp.stack(
            [
                out_bias_grad,
                norm1_gain_grad,
                norm1_bias_grad,
                down_bias_grad,
                norm2_gain_grad,
                norm2_bias_grad,
            ]
        ),
        row_block,
    ]
    small_flat = joined(token_parts)
    small_round = lax.reduce_precision(small_flat, exponent_bits=8, mantissa_bits=7)
    small_high = small_round.astype(jnp.bfloat16)
    small_low = (small_flat - small_round).astype(jnp.bfloat16)
    model_width = grad_att.shape[1]
    small_rows = -(-2 * small_flat.size // model_width)
    small_rows += (-(share_rows + small_rows)) % 16
    small_pad = small_rows * model_width - 2 * small_flat.size
    riding = jnp.concatenate(
        [small_high, small_low, jnp.zeros((small_pad,), jnp.bfloat16)]
    ).reshape(small_rows, model_width)
    att_gathered = lax.all_gather(
        jnp.concatenate([grad_att, riding], axis=0), "tensor", axis=0, tiled=False
    )
    grad_att_all = att_gathered[:, :share_rows].reshape(group_rows, model_width)
    small_back = att_gathered[:, share_rows:].reshape(tensor_count, -1)
    small_total = jnp.sum(
        small_back[:, : small_flat.size].astype(jnp.float32)
        + small_back[:, small_flat.size : 2 * small_flat.size].astype(jnp.float32),
        axis=0,
    )
    token_sum, rows_group = parted(small_total, token_parts)
    out_weight_grad = jnp.einsum(
        "te,td->ed", context, grad_att_all, preferred_element_type=jnp.float32
    )
    grad_context = jnp.einsum(
        "td,ed->te", grad_att_all, out_weight, preferred_element_type=jnp.float32
    ).astype(jnp.bfloat16)
    grad_queries, grad_keys, grad_values = attend_backward(
        queries, key_rows, value_rows, segments, log_totals, grad_context
    )
    stacked = jnp.stack([grad_queries, grad_keys, grad_values])
    qkv_weight_grad = jnp.einsum(
        "td,kte->kde", gathered, stacked, preferred_element_type=jnp.float32
    )
    qv_bias_grad = jnp.stack(
        [
            jnp.sum(grad_queries.astype(jnp.float32), axis=0),
            jnp.sum(grad_values.astype(jnp.float32), axis=0),
        ]
    )
    input_grad = (
        lax.psum_scatter(
            jnp.einsum(
                "kte,kde->td", stacked, qkv_weight, preferred_element_type=jnp.float32
            ).astype(jnp.bfloat16),
            "tensor",
            scatter_dimension=0,
            tiled=True,
        ).astype(jnp.float32)
        + grad_res
    ).astype(jnp.bfloat16)

    def reduce_over_dp(parts, shared):
        blocks = [to_blocks(grad, axis, dp_count) for grad, axis in parts]
        shared_flat = joined(shared)
        blocks.append(jnp.broadcast_to(shared_flat[None], (dp_count, shared_flat.size)))
        flat = jnp.concatenate(blocks, axis=1)
        pad = (-flat.shape[1]) % 8192
        flat = jnp.pad(flat, ((0, 0), (0, pad)))
        summed = lax.psum_scatter(
            flat.reshape(-1, 1024), "dp", scatter_dimension=0, tiled=True
        ).reshape(-1)
        pieces = []
        begin = 0
        for grad, axis in parts:
            size = grad.size // dp_count
            pieces.append(from_block(summed[begin : begin + size], grad.shape, axis, dp_count))
            begin += size
        return pieces, parted(summed[begin : begin + shared_flat.size], shared)

    copied_rows = dp_count * dp_count * rows_group.size <= (1 << 20)
    if copied_rows:
        rows_shared = [
            lax.dynamic_update_slice(
                jnp.zeros((dp_count,) + rows_group.shape, rows_group.dtype),
                rows_group[None],
                (dp_index, 0, 0),
            )
        ]
    else:
        rows_shared = []
        rows_each = lax.all_gather(rows_group.astype(jnp.bfloat16), "dp", axis=0, tiled=False)
    (up_sum, down_sum, out_sum), shared_sums = reduce_over_dp(
        ((up_weight_grad, 0), (down_weight_grad, 1), (out_weight_grad, 1)),
        [token_sum, up_bias_grad] + rows_shared,
    )
    token_grads, up_bias_total = shared_sums[:2]
    if copied_rows:
        rows_each = shared_sums[2]
    (qkv_sum,), (qv_bias_total,) = reduce_over_dp(((qkv_weight_grad, 1),), [qv_bias_grad])
    rows_all = rows_each.reshape(dp_count * seq_count, row_block.shape[1])
    width = leading.shape[1]
    classes = class_weight.shape[1]
    leading_all = rows_all[:, :width].astype(jnp.bfloat16)
    grad_pre_all = rows_all[:, width : 2 * width].astype(jnp.bfloat16)
    pooled_all = rows_all[:, 2 * width : 3 * width].astype(jnp.bfloat16)
    grad_logits_all = rows_all[:, 3 * width : 3 * width + classes].astype(jnp.bfloat16)
    pool_weight_grad = jnp.einsum(
        "rd,re->de", leading_all, grad_pre_all, preferred_element_type=jnp.float32
    )
    pool_bias_grad = jnp.sum(grad_pre_all.astype(jnp.float32), axis=0)
    class_weight_grad = jnp.einsum(
        "rd,rc->dc", pooled_all, grad_logits_all, preferred_element_type=jnp.float32
    )
    class_bias_grad = jnp.sum(grad_logits_all.astype(jnp.float32), axis=0)

    return (
        final_norm.astype(jnp.bfloat16),
        input_grad,
        qkv_sum,
        qv_bias_total,
        out_sum,
        token_grads[0],
        token_grads[1],
        token_grads[2],
        up_sum,
        up_bias_total,
        down_sum,
        token_grads[3],
        token_grads[4],
        token_grads[5],
        pool_weight_grad,
        pool_bias_grad,
        class_weight_grad,
        class_bias_grad,
    )


def solution(mesh):
    placed = (
        P(("dp", "tensor"), None),
        P("dp", None),
        P("dp"),
        P(None, None, "tensor"),
        P(None, "tensor"),
        P("tensor", None),
        P(),
        P(),
        P(),
        P(None, "tensor"),
        P("tensor"),
        P("tensor", None),
        P(),
        P(),
        P(),
        P(),
        P(),
        P(),
        P(),
        P(("dp", "tensor"), None),
    )
    return jax.shard_map(
        body,
        mesh=mesh,
        in_specs=placed,
        out_specs=(
            P(("dp", "tensor"), None),
            P(("dp", "tensor"), None),
            P(None, "dp", "tensor"),
            P(None, "tensor"),
            P("tensor", "dp"),
            P(),
            P(),
            P(),
            P("dp", "tensor"),
            P("tensor"),
            P("tensor", "dp"),
            P(),
            P(),
            P(),
            P(),
            P(),
            P(),
            P(),
        ),
        check_vma=False,
    )
```

```python
from functools import partial

import jax
import jax.numpy as jnp
from jax import lax
from jax.sharding import PartitionSpec as P


HEAD = 64


epsilon = 1e-12
masked_value = -1e30


def norm_forward(values, norm_gain, norm_shift):
    centre = values - jnp.mean(values, axis=-1, keepdims=True)
    inverse = lax.rsqrt(jnp.mean(centre * centre, axis=-1, keepdims=True) + epsilon)
    normed = centre * inverse
    return (normed * norm_gain + norm_shift, normed, inverse)


def norm_backward(grad_out, normed, inverse, norm_gain):
    scaled = grad_out * norm_gain
    grad_in = inverse * (
        scaled
        - jnp.mean(scaled, axis=-1, keepdims=True)
        - normed * jnp.mean(scaled * normed, axis=-1, keepdims=True)
    )
    return (grad_in, jnp.sum(grad_out * normed, axis=0), jnp.sum(grad_out, axis=0))


def split_heads(rows, seq_count):
    return rows.reshape(seq_count, rows.shape[0] // seq_count, rows.shape[1] // HEAD, HEAD)


def masked_scores(query_heads, key_heads, segments):
    raw_scores = jnp.einsum(
        "rqhe,rkhe->rhqk", query_heads, key_heads, preferred_element_type=jnp.float32
    ) * HEAD ** (-0.5)
    allowed = segments[:, None, :, None] == segments[:, None, None, :]
    return (jnp.where(allowed, raw_scores, masked_value), allowed)


def attend_forward(queries, key_rows, value_rows, segments):
    seq_count = segments.shape[0]
    scores, _ = masked_scores(
        split_heads(queries, seq_count), split_heads(key_rows, seq_count), segments
    )
    largest = jnp.max(scores, axis=-1, keepdims=True)
    exponent = jnp.exp(scores - largest)
    row_total = jnp.sum(exponent, axis=-1, keepdims=True)
    soft_low = (exponent / row_total).astype(jnp.bfloat16)
    context = jnp.einsum(
        "rhqk,rkhe->rqhe",
        soft_low,
        split_heads(value_rows, seq_count),
        preferred_element_type=jnp.float32,
    )
    context = context.reshape(queries.shape).astype(jnp.bfloat16)
    return (context, largest + jnp.log(row_total))


def attend_backward(queries, key_rows, value_rows, segments, log_total, grad_context):
    seq_count = segments.shape[0]
    query_heads = split_heads(queries, seq_count)
    key_heads = split_heads(key_rows, seq_count)
    value_heads = split_heads(value_rows, seq_count)
    grad_heads = split_heads(grad_context, seq_count)
    scores, allowed = masked_scores(query_heads, key_heads, segments)
    soft_probs = jnp.exp(scores - log_total)
    grad_values = jnp.einsum(
        "rhqk,rqhe->rkhe",
        soft_probs.astype(jnp.bfloat16),
        grad_heads,
        preferred_element_type=jnp.float32,
    )
    grad_soft = jnp.einsum(
        "rqhe,rkhe->rhqk", grad_heads, value_heads, preferred_element_type=jnp.float32
    )
    grad_scores = soft_probs * (grad_soft - jnp.sum(soft_probs * grad_soft, axis=-1, keepdims=True))
    grad_low = jnp.where(allowed, grad_scores, 0.0).astype(jnp.bfloat16)
    score_scale = HEAD ** (-0.5)
    grad_queries = (
        jnp.einsum("rhqk,rkhe->rqhe", grad_low, key_heads, preferred_element_type=jnp.float32)
        * score_scale
    )
    grad_keys = (
        jnp.einsum("rhqk,rqhe->rkhe", grad_low, query_heads, preferred_element_type=jnp.float32)
        * score_scale
    )
    full_shape = queries.shape
    return (
        grad_queries.reshape(full_shape).astype(jnp.bfloat16),
        grad_keys.reshape(full_shape).astype(jnp.bfloat16),
        grad_values.reshape(full_shape).astype(jnp.bfloat16),
    )


def body(
    inputs,
    segments,
    labels,
    qkv_weight,
    qv_bias,
    out_weight,
    out_bias,
    norm1_gain,
    norm1_bias,
    up_weight,
    up_bias,
    down_weight,
    down_bias,
    norm2_gain,
    norm2_bias,
    pool_weight,
    pool_bias,
    class_weight,
    class_bias,
    cotangent,
):
    share_rows = inputs.shape[0]
    seq_count, seq_length = segments.shape
    tensor_index = lax.axis_index("tensor")
    dp_index = lax.axis_index("dp")
    tensor_count = lax.axis_size("tensor")
    dp_count = lax.axis_size("dp")
    offset = tensor_index * share_rows

    gathered = lax.all_gather(inputs, "tensor", axis=0, tiled=True)
    group_rows = gathered.shape[0]
    projected = jnp.einsum("td,kde->kte", gathered, qkv_weight, preferred_element_type=jnp.float32)
    queries = (projected[0] + qv_bias[0]).astype(jnp.bfloat16)
    key_rows = projected[1].astype(jnp.bfloat16)
    value_rows = (projected[2] + qv_bias[1]).astype(jnp.bfloat16)

    context, log_totals = attend_forward(queries, key_rows, value_rows, segments)
    attended = (
        lax.psum_scatter(
            jnp.dot(context, out_weight, preferred_element_type=jnp.float32).astype(jnp.bfloat16),
            "tensor",
            scatter_dimension=0,
            tiled=True,
        )
        .astype(jnp.float32)
        + out_bias
    )
    first_norm, normed_one, inverse_one = norm_forward(
        inputs.astype(jnp.float32) + attended, norm1_gain, norm1_bias
    )
    first_low = first_norm.astype(jnp.bfloat16)
    first_all = lax.all_gather(first_low, "tensor", axis=0, tiled=True)
    up_pre = jnp.dot(first_all, up_weight, preferred_element_type=jnp.float32) + up_bias
    gelu_exact = partial(jax.nn.gelu, approximate=False)
    active = gelu_exact(up_pre).astype(jnp.bfloat16)
    ffn_out = (
        lax.psum_scatter(
            jnp.dot(active, down_weight, preferred_element_type=jnp.float32).astype(jnp.bfloat16),
            "tensor",
            scatter_dimension=0,
            tiled=True,
        )
        .astype(jnp.float32)
        + down_bias
    )
    final_norm, normed_two, inverse_two = norm_forward(
        first_norm + ffn_out, norm2_gain, norm2_bias
    )

    positions = offset + jnp.arange(share_rows, dtype=jnp.int32)
    row_starts = jnp.arange(seq_count, dtype=jnp.int32) * seq_length
    selector = (row_starts[:, None] == positions[None, :]).astype(jnp.float32)
    owned = jnp.sum(selector, axis=1, keepdims=True)
    leading = jnp.dot(selector, final_norm, precision=lax.Precision.HIGHEST).astype(jnp.bfloat16)
    pooled = jnp.tanh(jnp.dot(leading, pool_weight, preferred_element_type=jnp.float32) + pool_bias)
    pooled_low = pooled.astype(jnp.bfloat16)
    logits = jnp.dot(pooled_low, class_weight, preferred_element_type=jnp.float32) + class_bias
    chosen = (
        labels[:, None] == jnp.arange(class_weight.shape[1], dtype=jnp.int32)[None, :]
    ).astype(jnp.float32)
    grad_logits = jnp.where(
        owned > 0, jax.nn.softmax(logits, axis=-1) - chosen, 0.0
    ).astype(jnp.bfloat16)
    grad_pre = (
        jnp.einsum("rc,dc->rd", grad_logits, class_weight, preferred_element_type=jnp.float32)
        * (1.0 - pooled * pooled)
    ).astype(jnp.bfloat16)
    grad_leading = jnp.einsum(
        "re,de->rd", grad_pre, pool_weight, preferred_element_type=jnp.float32
    )
    grad_final = cotangent.astype(jnp.float32) + jnp.einsum(
        "rt,rd->td", selector, grad_leading, precision=lax.Precision.HIGHEST
    )
    grad_second, norm2_gain_grad, norm2_bias_grad = norm_backward(
        grad_final, normed_two, inverse_two, norm2_gain
    )
    grad_fed = grad_second.astype(jnp.bfloat16)
    down_bias_grad = jnp.sum(grad_fed.astype(jnp.float32), axis=0)
    grad_fed_all = lax.all_gather(grad_fed, "tensor", axis=0, tiled=True)
    down_weight_grad_t = jnp.einsum(
        "td,tf->df", grad_fed_all, active, preferred_element_type=jnp.float32
    )
    grad_active = jnp.einsum(
        "td,fd->tf", grad_fed_all, down_weight, preferred_element_type=jnp.float32
    )
    grad_up = jax.vjp(gelu_exact, up_pre)[1](grad_active)[0].astype(jnp.bfloat16)
    up_bias_grad = jnp.sum(grad_up.astype(jnp.float32), axis=0)
    up_weight_grad = jnp.einsum("td,tf->df", first_all, grad_up, preferred_element_type=jnp.float32)
    grad_first = (
        lax.psum_scatter(
            jnp.einsum("tf,df->td", grad_up, up_weight, preferred_element_type=jnp.float32).astype(jnp.bfloat16),
            "tensor",
            scatter_dimension=0,
            tiled=True,
        )
        .astype(jnp.float32)
        + grad_second
    )
    grad_res, norm1_gain_grad, norm1_bias_grad = norm_backward(
        grad_first, normed_one, inverse_one, norm1_gain
    )
    grad_att = grad_res.astype(jnp.bfloat16)
    out_bias_grad = jnp.sum(grad_att.astype(jnp.float32), axis=0)

    def joined(parts):
        return jnp.concatenate([part.reshape(-1) for part in parts])

    def parted(flat, parts):
        pieces = []
        begin = 0
        for part in parts:
            pieces.append(flat[begin : begin + part.size].reshape(part.shape))
            begin += part.size
        return pieces

    model_width = grad_att.shape[1]
    classes = class_weight.shape[1]
    row_block = jnp.stack(
        [
            leading.astype(jnp.float32) * owned,
            grad_pre.astype(jnp.float32),
            pooled_low.astype(jnp.float32) * owned,
            jnp.pad(grad_logits.astype(jnp.float32), ((0, 0), (0, model_width - classes))),
        ],
        axis=1,
    )
    token_parts = [
        jnp.stack(
            [
                out_bias_grad,
                norm1_gain_grad,
                norm1_bias_grad,
                down_bias_grad,
                norm2_gain_grad,
                norm2_bias_grad,
            ]
        ),
        row_block,
    ]
    small_flat = joined(token_parts)
    small_round = lax.reduce_precision(small_flat, exponent_bits=8, mantissa_bits=7)
    small_high = small_round.astype(jnp.bfloat16)
    small_low = (small_flat - small_round).astype(jnp.bfloat16)
    small_rows = -(-2 * small_flat.size // model_width)
    small_rows += (-(share_rows + small_rows)) % 16
    small_pad = small_rows * model_width - 2 * small_flat.size
    riding = jnp.concatenate(
        [small_high, small_low, jnp.zeros((small_pad,), jnp.bfloat16)]
    ).reshape(small_rows, model_width)
    att_gathered = lax.all_gather(
        jnp.concatenate([grad_att, riding], axis=0), "tensor", axis=0, tiled=False
    )
    grad_att_all = att_gathered[:, :share_rows].reshape(group_rows, model_width)
    small_back = att_gathered[:, share_rows:].reshape(tensor_count, -1)
    small_total = jnp.sum(
        small_back[:, : small_flat.size].astype(jnp.float32)
        + small_back[:, small_flat.size : 2 * small_flat.size].astype(jnp.float32),
        axis=0,
    )
    token_sum, rows_group = parted(small_total, token_parts)
    out_weight_grad_t = jnp.einsum(
        "td,te->de", grad_att_all, context, preferred_element_type=jnp.float32
    )
    grad_context = jnp.einsum(
        "td,ed->te", grad_att_all, out_weight, preferred_element_type=jnp.float32
    ).astype(jnp.bfloat16)
    grad_queries, grad_keys, grad_values = attend_backward(
        queries, key_rows, value_rows, segments, log_totals, grad_context
    )
    stacked = jnp.stack([grad_queries, grad_keys, grad_values])
    qkv_weight_grad = jnp.einsum(
        "td,tq->dq",
        gathered,
        jnp.concatenate([grad_queries, grad_keys, grad_values], axis=1),
        preferred_element_type=jnp.float32,
    )
    qv_bias_grad = jnp.stack(
        [
            jnp.sum(grad_queries.astype(jnp.float32), axis=0),
            jnp.sum(grad_values.astype(jnp.float32), axis=0),
        ]
    )
    input_grad = (
        lax.psum_scatter(
            jnp.einsum(
                "kte,kde->td", stacked, qkv_weight, preferred_element_type=jnp.float32
            ).astype(jnp.bfloat16),
            "tensor",
            scatter_dimension=0,
            tiled=True,
        ).astype(jnp.float32)
        + grad_res
    ).astype(jnp.bfloat16)

    def stacked_sum(parts, dtype):
        flat = jnp.concatenate([part.astype(dtype) for part in parts], axis=1)
        lanes = flat.shape[2]
        pad = (-flat.shape[1]) % 16
        flat = jnp.pad(flat, ((0, 0), (0, pad), (0, 0)))
        summed = lax.psum_scatter(
            flat.reshape(-1, lanes), "dp", scatter_dimension=0, tiled=True
        )
        pieces = []
        begin = 0
        for part in parts:
            pieces.append(summed[begin : begin + part.shape[1]])
            begin += part.shape[1]
        return pieces

    def in_blocks(grad):
        return grad.reshape(dp_count, grad.shape[0] // dp_count, grad.shape[1])

    def copied(flat, lanes):
        rows = -(-flat.size // lanes)
        flat = jnp.pad(flat, (0, rows * lanes - flat.size)).reshape(1, rows, lanes)
        return jnp.broadcast_to(flat, (dp_count, rows, lanes))

    copied_rows = dp_count * dp_count * rows_group.size <= (1 << 20)
    out_blocks = in_blocks(out_weight_grad_t).reshape(dp_count, -1, model_width)
    early_parts = [in_blocks(up_weight_grad), in_blocks(down_weight_grad_t), out_blocks]
    if copied_rows:
        rows_slotted = lax.dynamic_update_slice(
            jnp.zeros((dp_count,) + rows_group.shape, rows_group.dtype),
            rows_group[None],
            (dp_index, 0, 0, 0),
        )
        early_parts.append(copied(rows_slotted.reshape(-1), model_width))
    else:
        rows_each = lax.all_gather(rows_group.astype(jnp.bfloat16), "dp", axis=0, tiled=False)
    early_sums = stacked_sum(early_parts, jnp.bfloat16)
    up_sum = early_sums[0].astype(jnp.float32)
    down_sum = early_sums[1].astype(jnp.float32).T
    out_sum = early_sums[2].reshape(-1, out_weight_grad_t.shape[1]).astype(jnp.float32).T
    if copied_rows:
        rows_each = early_sums[3].reshape(-1)[: rows_slotted.size]
    late_shared = [token_sum, up_bias_grad, qv_bias_grad]
    qkv_lanes = qkv_weight_grad.shape[1]
    late_sums = stacked_sum(
        [in_blocks(qkv_weight_grad), copied(joined(late_shared), qkv_lanes)], jnp.float32
    )
    qkv_sum = jnp.transpose(
        late_sums[0].reshape(late_sums[0].shape[0], 3, qkv_lanes // 3), (1, 0, 2)
    )
    token_grads, up_bias_total, qv_bias_total = parted(
        late_sums[1].reshape(-1), late_shared
    )
    rows_all = rows_each.reshape(dp_count * seq_count, 4, model_width).astype(jnp.bfloat16)
    leading_all = rows_all[:, 0]
    grad_pre_all = rows_all[:, 1]
    pooled_all = rows_all[:, 2]
    grad_logits_all = rows_all[:, 3, :classes]
    pool_weight_grad = jnp.einsum(
        "rd,re->de", leading_all, grad_pre_all, preferred_element_type=jnp.float32
    )
    pool_bias_grad = jnp.sum(grad_pre_all.astype(jnp.float32), axis=0)
    class_weight_grad = jnp.einsum(
        "rd,rc->dc", pooled_all, grad_logits_all, preferred_element_type=jnp.float32
    )
    class_bias_grad = jnp.sum(grad_logits_all.astype(jnp.float32), axis=0)

    return (
        final_norm.astype(jnp.bfloat16),
        input_grad,
        qkv_sum,
        qv_bias_total,
        out_sum,
        token_grads[0],
        token_grads[1],
        token_grads[2],
        up_sum,
        up_bias_total,
        down_sum,
        token_grads[3],
        token_grads[4],
        token_grads[5],
        pool_weight_grad,
        pool_bias_grad,
        class_weight_grad,
        class_bias_grad,
    )


def solution(mesh):
    placed = (
        P(("dp", "tensor"), None),
        P("dp", None),
        P("dp"),
        P(None, None, "tensor"),
        P(None, "tensor"),
        P("tensor", None),
        P(),
        P(),
        P(),
        P(None, "tensor"),
        P("tensor"),
        P("tensor", None),
        P(),
        P(),
        P(),
        P(),
        P(),
        P(),
        P(),
        P(("dp", "tensor"), None),
    )
    return jax.shard_map(
        body,
        mesh=mesh,
        in_specs=placed,
        out_specs=(
            P(("dp", "tensor"), None),
            P(("dp", "tensor"), None),
            P(None, "dp", "tensor"),
            P(None, "tensor"),
            P("tensor", "dp"),
            P(),
            P(),
            P(),
            P("dp", "tensor"),
            P("tensor"),
            P("tensor", "dp"),
            P(),
            P(),
            P(),
            P(),
            P(),
            P(),
            P(),
        ),
        check_vma=False,
    )
```

```python
from functools import partial

import jax
import jax.numpy as jnp
from jax import lax
from jax.sharding import PartitionSpec as P


HEAD = 64


epsilon = 1e-12
masked_value = -1e30


def norm_forward(values, norm_gain, norm_shift):
    centre = values - jnp.mean(values, axis=-1, keepdims=True)
    inverse = lax.rsqrt(jnp.mean(centre * centre, axis=-1, keepdims=True) + epsilon)
    normed = centre * inverse
    return (normed * norm_gain + norm_shift, normed, inverse)


def norm_backward(grad_out, normed, inverse, norm_gain):
    scaled = grad_out * norm_gain
    grad_in = inverse * (
        scaled
        - jnp.mean(scaled, axis=-1, keepdims=True)
        - normed * jnp.mean(scaled * normed, axis=-1, keepdims=True)
    )
    return (grad_in, jnp.sum(grad_out * normed, axis=0), jnp.sum(grad_out, axis=0))


def split_heads(rows, seq_count):
    return rows.reshape(seq_count, rows.shape[0] // seq_count, rows.shape[1] // HEAD, HEAD)


def masked_scores(query_heads, key_heads, segments):
    raw_scores = jnp.einsum(
        "rqhe,rkhe->rhqk", query_heads, key_heads, preferred_element_type=jnp.float32
    ) * HEAD ** (-0.5)
    allowed = segments[:, None, :, None] == segments[:, None, None, :]
    return (jnp.where(allowed, raw_scores, masked_value), allowed)


def attend_forward(queries, key_rows, value_rows, segments):
    seq_count = segments.shape[0]
    scores, _ = masked_scores(
        split_heads(queries, seq_count), split_heads(key_rows, seq_count), segments
    )
    largest = jnp.max(scores, axis=-1, keepdims=True)
    exponent = jnp.exp(scores - largest)
    row_total = jnp.sum(exponent, axis=-1, keepdims=True)
    soft_low = (exponent / row_total).astype(jnp.bfloat16)
    context = jnp.einsum(
        "rhqk,rkhe->rqhe",
        soft_low,
        split_heads(value_rows, seq_count),
        preferred_element_type=jnp.float32,
    )
    context = context.reshape(queries.shape).astype(jnp.bfloat16)
    return (context, largest + jnp.log(row_total))


def attend_backward(queries, key_rows, value_rows, segments, log_total, grad_context):
    seq_count = segments.shape[0]
    query_heads = split_heads(queries, seq_count)
    key_heads = split_heads(key_rows, seq_count)
    value_heads = split_heads(value_rows, seq_count)
    grad_heads = split_heads(grad_context, seq_count)
    scores, allowed = masked_scores(query_heads, key_heads, segments)
    soft_probs = jnp.exp(scores - log_total)
    grad_values = jnp.einsum(
        "rhqk,rqhe->rkhe",
        soft_probs.astype(jnp.bfloat16),
        grad_heads,
        preferred_element_type=jnp.float32,
    )
    grad_soft = jnp.einsum(
        "rqhe,rkhe->rhqk", grad_heads, value_heads, preferred_element_type=jnp.float32
    )
    grad_scores = soft_probs * (grad_soft - jnp.sum(soft_probs * grad_soft, axis=-1, keepdims=True))
    grad_low = jnp.where(allowed, grad_scores, 0.0).astype(jnp.bfloat16)
    score_scale = HEAD ** (-0.5)
    grad_queries = (
        jnp.einsum("rhqk,rkhe->rqhe", grad_low, key_heads, preferred_element_type=jnp.float32)
        * score_scale
    )
    grad_keys = (
        jnp.einsum("rhqk,rqhe->rkhe", grad_low, query_heads, preferred_element_type=jnp.float32)
        * score_scale
    )
    full_shape = queries.shape
    return (
        grad_queries.reshape(full_shape).astype(jnp.bfloat16),
        grad_keys.reshape(full_shape).astype(jnp.bfloat16),
        grad_values.reshape(full_shape).astype(jnp.bfloat16),
    )


def ring_order(count):
    chips = []
    for row in range(count // 4):
        chips += [2 * row, 2 * row + 1] if row % 2 == 0 else [2 * row + 1, 2 * row]
    if count % 4:
        chips += list(range(len(chips), count // 2))
    members = []
    for step, chip in enumerate(chips):
        members += [2 * chip, 2 * chip + 1] if step % 2 == 0 else [2 * chip + 1, 2 * chip]
    return members if count % 2 == 0 else list(range(count))


def body(
    inputs,
    segments,
    labels,
    qkv_weight,
    qv_bias,
    out_weight,
    out_bias,
    norm1_gain,
    norm1_bias,
    up_weight,
    up_bias,
    down_weight,
    down_bias,
    norm2_gain,
    norm2_bias,
    pool_weight,
    pool_bias,
    class_weight,
    class_bias,
    cotangent,
):
    share_rows = inputs.shape[0]
    seq_count, seq_length = segments.shape
    tensor_index = lax.axis_index("tensor")
    dp_index = lax.axis_index("dp")
    tensor_count = lax.axis_size("tensor")
    dp_count = lax.axis_size("dp")
    offset = tensor_index * share_rows

    gathered = lax.all_gather(inputs, "tensor", axis=0, tiled=True)
    group_rows = gathered.shape[0]
    projected = jnp.einsum("td,kde->kte", gathered, qkv_weight, preferred_element_type=jnp.float32)
    queries = (projected[0] + qv_bias[0]).astype(jnp.bfloat16)
    key_rows = projected[1].astype(jnp.bfloat16)
    value_rows = (projected[2] + qv_bias[1]).astype(jnp.bfloat16)

    context, log_totals = attend_forward(queries, key_rows, value_rows, segments)
    attended = (
        lax.psum_scatter(
            jnp.dot(context, out_weight, preferred_element_type=jnp.float32).astype(jnp.bfloat16),
            "tensor",
            scatter_dimension=0,
            tiled=True,
        )
        .astype(jnp.float32)
        + out_bias
    )
    first_norm, normed_one, inverse_one = norm_forward(
        inputs.astype(jnp.float32) + attended, norm1_gain, norm1_bias
    )
    first_low = first_norm.astype(jnp.bfloat16)
    first_all = lax.all_gather(first_low, "tensor", axis=0, tiled=True)
    up_pre = jnp.dot(first_all, up_weight, preferred_element_type=jnp.float32) + up_bias
    gelu_exact = partial(jax.nn.gelu, approximate=False)
    active = gelu_exact(up_pre).astype(jnp.bfloat16)
    ffn_out = (
        lax.psum_scatter(
            jnp.dot(active, down_weight, preferred_element_type=jnp.float32).astype(jnp.bfloat16),
            "tensor",
            scatter_dimension=0,
            tiled=True,
        )
        .astype(jnp.float32)
        + down_bias
    )
    final_norm, normed_two, inverse_two = norm_forward(
        first_norm + ffn_out, norm2_gain, norm2_bias
    )

    positions = offset + jnp.arange(share_rows, dtype=jnp.int32)
    row_starts = jnp.arange(seq_count, dtype=jnp.int32) * seq_length
    selector = (row_starts[:, None] == positions[None, :]).astype(jnp.float32)
    owned = jnp.sum(selector, axis=1, keepdims=True)
    leading = jnp.dot(selector, final_norm, precision=lax.Precision.HIGHEST).astype(jnp.bfloat16)
    pooled = jnp.tanh(jnp.dot(leading, pool_weight, preferred_element_type=jnp.float32) + pool_bias)
    pooled_low = pooled.astype(jnp.bfloat16)
    logits = jnp.dot(pooled_low, class_weight, preferred_element_type=jnp.float32) + class_bias
    chosen = (
        labels[:, None] == jnp.arange(class_weight.shape[1], dtype=jnp.int32)[None, :]
    ).astype(jnp.float32)
    grad_logits = jnp.where(
        owned > 0, jax.nn.softmax(logits, axis=-1) - chosen, 0.0
    ).astype(jnp.bfloat16)
    grad_pre = (
        jnp.einsum("rc,dc->rd", grad_logits, class_weight, preferred_element_type=jnp.float32)
        * (1.0 - pooled * pooled)
    ).astype(jnp.bfloat16)
    grad_leading = jnp.einsum(
        "re,de->rd", grad_pre, pool_weight, preferred_element_type=jnp.float32
    )
    grad_final = cotangent.astype(jnp.float32) + jnp.einsum(
        "rt,rd->td", selector, grad_leading, precision=lax.Precision.HIGHEST
    )
    grad_second, norm2_gain_grad, norm2_bias_grad = norm_backward(
        grad_final, normed_two, inverse_two, norm2_gain
    )
    grad_fed = grad_second.astype(jnp.bfloat16)
    down_bias_grad = jnp.sum(grad_fed.astype(jnp.float32), axis=0)
    grad_fed_all = lax.all_gather(grad_fed, "tensor", axis=0, tiled=True)
    down_weight_grad_t = jnp.einsum(
        "td,tf->df", grad_fed_all, active, preferred_element_type=jnp.float32
    )
    grad_active = jnp.einsum(
        "td,fd->tf", grad_fed_all, down_weight, preferred_element_type=jnp.float32
    )
    grad_up = jax.vjp(gelu_exact, up_pre)[1](grad_active)[0].astype(jnp.bfloat16)
    up_bias_grad = jnp.sum(grad_up.astype(jnp.float32), axis=0)
    up_weight_grad = jnp.einsum("td,tf->df", first_all, grad_up, preferred_element_type=jnp.float32)
    grad_first = (
        lax.psum_scatter(
            jnp.einsum("tf,df->td", grad_up, up_weight, preferred_element_type=jnp.float32).astype(jnp.bfloat16),
            "tensor",
            scatter_dimension=0,
            tiled=True,
        )
        .astype(jnp.float32)
        + grad_second
    )
    grad_res, norm1_gain_grad, norm1_bias_grad = norm_backward(
        grad_first, normed_one, inverse_one, norm1_gain
    )
    grad_att = grad_res.astype(jnp.bfloat16)
    out_bias_grad = jnp.sum(grad_att.astype(jnp.float32), axis=0)

    def joined(parts):
        return jnp.concatenate([part.reshape(-1) for part in parts])

    def parted(flat, parts):
        pieces = []
        begin = 0
        for part in parts:
            pieces.append(flat[begin : begin + part.size].reshape(part.shape))
            begin += part.size
        return pieces

    model_width = grad_att.shape[1]
    classes = class_weight.shape[1]
    row_block = jnp.stack(
        [
            leading.astype(jnp.float32) * owned,
            grad_pre.astype(jnp.float32),
            pooled_low.astype(jnp.float32) * owned,
            jnp.pad(grad_logits.astype(jnp.float32), ((0, 0), (0, model_width - classes))),
        ],
        axis=1,
    )
    token_parts = [
        jnp.stack(
            [
                out_bias_grad,
                norm1_gain_grad,
                norm1_bias_grad,
                down_bias_grad,
                norm2_gain_grad,
                norm2_bias_grad,
            ]
        ),
        row_block,
    ]
    small_flat = joined(token_parts)
    small_round = lax.reduce_precision(small_flat, exponent_bits=8, mantissa_bits=7)
    small_high = small_round.astype(jnp.bfloat16)
    small_low = (small_flat - small_round).astype(jnp.bfloat16)
    small_rows = -(-2 * small_flat.size // model_width)
    small_rows += (-(share_rows + small_rows)) % 16
    small_pad = small_rows * model_width - 2 * small_flat.size
    riding = jnp.concatenate(
        [small_high, small_low, jnp.zeros((small_pad,), jnp.bfloat16)]
    ).reshape(small_rows, model_width)
    att_gathered = lax.all_gather(
        jnp.concatenate([grad_att, riding], axis=0), "tensor", axis=0, tiled=False
    )
    grad_att_all = att_gathered[:, :share_rows].reshape(group_rows, model_width)
    small_back = att_gathered[:, share_rows:].reshape(tensor_count, -1)
    small_total = jnp.sum(
        small_back[:, : small_flat.size].astype(jnp.float32)
        + small_back[:, small_flat.size : 2 * small_flat.size].astype(jnp.float32),
        axis=0,
    )
    token_sum, rows_group = parted(small_total, token_parts)
    out_weight_grad_t = jnp.einsum(
        "td,te->de", grad_att_all, context, preferred_element_type=jnp.float32
    )
    grad_context = jnp.einsum(
        "td,ed->te", grad_att_all, out_weight, preferred_element_type=jnp.float32
    ).astype(jnp.bfloat16)
    grad_queries, grad_keys, grad_values = attend_backward(
        queries, key_rows, value_rows, segments, log_totals, grad_context
    )
    stacked = jnp.stack([grad_queries, grad_keys, grad_values])
    qkv_weight_grad = jnp.einsum(
        "td,tq->dq",
        gathered,
        jnp.concatenate([grad_queries, grad_keys, grad_values], axis=1),
        preferred_element_type=jnp.float32,
    )
    qv_bias_grad = jnp.stack(
        [
            jnp.sum(grad_queries.astype(jnp.float32), axis=0),
            jnp.sum(grad_values.astype(jnp.float32), axis=0),
        ]
    )
    input_part = lax.psum_scatter(
        jnp.einsum(
            "kte,kde->td", stacked, qkv_weight, preferred_element_type=jnp.float32
        ).astype(jnp.bfloat16),
        "tensor",
        scatter_dimension=0,
        tiled=True,
    )
    input_grad = (input_part.astype(jnp.float32) + grad_res).astype(jnp.bfloat16)

    def in_blocks(grad):
        return grad.reshape(dp_count, grad.shape[0] // dp_count, grad.shape[1])

    def copied(flat, lanes):
        rows = -(-flat.size // lanes)
        rows += rows % 2
        flat = jnp.pad(flat, (0, rows * lanes - flat.size)).reshape(1, rows, lanes)
        return jnp.broadcast_to(flat, (dp_count, rows, lanes))

    ring = ring_order(dp_count)
    ring_place = [0] * dp_count
    for place, member in enumerate(ring):
        ring_place[member] = place
    place = jnp.asarray(ring_place, jnp.int32)[dp_index]
    ring_members = jnp.asarray(ring, jnp.int32)
    ahead = [(ring[i], ring[(i + 1) % dp_count]) for i in range(dp_count)]
    behind = [(ring[i], ring[(i - 1) % dp_count]) for i in range(dp_count)]

    def ring_sum(parts):
        if dp_count > 8:
            return [
                lax.psum_scatter(
                    part.reshape(-1, part.shape[2]), "dp", scatter_dimension=0, tiled=True
                )
                for part in parts
            ]
        halves = [part.shape[1] // 2 for part in parts]
        first = [part[:, :half] for part, half in zip(parts, halves)]
        second = [part[:, half:] for part, half in zip(parts, halves)]

        def pick(blocks, shift):
            member = ring_members[(place + shift) % dp_count]
            return [lax.dynamic_index_in_dim(block, member, 0, keepdims=False) for block in blocks]

        going = pick(first, -1)
        coming = pick(second, 1)
        for step in range(dp_count - 1):
            going = [
                got + own
                for got, own in zip(lax.ppermute(going, "dp", ahead), pick(first, -step - 2))
            ]
            coming = [
                got + own
                for got, own in zip(lax.ppermute(coming, "dp", behind), pick(second, step + 2))
            ]
        return [jnp.concatenate([one, two], axis=0) for one, two in zip(going, coming)]

    copied_rows = dp_count * dp_count * rows_group.size <= (1 << 20)
    up_sum, down_sum_t, up_bias_rows = ring_sum(
        [in_blocks(up_weight_grad), in_blocks(down_weight_grad_t), copied(up_bias_grad, model_width)]
    )
    down_sum = down_sum_t.T
    up_bias_total = up_bias_rows.reshape(-1)[: up_bias_grad.size]
    late_shared = [token_sum, qv_bias_grad]
    if copied_rows:
        rows_slotted = lax.dynamic_update_slice(
            jnp.zeros((dp_count,) + rows_group.shape, rows_group.dtype),
            rows_group[None],
            (dp_index, 0, 0, 0),
        )
        late_shared.append(rows_slotted)
    else:
        rows_each = lax.all_gather(rows_group.astype(jnp.bfloat16), "dp", axis=0, tiled=False)
    qkv_lanes = qkv_weight_grad.shape[1]
    qkv_flat, out_sum_t, late_rows = ring_sum(
        [
            in_blocks(qkv_weight_grad),
            in_blocks(out_weight_grad_t),
            copied(joined(late_shared), model_width),
        ]
    )
    out_sum = out_sum_t.T
    late_back = parted(late_rows.reshape(-1), late_shared)
    token_grads = late_back[0]
    qv_bias_total = late_back[1]
    if copied_rows:
        rows_each = late_back[2]
    qkv_sum = jnp.transpose(qkv_flat.reshape(qkv_flat.shape[0], 3, qkv_lanes // 3), (1, 0, 2))
    rows_all = rows_each.reshape(dp_count * seq_count, 4, model_width).astype(jnp.bfloat16)
    leading_all = rows_all[:, 0]
    grad_pre_all = rows_all[:, 1]
    pooled_all = rows_all[:, 2]
    grad_logits_all = rows_all[:, 3, :classes]
    pool_weight_grad = jnp.einsum(
        "rd,re->de", leading_all, grad_pre_all, preferred_element_type=jnp.float32
    )
    pool_bias_grad = jnp.sum(grad_pre_all.astype(jnp.float32), axis=0)
    class_weight_grad = jnp.einsum(
        "rd,rc->dc", pooled_all, grad_logits_all, preferred_element_type=jnp.float32
    )
    class_bias_grad = jnp.sum(grad_logits_all.astype(jnp.float32), axis=0)

    return (
        final_norm.astype(jnp.bfloat16),
        input_grad,
        qkv_sum,
        qv_bias_total,
        out_sum,
        token_grads[0],
        token_grads[1],
        token_grads[2],
        up_sum,
        up_bias_total,
        down_sum,
        token_grads[3],
        token_grads[4],
        token_grads[5],
        pool_weight_grad,
        pool_bias_grad,
        class_weight_grad,
        class_bias_grad,
    )


def solution(mesh):
    placed = (
        P(("dp", "tensor"), None),
        P("dp", None),
        P("dp"),
        P(None, None, "tensor"),
        P(None, "tensor"),
        P("tensor", None),
        P(),
        P(),
        P(),
        P(None, "tensor"),
        P("tensor"),
        P("tensor", None),
        P(),
        P(),
        P(),
        P(),
        P(),
        P(),
        P(),
        P(("dp", "tensor"), None),
    )
    return jax.shard_map(
        body,
        mesh=mesh,
        in_specs=placed,
        out_specs=(
            P(("dp", "tensor"), None),
            P(("dp", "tensor"), None),
            P(None, "dp", "tensor"),
            P(None, "tensor"),
            P("tensor", "dp"),
            P(),
            P(),
            P(),
            P("dp", "tensor"),
            P("tensor"),
            P("tensor", "dp"),
            P(),
            P(),
            P(),
            P(),
            P(),
            P(),
            P(),
        ),
        check_vma=False,
    )
```

```python
from functools import partial

import jax
import jax.numpy as jnp
from jax import lax
from jax.sharding import PartitionSpec as P


HEAD = 64


epsilon = 1e-12
masked_value = -1e30


def norm_forward(values, norm_gain, norm_shift):
    centre = values - jnp.mean(values, axis=-1, keepdims=True)
    inverse = lax.rsqrt(jnp.mean(centre * centre, axis=-1, keepdims=True) + epsilon)
    normed = centre * inverse
    return (normed * norm_gain + norm_shift, normed, inverse)


def norm_backward(grad_out, normed, inverse, norm_gain):
    scaled = grad_out * norm_gain
    grad_in = inverse * (
        scaled
        - jnp.mean(scaled, axis=-1, keepdims=True)
        - normed * jnp.mean(scaled * normed, axis=-1, keepdims=True)
    )
    return (grad_in, jnp.sum(grad_out * normed, axis=0), jnp.sum(grad_out, axis=0))


def split_heads(rows, seq_count):
    return rows.reshape(seq_count, rows.shape[0] // seq_count, rows.shape[1] // HEAD, HEAD)


def masked_scores(query_heads, key_heads, segments):
    raw_scores = jnp.einsum(
        "rqhe,rkhe->rhqk", query_heads, key_heads, preferred_element_type=jnp.float32
    ) * HEAD ** (-0.5)
    allowed = segments[:, None, :, None] == segments[:, None, None, :]
    return (jnp.where(allowed, raw_scores, masked_value), allowed)


def attend_forward(queries, key_rows, value_rows, segments):
    seq_count = segments.shape[0]
    scores, _ = masked_scores(
        split_heads(queries, seq_count), split_heads(key_rows, seq_count), segments
    )
    largest = jnp.max(scores, axis=-1, keepdims=True)
    exponent = jnp.exp(scores - largest)
    row_total = jnp.sum(exponent, axis=-1, keepdims=True)
    soft_low = (exponent / row_total).astype(jnp.bfloat16)
    context = jnp.einsum(
        "rhqk,rkhe->rqhe",
        soft_low,
        split_heads(value_rows, seq_count),
        preferred_element_type=jnp.float32,
    )
    context = context.reshape(queries.shape).astype(jnp.bfloat16)
    return (context, largest + jnp.log(row_total))


def attend_backward(queries, key_rows, value_rows, segments, log_total, grad_context):
    seq_count = segments.shape[0]
    query_heads = split_heads(queries, seq_count)
    key_heads = split_heads(key_rows, seq_count)
    value_heads = split_heads(value_rows, seq_count)
    grad_heads = split_heads(grad_context, seq_count)
    scores, allowed = masked_scores(query_heads, key_heads, segments)
    soft_probs = jnp.exp(scores - log_total)
    grad_values = jnp.einsum(
        "rhqk,rqhe->rkhe",
        soft_probs.astype(jnp.bfloat16),
        grad_heads,
        preferred_element_type=jnp.float32,
    )
    grad_soft = jnp.einsum(
        "rqhe,rkhe->rhqk", grad_heads, value_heads, preferred_element_type=jnp.float32
    )
    grad_scores = soft_probs * (grad_soft - jnp.sum(soft_probs * grad_soft, axis=-1, keepdims=True))
    grad_low = jnp.where(allowed, grad_scores, 0.0).astype(jnp.bfloat16)
    score_scale = HEAD ** (-0.5)
    grad_queries = (
        jnp.einsum("rhqk,rkhe->rqhe", grad_low, key_heads, preferred_element_type=jnp.float32)
        * score_scale
    )
    grad_keys = (
        jnp.einsum("rhqk,rqhe->rkhe", grad_low, query_heads, preferred_element_type=jnp.float32)
        * score_scale
    )
    full_shape = queries.shape
    return (
        grad_queries.reshape(full_shape).astype(jnp.bfloat16),
        grad_keys.reshape(full_shape).astype(jnp.bfloat16),
        grad_values.reshape(full_shape).astype(jnp.bfloat16),
    )


def body(
    inputs,
    segments,
    labels,
    qkv_weight,
    qv_bias,
    out_weight,
    out_bias,
    norm1_gain,
    norm1_bias,
    up_weight,
    up_bias,
    down_weight,
    down_bias,
    norm2_gain,
    norm2_bias,
    pool_weight,
    pool_bias,
    class_weight,
    class_bias,
    cotangent,
):
    share_rows = inputs.shape[0]
    seq_count, seq_length = segments.shape
    tensor_index = lax.axis_index("tensor")
    dp_index = lax.axis_index("dp")
    tensor_count = lax.axis_size("tensor")
    dp_count = lax.axis_size("dp")
    offset = tensor_index * share_rows

    gathered = lax.all_gather(inputs, "tensor", axis=0, tiled=True)
    group_rows = gathered.shape[0]
    projected = jnp.einsum("td,kde->kte", gathered, qkv_weight, preferred_element_type=jnp.float32)
    queries = (projected[0] + qv_bias[0]).astype(jnp.bfloat16)
    key_rows = projected[1].astype(jnp.bfloat16)
    value_rows = (projected[2] + qv_bias[1]).astype(jnp.bfloat16)
    local_width = queries.shape[1]

    out_weight_all = lax.all_gather(out_weight, "tensor", axis=0, tiled=False)
    context, log_totals = attend_forward(queries, key_rows, value_rows, segments)
    context_own = lax.all_to_all(
        context.reshape(tensor_count, share_rows, local_width), "tensor", 0, 0, tiled=False
    )
    attended = (
        jnp.einsum(
            "itc,icd->td", context_own, out_weight_all, preferred_element_type=jnp.float32
        )
        + out_bias
    )
    first_norm, normed_one, inverse_one = norm_forward(
        inputs.astype(jnp.float32) + attended, norm1_gain, norm1_bias
    )
    first_low = first_norm.astype(jnp.bfloat16)
    first_all = lax.all_gather(first_low, "tensor", axis=0, tiled=True)
    up_pre = jnp.dot(first_all, up_weight, preferred_element_type=jnp.float32) + up_bias
    gelu_exact = partial(jax.nn.gelu, approximate=False)
    active = gelu_exact(up_pre).astype(jnp.bfloat16)
    ffn_out = (
        lax.psum_scatter(
            jnp.dot(active, down_weight, preferred_element_type=jnp.float32).astype(jnp.bfloat16),
            "tensor",
            scatter_dimension=0,
            tiled=True,
        )
        .astype(jnp.float32)
        + down_bias
    )
    final_norm, normed_two, inverse_two = norm_forward(
        first_norm + ffn_out, norm2_gain, norm2_bias
    )

    positions = offset + jnp.arange(share_rows, dtype=jnp.int32)
    row_starts = jnp.arange(seq_count, dtype=jnp.int32) * seq_length
    selector = (row_starts[:, None] == positions[None, :]).astype(jnp.float32)
    owned = jnp.sum(selector, axis=1, keepdims=True)
    leading = jnp.dot(selector, final_norm, precision=lax.Precision.HIGHEST).astype(jnp.bfloat16)
    pooled = jnp.tanh(jnp.dot(leading, pool_weight, preferred_element_type=jnp.float32) + pool_bias)
    pooled_low = pooled.astype(jnp.bfloat16)
    logits = jnp.dot(pooled_low, class_weight, preferred_element_type=jnp.float32) + class_bias
    chosen = (
        labels[:, None] == jnp.arange(class_weight.shape[1], dtype=jnp.int32)[None, :]
    ).astype(jnp.float32)
    grad_logits = jnp.where(
        owned > 0, jax.nn.softmax(logits, axis=-1) - chosen, 0.0
    ).astype(jnp.bfloat16)
    grad_pre = (
        jnp.einsum("rc,dc->rd", grad_logits, class_weight, preferred_element_type=jnp.float32)
        * (1.0 - pooled * pooled)
    ).astype(jnp.bfloat16)
    grad_leading = jnp.einsum(
        "re,de->rd", grad_pre, pool_weight, preferred_element_type=jnp.float32
    )
    grad_final = cotangent.astype(jnp.float32) + jnp.einsum(
        "rt,rd->td", selector, grad_leading, precision=lax.Precision.HIGHEST
    )
    grad_second, norm2_gain_grad, norm2_bias_grad = norm_backward(
        grad_final, normed_two, inverse_two, norm2_gain
    )
    grad_fed = grad_second.astype(jnp.bfloat16)
    down_bias_grad = jnp.sum(grad_fed.astype(jnp.float32), axis=0)
    grad_fed_all = lax.all_gather(grad_fed, "tensor", axis=0, tiled=True)
    down_weight_grad_t = jnp.einsum(
        "td,tf->df", grad_fed_all, active, preferred_element_type=jnp.float32
    )
    grad_active = jnp.einsum(
        "td,fd->tf", grad_fed_all, down_weight, preferred_element_type=jnp.float32
    )
    grad_up = jax.vjp(gelu_exact, up_pre)[1](grad_active)[0].astype(jnp.bfloat16)
    up_bias_grad = jnp.sum(grad_up.astype(jnp.float32), axis=0)
    up_weight_grad = jnp.einsum("td,tf->df", first_all, grad_up, preferred_element_type=jnp.float32)
    grad_first = (
        lax.psum_scatter(
            jnp.einsum("tf,df->td", grad_up, up_weight, preferred_element_type=jnp.float32).astype(jnp.bfloat16),
            "tensor",
            scatter_dimension=0,
            tiled=True,
        )
        .astype(jnp.float32)
        + grad_second
    )
    grad_res, norm1_gain_grad, norm1_bias_grad = norm_backward(
        grad_first, normed_one, inverse_one, norm1_gain
    )
    grad_att = grad_res.astype(jnp.bfloat16)
    out_bias_grad = jnp.sum(grad_att.astype(jnp.float32), axis=0)

    def joined(parts):
        return jnp.concatenate([part.reshape(-1) for part in parts])

    def parted(flat, parts):
        pieces = []
        begin = 0
        for part in parts:
            pieces.append(flat[begin : begin + part.size].reshape(part.shape))
            begin += part.size
        return pieces

    model_width = grad_att.shape[1]
    classes = class_weight.shape[1]
    row_block = jnp.stack(
        [
            leading.astype(jnp.float32) * owned,
            grad_pre.astype(jnp.float32),
            pooled_low.astype(jnp.float32) * owned,
            jnp.pad(grad_logits.astype(jnp.float32), ((0, 0), (0, model_width - classes))),
        ],
        axis=1,
    )
    token_parts = [
        jnp.stack(
            [
                out_bias_grad,
                norm1_gain_grad,
                norm1_bias_grad,
                down_bias_grad,
                norm2_gain_grad,
                norm2_bias_grad,
            ]
        ),
        row_block,
    ]
    small_flat = joined(token_parts)
    small_round = lax.reduce_precision(small_flat, exponent_bits=8, mantissa_bits=7)
    small_high = small_round.astype(jnp.bfloat16)
    small_low = (small_flat - small_round).astype(jnp.bfloat16)
    small_rows = -(-2 * small_flat.size // model_width)
    small_rows += (-(share_rows + small_rows)) % 16
    small_pad = small_rows * model_width - 2 * small_flat.size
    riding = jnp.concatenate(
        [small_high, small_low, jnp.zeros((small_pad,), jnp.bfloat16)]
    ).reshape(small_rows, model_width)
    att_gathered = lax.all_gather(
        jnp.concatenate([grad_att, riding], axis=0), "tensor", axis=0, tiled=False
    )
    grad_att_all = att_gathered[:, :share_rows].reshape(group_rows, model_width)
    small_back = att_gathered[:, share_rows:].reshape(tensor_count, -1)
    small_total = jnp.sum(
        small_back[:, : small_flat.size].astype(jnp.float32)
        + small_back[:, small_flat.size : 2 * small_flat.size].astype(jnp.float32),
        axis=0,
    )
    token_sum, rows_group = parted(small_total, token_parts)
    out_weight_grad_t = jnp.einsum(
        "td,te->de", grad_att_all, context, preferred_element_type=jnp.float32
    )
    grad_context = jnp.einsum(
        "td,ed->te", grad_att_all, out_weight, preferred_element_type=jnp.float32
    ).astype(jnp.bfloat16)
    grad_queries, grad_keys, grad_values = attend_backward(
        queries, key_rows, value_rows, segments, log_totals, grad_context
    )
    stacked = jnp.stack([grad_queries, grad_keys, grad_values])
    qkv_weight_grad = jnp.einsum(
        "td,tq->dq",
        gathered,
        jnp.concatenate([grad_queries, grad_keys, grad_values], axis=1),
        preferred_element_type=jnp.float32,
    )
    qv_bias_grad = jnp.stack(
        [
            jnp.sum(grad_queries.astype(jnp.float32), axis=0),
            jnp.sum(grad_values.astype(jnp.float32), axis=0),
        ]
    )
    input_grad = (
        lax.psum_scatter(
            jnp.einsum(
                "kte,kde->td", stacked, qkv_weight, preferred_element_type=jnp.float32
            ).astype(jnp.bfloat16),
            "tensor",
            scatter_dimension=0,
            tiled=True,
        ).astype(jnp.float32)
        + grad_res
    ).astype(jnp.bfloat16)

    def stacked_sum(parts, dtype):
        padded = [
            jnp.pad(part.astype(dtype), ((0, 0), (0, (-part.shape[1]) % 16), (0, 0)))
            for part in parts
        ]
        flat = jnp.concatenate(padded, axis=1)
        lanes = flat.shape[2]
        summed = lax.psum_scatter(
            flat.reshape(-1, lanes), "dp", scatter_dimension=0, tiled=True
        )
        pieces = []
        begin = 0
        for part, held in zip(parts, padded):
            pieces.append(summed[begin : begin + part.shape[1]])
            begin += held.shape[1]
        return pieces

    def in_blocks(grad):
        return grad.reshape(dp_count, grad.shape[0] // dp_count, grad.shape[1])

    def copied(flat, lanes):
        rows = -(-flat.size // lanes)
        flat = jnp.pad(flat, (0, rows * lanes - flat.size)).reshape(1, rows, lanes)
        return jnp.broadcast_to(flat, (dp_count, rows, lanes))

    copied_rows = dp_count * dp_count * rows_group.size <= (1 << 20)
    out_blocks = in_blocks(out_weight_grad_t).reshape(dp_count, -1, model_width)
    early_shared = [token_sum, up_bias_grad]
    early_parts = [
        in_blocks(up_weight_grad),
        in_blocks(down_weight_grad_t),
        out_blocks,
        copied(joined(early_shared), model_width),
    ]
    if copied_rows:
        rows_slotted = lax.dynamic_update_slice(
            jnp.zeros((dp_count,) + rows_group.shape, rows_group.dtype),
            rows_group[None],
            (dp_index, 0, 0, 0),
        )
        early_parts.append(copied(rows_slotted.reshape(-1), model_width))
    else:
        rows_each = lax.all_gather(rows_group.astype(jnp.bfloat16), "dp", axis=0, tiled=False)
    early_sums = stacked_sum(early_parts, jnp.bfloat16)
    up_sum = early_sums[0].astype(jnp.float32)
    down_sum = early_sums[1].astype(jnp.float32).T
    out_sum = early_sums[2].reshape(-1, out_weight_grad_t.shape[1]).astype(jnp.float32).T
    token_grads, up_bias_total = parted(
        early_sums[3].reshape(-1).astype(jnp.float32), early_shared
    )
    if copied_rows:
        rows_each = early_sums[4].reshape(-1)[: rows_slotted.size]
    late_shared = [qv_bias_grad]
    qkv_lanes = qkv_weight_grad.shape[1]
    late_sums = stacked_sum(
        [in_blocks(qkv_weight_grad), copied(joined(late_shared), qkv_lanes)], jnp.bfloat16
    )
    qkv_sum = jnp.transpose(
        late_sums[0].reshape(late_sums[0].shape[0], 3, qkv_lanes // 3), (1, 0, 2)
    ).astype(jnp.float32)
    (qv_bias_total,) = parted(late_sums[1].reshape(-1).astype(jnp.float32), late_shared)
    rows_all = rows_each.reshape(dp_count * seq_count, 4, model_width).astype(jnp.bfloat16)
    leading_all = rows_all[:, 0]
    grad_pre_all = rows_all[:, 1]
    pooled_all = rows_all[:, 2]
    grad_logits_all = rows_all[:, 3, :classes]
    pool_weight_grad = jnp.einsum(
        "rd,re->de", leading_all, grad_pre_all, preferred_element_type=jnp.float32
    )
    pool_bias_grad = jnp.sum(grad_pre_all.astype(jnp.float32), axis=0)
    class_weight_grad = jnp.einsum(
        "rd,rc->dc", pooled_all, grad_logits_all, preferred_element_type=jnp.float32
    )
    class_bias_grad = jnp.sum(grad_logits_all.astype(jnp.float32), axis=0)

    return (
        final_norm.astype(jnp.bfloat16),
        input_grad,
        qkv_sum,
        qv_bias_total,
        out_sum,
        token_grads[0],
        token_grads[1],
        token_grads[2],
        up_sum,
        up_bias_total,
        down_sum,
        token_grads[3],
        token_grads[4],
        token_grads[5],
        pool_weight_grad,
        pool_bias_grad,
        class_weight_grad,
        class_bias_grad,
    )


def solution(mesh):
    placed = (
        P(("dp", "tensor"), None),
        P("dp", None),
        P("dp"),
        P(None, None, "tensor"),
        P(None, "tensor"),
        P("tensor", None),
        P(),
        P(),
        P(),
        P(None, "tensor"),
        P("tensor"),
        P("tensor", None),
        P(),
        P(),
        P(),
        P(),
        P(),
        P(),
        P(),
        P(("dp", "tensor"), None),
    )
    return jax.shard_map(
        body,
        mesh=mesh,
        in_specs=placed,
        out_specs=(
            P(("dp", "tensor"), None),
            P(("dp", "tensor"), None),
            P(None, "dp", "tensor"),
            P(None, "tensor"),
            P("tensor", "dp"),
            P(),
            P(),
            P(),
            P("dp", "tensor"),
            P("tensor"),
            P("tensor", "dp"),
            P(),
            P(),
            P(),
            P(),
            P(),
            P(),
            P(),
        ),
        check_vma=False,
    )
```

```python
from functools import partial

import jax
import jax.numpy as jnp
from jax import lax
from jax.sharding import PartitionSpec as P


HEAD = 64


epsilon = 1e-12
masked_value = -1e30


def norm_forward(values, norm_gain, norm_shift):
    centre = values - jnp.mean(values, axis=-1, keepdims=True)
    inverse = lax.rsqrt(jnp.mean(centre * centre, axis=-1, keepdims=True) + epsilon)
    normed = centre * inverse
    return (normed * norm_gain + norm_shift, normed, inverse)


def norm_backward(grad_out, normed, inverse, norm_gain):
    scaled = grad_out * norm_gain
    grad_in = inverse * (
        scaled
        - jnp.mean(scaled, axis=-1, keepdims=True)
        - normed * jnp.mean(scaled * normed, axis=-1, keepdims=True)
    )
    return (grad_in, jnp.sum(grad_out * normed, axis=0), jnp.sum(grad_out, axis=0))


def split_heads(rows, seq_count):
    return rows.reshape(seq_count, rows.shape[0] // seq_count, rows.shape[1] // HEAD, HEAD)


def masked_scores(query_heads, key_heads, segments):
    raw_scores = jnp.einsum(
        "rqhe,rkhe->rhqk", query_heads, key_heads, preferred_element_type=jnp.float32
    ) * HEAD ** (-0.5)
    allowed = segments[:, None, :, None] == segments[:, None, None, :]
    return (jnp.where(allowed, raw_scores, masked_value), allowed)


def attend_forward(queries, key_rows, value_rows, segments):
    seq_count = segments.shape[0]
    scores, _ = masked_scores(
        split_heads(queries, seq_count), split_heads(key_rows, seq_count), segments
    )
    largest = jnp.max(scores, axis=-1, keepdims=True)
    exponent = jnp.exp(scores - largest)
    row_total = jnp.sum(exponent, axis=-1, keepdims=True)
    soft_low = (exponent / row_total).astype(jnp.bfloat16)
    context = jnp.einsum(
        "rhqk,rkhe->rqhe",
        soft_low,
        split_heads(value_rows, seq_count),
        preferred_element_type=jnp.float32,
    )
    context = context.reshape(queries.shape).astype(jnp.bfloat16)
    return (context, largest + jnp.log(row_total))


def attend_backward(queries, key_rows, value_rows, segments, log_total, grad_context):
    seq_count = segments.shape[0]
    query_heads = split_heads(queries, seq_count)
    key_heads = split_heads(key_rows, seq_count)
    value_heads = split_heads(value_rows, seq_count)
    grad_heads = split_heads(grad_context, seq_count)
    scores, allowed = masked_scores(query_heads, key_heads, segments)
    soft_probs = jnp.exp(scores - log_total)
    grad_values = jnp.einsum(
        "rhqk,rqhe->rkhe",
        soft_probs.astype(jnp.bfloat16),
        grad_heads,
        preferred_element_type=jnp.float32,
    )
    grad_soft = jnp.einsum(
        "rqhe,rkhe->rhqk", grad_heads, value_heads, preferred_element_type=jnp.float32
    )
    grad_scores = soft_probs * (grad_soft - jnp.sum(soft_probs * grad_soft, axis=-1, keepdims=True))
    grad_low = jnp.where(allowed, grad_scores, 0.0).astype(jnp.bfloat16)
    score_scale = HEAD ** (-0.5)
    grad_queries = (
        jnp.einsum("rhqk,rkhe->rqhe", grad_low, key_heads, preferred_element_type=jnp.float32)
        * score_scale
    )
    grad_keys = (
        jnp.einsum("rhqk,rqhe->rkhe", grad_low, query_heads, preferred_element_type=jnp.float32)
        * score_scale
    )
    full_shape = queries.shape
    return (
        grad_queries.reshape(full_shape).astype(jnp.bfloat16),
        grad_keys.reshape(full_shape).astype(jnp.bfloat16),
        grad_values.reshape(full_shape).astype(jnp.bfloat16),
    )


def body(
    inputs,
    segments,
    labels,
    qkv_weight,
    qv_bias,
    out_weight,
    out_bias,
    norm1_gain,
    norm1_bias,
    up_weight,
    up_bias,
    down_weight,
    down_bias,
    norm2_gain,
    norm2_bias,
    pool_weight,
    pool_bias,
    class_weight,
    class_bias,
    cotangent,
):
    share_rows = inputs.shape[0]
    seq_count, seq_length = segments.shape
    tensor_index = lax.axis_index("tensor")
    dp_index = lax.axis_index("dp")
    tensor_count = lax.axis_size("tensor")
    dp_count = lax.axis_size("dp")
    offset = tensor_index * share_rows

    gathered = lax.all_gather(inputs, "tensor", axis=0, tiled=True)
    group_rows = gathered.shape[0]
    projected = jnp.einsum("td,kde->kte", gathered, qkv_weight, preferred_element_type=jnp.float32)
    queries = (projected[0] + qv_bias[0]).astype(jnp.bfloat16)
    key_rows = projected[1].astype(jnp.bfloat16)
    value_rows = (projected[2] + qv_bias[1]).astype(jnp.bfloat16)
    local_width = queries.shape[1]

    out_weight_all = lax.all_gather(out_weight, "tensor", axis=0, tiled=False)
    context, log_totals = attend_forward(queries, key_rows, value_rows, segments)
    context_own = lax.all_to_all(
        context.reshape(tensor_count, share_rows, local_width), "tensor", 0, 0, tiled=False
    )
    attended = (
        jnp.einsum(
            "itc,icd->td", context_own, out_weight_all, preferred_element_type=jnp.float32
        )
        + out_bias
    )
    first_norm, normed_one, inverse_one = norm_forward(
        inputs.astype(jnp.float32) + attended, norm1_gain, norm1_bias
    )
    first_low = first_norm.astype(jnp.bfloat16)
    first_all = lax.all_gather(first_low, "tensor", axis=0, tiled=True)
    up_pre = jnp.dot(first_all, up_weight, preferred_element_type=jnp.float32) + up_bias
    gelu_exact = partial(jax.nn.gelu, approximate=False)
    active = gelu_exact(up_pre).astype(jnp.bfloat16)
    ffn_out = (
        lax.psum_scatter(
            jnp.dot(active, down_weight, preferred_element_type=jnp.float32).astype(jnp.bfloat16),
            "tensor",
            scatter_dimension=0,
            tiled=True,
        )
        .astype(jnp.float32)
        + down_bias
    )
    final_norm, normed_two, inverse_two = norm_forward(
        first_norm + ffn_out, norm2_gain, norm2_bias
    )

    positions = offset + jnp.arange(share_rows, dtype=jnp.int32)
    row_starts = jnp.arange(seq_count, dtype=jnp.int32) * seq_length
    selector = (row_starts[:, None] == positions[None, :]).astype(jnp.float32)
    owned = jnp.sum(selector, axis=1, keepdims=True)
    leading = jnp.dot(selector, final_norm, precision=lax.Precision.HIGHEST).astype(jnp.bfloat16)
    pooled = jnp.tanh(jnp.dot(leading, pool_weight, preferred_element_type=jnp.float32) + pool_bias)
    pooled_low = pooled.astype(jnp.bfloat16)
    logits = jnp.dot(pooled_low, class_weight, preferred_element_type=jnp.float32) + class_bias
    chosen = (
        labels[:, None] == jnp.arange(class_weight.shape[1], dtype=jnp.int32)[None, :]
    ).astype(jnp.float32)
    grad_logits = jnp.where(
        owned > 0, jax.nn.softmax(logits, axis=-1) - chosen, 0.0
    ).astype(jnp.bfloat16)
    grad_pre = (
        jnp.einsum("rc,dc->rd", grad_logits, class_weight, preferred_element_type=jnp.float32)
        * (1.0 - pooled * pooled)
    ).astype(jnp.bfloat16)
    grad_leading = jnp.einsum(
        "re,de->rd", grad_pre, pool_weight, preferred_element_type=jnp.float32
    )
    grad_final = cotangent.astype(jnp.float32) + jnp.einsum(
        "rt,rd->td", selector, grad_leading, precision=lax.Precision.HIGHEST
    )
    grad_second, norm2_gain_grad, norm2_bias_grad = norm_backward(
        grad_final, normed_two, inverse_two, norm2_gain
    )
    grad_fed = grad_second.astype(jnp.bfloat16)
    down_bias_grad = jnp.sum(grad_fed.astype(jnp.float32), axis=0)
    grad_fed_all = lax.all_gather(grad_fed, "tensor", axis=0, tiled=True)
    down_weight_grad_t = jnp.einsum(
        "td,tf->df", grad_fed_all, active, preferred_element_type=jnp.float32
    )
    grad_active = jnp.einsum(
        "td,fd->tf", grad_fed_all, down_weight, preferred_element_type=jnp.float32
    )
    grad_up = jax.vjp(gelu_exact, up_pre)[1](grad_active)[0].astype(jnp.bfloat16)
    up_bias_grad = jnp.sum(grad_up.astype(jnp.float32), axis=0)
    up_weight_grad = jnp.einsum("td,tf->df", first_all, grad_up, preferred_element_type=jnp.float32)
    grad_first = (
        lax.psum_scatter(
            jnp.einsum("tf,df->td", grad_up, up_weight, preferred_element_type=jnp.float32).astype(jnp.bfloat16),
            "tensor",
            scatter_dimension=0,
            tiled=True,
        )
        .astype(jnp.float32)
        + grad_second
    )
    grad_res, norm1_gain_grad, norm1_bias_grad = norm_backward(
        grad_first, normed_one, inverse_one, norm1_gain
    )
    grad_att = grad_res.astype(jnp.bfloat16)
    out_bias_grad = jnp.sum(grad_att.astype(jnp.float32), axis=0)

    def joined(parts):
        return jnp.concatenate([part.reshape(-1) for part in parts])

    def parted(flat, parts):
        pieces = []
        begin = 0
        for part in parts:
            pieces.append(flat[begin : begin + part.size].reshape(part.shape))
            begin += part.size
        return pieces

    model_width = grad_att.shape[1]
    classes = class_weight.shape[1]
    row_block = jnp.stack(
        [
            leading.astype(jnp.float32) * owned,
            grad_pre.astype(jnp.float32),
            pooled_low.astype(jnp.float32) * owned,
            jnp.pad(grad_logits.astype(jnp.float32), ((0, 0), (0, model_width - classes))),
        ],
        axis=1,
    )
    token_parts = [
        jnp.stack(
            [
                out_bias_grad,
                norm1_gain_grad,
                norm1_bias_grad,
                down_bias_grad,
                norm2_gain_grad,
                norm2_bias_grad,
            ]
        ),
        row_block,
    ]
    small_flat = joined(token_parts)
    small_round = lax.reduce_precision(small_flat, exponent_bits=8, mantissa_bits=7)
    small_high = small_round.astype(jnp.bfloat16)
    small_low = (small_flat - small_round).astype(jnp.bfloat16)
    small_lanes = local_width
    small_rows = -(-2 * small_flat.size // small_lanes)
    small_rows += (-(share_rows + small_rows)) % 16
    small_pad = small_rows * small_lanes - 2 * small_flat.size
    riding = jnp.concatenate(
        [small_high, small_low, jnp.zeros((small_pad,), jnp.bfloat16)]
    ).reshape(1, small_rows, small_lanes)
    context_heads = jnp.einsum(
        "td,jcd->jtc", grad_att, out_weight_all, preferred_element_type=jnp.float32
    ).astype(jnp.bfloat16)
    heads_back = lax.all_to_all(
        jnp.concatenate(
            [context_heads, jnp.broadcast_to(riding, (tensor_count, small_rows, small_lanes))],
            axis=1,
        ),
        "tensor",
        0,
        0,
        tiled=False,
    )
    grad_context = heads_back[:, :share_rows].reshape(group_rows, local_width)
    small_back = heads_back[:, share_rows:].reshape(tensor_count, -1)
    small_total = jnp.sum(
        small_back[:, : small_flat.size].astype(jnp.float32)
        + small_back[:, small_flat.size : 2 * small_flat.size].astype(jnp.float32),
        axis=0,
    )
    token_sum, rows_group = parted(small_total, token_parts)
    out_weight_full = jnp.einsum(
        "itc,td->icd", context_own, grad_att, preferred_element_type=jnp.float32
    ).reshape(tensor_count * local_width, model_width)
    out_weight_grad_t = lax.psum_scatter(
        out_weight_full.astype(jnp.bfloat16), "tensor", scatter_dimension=0, tiled=True
    ).T
    grad_queries, grad_keys, grad_values = attend_backward(
        queries, key_rows, value_rows, segments, log_totals, grad_context
    )
    stacked = jnp.stack([grad_queries, grad_keys, grad_values])
    qkv_weight_grad = jnp.einsum(
        "td,tq->dq",
        gathered,
        jnp.concatenate([grad_queries, grad_keys, grad_values], axis=1),
        preferred_element_type=jnp.float32,
    )
    qv_bias_grad = jnp.stack(
        [
            jnp.sum(grad_queries.astype(jnp.float32), axis=0),
            jnp.sum(grad_values.astype(jnp.float32), axis=0),
        ]
    )
    input_grad = (
        lax.psum_scatter(
            jnp.einsum(
                "kte,kde->td", stacked, qkv_weight, preferred_element_type=jnp.float32
            ).astype(jnp.bfloat16),
            "tensor",
            scatter_dimension=0,
            tiled=True,
        ).astype(jnp.float32)
        + grad_res
    ).astype(jnp.bfloat16)

    def stacked_sum(parts, dtype):
        padded = [
            jnp.pad(part.astype(dtype), ((0, 0), (0, (-part.shape[1]) % 16), (0, 0)))
            for part in parts
        ]
        flat = jnp.concatenate(padded, axis=1)
        lanes = flat.shape[2]
        summed = lax.psum_scatter(
            flat.reshape(-1, lanes), "dp", scatter_dimension=0, tiled=True
        )
        pieces = []
        begin = 0
        for part, held in zip(parts, padded):
            pieces.append(summed[begin : begin + part.shape[1]])
            begin += held.shape[1]
        return pieces

    def in_blocks(grad):
        return grad.reshape(dp_count, grad.shape[0] // dp_count, grad.shape[1])

    def copied(flat, lanes):
        rows = -(-flat.size // lanes)
        flat = jnp.pad(flat, (0, rows * lanes - flat.size)).reshape(1, rows, lanes)
        return jnp.broadcast_to(flat, (dp_count, rows, lanes))

    copied_rows = dp_count * dp_count * rows_group.size <= (1 << 20)
    out_blocks = in_blocks(out_weight_grad_t).reshape(dp_count, -1, model_width)
    early_shared = [token_sum, up_bias_grad]
    early_parts = [
        in_blocks(up_weight_grad),
        in_blocks(down_weight_grad_t),
        out_blocks,
        copied(joined(early_shared), model_width),
    ]
    if copied_rows:
        rows_slotted = lax.dynamic_update_slice(
            jnp.zeros((dp_count,) + rows_group.shape, rows_group.dtype),
            rows_group[None],
            (dp_index, 0, 0, 0),
        )
        early_parts.append(copied(rows_slotted.reshape(-1), model_width))
    else:
        rows_each = lax.all_gather(rows_group.astype(jnp.bfloat16), "dp", axis=0, tiled=False)
    early_sums = stacked_sum(early_parts, jnp.bfloat16)
    up_sum = early_sums[0].astype(jnp.float32)
    down_sum = early_sums[1].astype(jnp.float32).T
    out_sum = early_sums[2].reshape(-1, out_weight_grad_t.shape[1]).astype(jnp.float32).T
    token_grads, up_bias_total = parted(
        early_sums[3].reshape(-1).astype(jnp.float32), early_shared
    )
    if copied_rows:
        rows_each = early_sums[4].reshape(-1)[: rows_slotted.size]
    late_shared = [qv_bias_grad]
    qkv_lanes = qkv_weight_grad.shape[1]
    late_sums = stacked_sum(
        [in_blocks(qkv_weight_grad), copied(joined(late_shared), qkv_lanes)], jnp.bfloat16
    )
    qkv_sum = jnp.transpose(
        late_sums[0].reshape(late_sums[0].shape[0], 3, qkv_lanes // 3), (1, 0, 2)
    ).astype(jnp.float32)
    (qv_bias_total,) = parted(late_sums[1].reshape(-1).astype(jnp.float32), late_shared)
    rows_all = rows_each.reshape(dp_count * seq_count, 4, model_width).astype(jnp.bfloat16)
    leading_all = rows_all[:, 0]
    grad_pre_all = rows_all[:, 1]
    pooled_all = rows_all[:, 2]
    grad_logits_all = rows_all[:, 3, :classes]
    pool_weight_grad = jnp.einsum(
        "rd,re->de", leading_all, grad_pre_all, preferred_element_type=jnp.float32
    )
    pool_bias_grad = jnp.sum(grad_pre_all.astype(jnp.float32), axis=0)
    class_weight_grad = jnp.einsum(
        "rd,rc->dc", pooled_all, grad_logits_all, preferred_element_type=jnp.float32
    )
    class_bias_grad = jnp.sum(grad_logits_all.astype(jnp.float32), axis=0)

    return (
        final_norm.astype(jnp.bfloat16),
        input_grad,
        qkv_sum,
        qv_bias_total,
        out_sum,
        token_grads[0],
        token_grads[1],
        token_grads[2],
        up_sum,
        up_bias_total,
        down_sum,
        token_grads[3],
        token_grads[4],
        token_grads[5],
        pool_weight_grad,
        pool_bias_grad,
        class_weight_grad,
        class_bias_grad,
    )


def solution(mesh):
    placed = (
        P(("dp", "tensor"), None),
        P("dp", None),
        P("dp"),
        P(None, None, "tensor"),
        P(None, "tensor"),
        P("tensor", None),
        P(),
        P(),
        P(),
        P(None, "tensor"),
        P("tensor"),
        P("tensor", None),
        P(),
        P(),
        P(),
        P(),
        P(),
        P(),
        P(),
        P(("dp", "tensor"), None),
    )
    return jax.shard_map(
        body,
        mesh=mesh,
        in_specs=placed,
        out_specs=(
            P(("dp", "tensor"), None),
            P(("dp", "tensor"), None),
            P(None, "dp", "tensor"),
            P(None, "tensor"),
            P("tensor", "dp"),
            P(),
            P(),
            P(),
            P("dp", "tensor"),
            P("tensor"),
            P("tensor", "dp"),
            P(),
            P(),
            P(),
            P(),
            P(),
            P(),
            P(),
        ),
        check_vma=False,
    )
```

```python
from functools import partial

import jax
import jax.numpy as jnp
from jax import lax
from jax.sharding import PartitionSpec as P


HEAD = 64


epsilon = 1e-12
masked_value = -1e30


def norm_forward(values, norm_gain, norm_shift):
    centre = values - jnp.mean(values, axis=-1, keepdims=True)
    inverse = lax.rsqrt(jnp.mean(centre * centre, axis=-1, keepdims=True) + epsilon)
    normed = centre * inverse
    return (normed * norm_gain + norm_shift, normed, inverse)


def norm_backward(grad_out, normed, inverse, norm_gain):
    scaled = grad_out * norm_gain
    grad_in = inverse * (
        scaled
        - jnp.mean(scaled, axis=-1, keepdims=True)
        - normed * jnp.mean(scaled * normed, axis=-1, keepdims=True)
    )
    return (grad_in, jnp.sum(grad_out * normed, axis=0), jnp.sum(grad_out, axis=0))


def split_heads(rows, seq_count):
    return rows.reshape(seq_count, rows.shape[0] // seq_count, rows.shape[1] // HEAD, HEAD)


def masked_scores(query_heads, key_heads, segments):
    raw_scores = jnp.einsum(
        "rqhe,rkhe->rhqk", query_heads, key_heads, preferred_element_type=jnp.float32
    ) * HEAD ** (-0.5)
    allowed = segments[:, None, :, None] == segments[:, None, None, :]
    return (jnp.where(allowed, raw_scores, masked_value), allowed)


def attend_forward(queries, key_rows, value_rows, segments):
    seq_count = segments.shape[0]
    scores, _ = masked_scores(
        split_heads(queries, seq_count), split_heads(key_rows, seq_count), segments
    )
    largest = jnp.max(scores, axis=-1, keepdims=True)
    exponent = jnp.exp(scores - largest)
    row_total = jnp.sum(exponent, axis=-1, keepdims=True)
    soft_low = (exponent / row_total).astype(jnp.bfloat16)
    context = jnp.einsum(
        "rhqk,rkhe->rqhe",
        soft_low,
        split_heads(value_rows, seq_count),
        preferred_element_type=jnp.float32,
    )
    context = context.reshape(queries.shape).astype(jnp.bfloat16)
    return (context, largest + jnp.log(row_total))


def attend_backward(queries, key_rows, value_rows, segments, log_total, grad_context):
    seq_count = segments.shape[0]
    query_heads = split_heads(queries, seq_count)
    key_heads = split_heads(key_rows, seq_count)
    value_heads = split_heads(value_rows, seq_count)
    grad_heads = split_heads(grad_context, seq_count)
    scores, allowed = masked_scores(query_heads, key_heads, segments)
    soft_probs = jnp.exp(scores - log_total)
    grad_values = jnp.einsum(
        "rhqk,rqhe->rkhe",
        soft_probs.astype(jnp.bfloat16),
        grad_heads,
        preferred_element_type=jnp.float32,
    )
    grad_soft = jnp.einsum(
        "rqhe,rkhe->rhqk", grad_heads, value_heads, preferred_element_type=jnp.float32
    )
    grad_scores = soft_probs * (grad_soft - jnp.sum(soft_probs * grad_soft, axis=-1, keepdims=True))
    grad_low = jnp.where(allowed, grad_scores, 0.0).astype(jnp.bfloat16)
    score_scale = HEAD ** (-0.5)
    grad_queries = (
        jnp.einsum("rhqk,rkhe->rqhe", grad_low, key_heads, preferred_element_type=jnp.float32)
        * score_scale
    )
    grad_keys = (
        jnp.einsum("rhqk,rqhe->rkhe", grad_low, query_heads, preferred_element_type=jnp.float32)
        * score_scale
    )
    full_shape = queries.shape
    return (
        grad_queries.reshape(full_shape).astype(jnp.bfloat16),
        grad_keys.reshape(full_shape).astype(jnp.bfloat16),
        grad_values.reshape(full_shape).astype(jnp.bfloat16),
    )


def body(
    inputs,
    segments,
    labels,
    qkv_weight,
    qv_bias,
    out_weight,
    out_bias,
    norm1_gain,
    norm1_bias,
    up_weight,
    up_bias,
    down_weight,
    down_bias,
    norm2_gain,
    norm2_bias,
    pool_weight,
    pool_bias,
    class_weight,
    class_bias,
    cotangent,
):
    share_rows = inputs.shape[0]
    seq_count, seq_length = segments.shape
    tensor_index = lax.axis_index("tensor")
    dp_index = lax.axis_index("dp")
    tensor_count = lax.axis_size("tensor")
    dp_count = lax.axis_size("dp")
    offset = tensor_index * share_rows

    gathered = lax.all_gather(inputs, "tensor", axis=0, tiled=True)
    group_rows = gathered.shape[0]
    projected = jnp.einsum("td,kde->kte", gathered, qkv_weight, preferred_element_type=jnp.float32)
    queries = (projected[0] + qv_bias[0]).astype(jnp.bfloat16)
    key_rows = projected[1].astype(jnp.bfloat16)
    value_rows = (projected[2] + qv_bias[1]).astype(jnp.bfloat16)
    local_width = queries.shape[1]

    out_weight_all = lax.all_gather(out_weight, "tensor", axis=0, tiled=False)
    context, log_totals = attend_forward(queries, key_rows, value_rows, segments)
    context_own = lax.all_to_all(
        context.reshape(tensor_count, share_rows, local_width), "tensor", 0, 0, tiled=False
    )
    attended = (
        jnp.einsum(
            "itc,icd->td", context_own, out_weight_all, preferred_element_type=jnp.float32
        )
        + out_bias
    )
    first_norm, normed_one, inverse_one = norm_forward(
        inputs.astype(jnp.float32) + attended, norm1_gain, norm1_bias
    )
    first_low = first_norm.astype(jnp.bfloat16)
    first_all = lax.all_gather(first_low, "tensor", axis=0, tiled=True)
    up_pre = jnp.dot(first_all, up_weight, preferred_element_type=jnp.float32) + up_bias
    gelu_exact = partial(jax.nn.gelu, approximate=False)
    active = gelu_exact(up_pre).astype(jnp.bfloat16)
    ffn_out = (
        lax.psum_scatter(
            jnp.dot(active, down_weight, preferred_element_type=jnp.float32).astype(jnp.bfloat16),
            "tensor",
            scatter_dimension=0,
            tiled=True,
        )
        .astype(jnp.float32)
        + down_bias
    )
    final_norm, normed_two, inverse_two = norm_forward(
        first_norm + ffn_out, norm2_gain, norm2_bias
    )

    positions = offset + jnp.arange(share_rows, dtype=jnp.int32)
    row_starts = jnp.arange(seq_count, dtype=jnp.int32) * seq_length
    selector = (row_starts[:, None] == positions[None, :]).astype(jnp.float32)
    owned = jnp.sum(selector, axis=1, keepdims=True)
    leading = jnp.dot(selector, final_norm, precision=lax.Precision.HIGHEST).astype(jnp.bfloat16)
    pooled = jnp.tanh(jnp.dot(leading, pool_weight, preferred_element_type=jnp.float32) + pool_bias)
    pooled_low = pooled.astype(jnp.bfloat16)
    logits = jnp.dot(pooled_low, class_weight, preferred_element_type=jnp.float32) + class_bias
    chosen = (
        labels[:, None] == jnp.arange(class_weight.shape[1], dtype=jnp.int32)[None, :]
    ).astype(jnp.float32)
    grad_logits = jnp.where(
        owned > 0, jax.nn.softmax(logits, axis=-1) - chosen, 0.0
    ).astype(jnp.bfloat16)
    grad_pre = (
        jnp.einsum("rc,dc->rd", grad_logits, class_weight, preferred_element_type=jnp.float32)
        * (1.0 - pooled * pooled)
    ).astype(jnp.bfloat16)
    grad_leading = jnp.einsum(
        "re,de->rd", grad_pre, pool_weight, preferred_element_type=jnp.float32
    )
    grad_final = cotangent.astype(jnp.float32) + jnp.einsum(
        "rt,rd->td", selector, grad_leading, precision=lax.Precision.HIGHEST
    )
    grad_second, norm2_gain_grad, norm2_bias_grad = norm_backward(
        grad_final, normed_two, inverse_two, norm2_gain
    )
    grad_fed = grad_second.astype(jnp.bfloat16)
    down_bias_grad = jnp.sum(grad_fed.astype(jnp.float32), axis=0)
    grad_fed_all = lax.all_gather(grad_fed, "tensor", axis=0, tiled=True)
    down_weight_grad_t = jnp.einsum(
        "td,tf->df", grad_fed_all, active, preferred_element_type=jnp.float32
    )
    grad_active = jnp.einsum(
        "td,fd->tf", grad_fed_all, down_weight, preferred_element_type=jnp.float32
    )
    grad_up = jax.vjp(gelu_exact, up_pre)[1](grad_active)[0].astype(jnp.bfloat16)
    up_bias_grad = jnp.sum(grad_up.astype(jnp.float32), axis=0)
    up_weight_grad = jnp.einsum("td,tf->df", first_all, grad_up, preferred_element_type=jnp.float32)
    grad_first = (
        lax.psum_scatter(
            jnp.einsum("tf,df->td", grad_up, up_weight, preferred_element_type=jnp.float32).astype(jnp.bfloat16),
            "tensor",
            scatter_dimension=0,
            tiled=True,
        )
        .astype(jnp.float32)
        + grad_second
    )
    grad_res, norm1_gain_grad, norm1_bias_grad = norm_backward(
        grad_first, normed_one, inverse_one, norm1_gain
    )
    grad_att = grad_res.astype(jnp.bfloat16)
    out_bias_grad = jnp.sum(grad_att.astype(jnp.float32), axis=0)

    def joined(parts):
        return jnp.concatenate([part.reshape(-1) for part in parts])

    def parted(flat, parts):
        pieces = []
        begin = 0
        for part in parts:
            pieces.append(flat[begin : begin + part.size].reshape(part.shape))
            begin += part.size
        return pieces

    model_width = grad_att.shape[1]
    classes = class_weight.shape[1]
    row_block = jnp.stack(
        [
            leading.astype(jnp.float32) * owned,
            grad_pre.astype(jnp.float32),
            pooled_low.astype(jnp.float32) * owned,
            jnp.pad(grad_logits.astype(jnp.float32), ((0, 0), (0, model_width - classes))),
        ],
        axis=1,
    )
    token_parts = [
        jnp.stack(
            [
                out_bias_grad,
                norm1_gain_grad,
                norm1_bias_grad,
                down_bias_grad,
                norm2_gain_grad,
                norm2_bias_grad,
            ]
        ),
        row_block,
    ]
    small_flat = joined(token_parts)
    small_round = lax.reduce_precision(small_flat, exponent_bits=8, mantissa_bits=7)
    small_high = small_round.astype(jnp.bfloat16)
    small_low = (small_flat - small_round).astype(jnp.bfloat16)
    small_rows = -(-2 * small_flat.size // model_width)
    small_rows += (-(share_rows + small_rows)) % 16
    small_pad = small_rows * model_width - 2 * small_flat.size
    riding = jnp.concatenate(
        [small_high, small_low, jnp.zeros((small_pad,), jnp.bfloat16)]
    ).reshape(small_rows, model_width)
    att_gathered = lax.all_gather(
        jnp.concatenate([grad_att, riding], axis=0), "tensor", axis=0, tiled=False
    )
    grad_att_all = att_gathered[:, :share_rows].reshape(group_rows, model_width)
    small_back = att_gathered[:, share_rows:].reshape(tensor_count, -1)
    small_total = jnp.sum(
        small_back[:, : small_flat.size].astype(jnp.float32)
        + small_back[:, small_flat.size : 2 * small_flat.size].astype(jnp.float32),
        axis=0,
    )
    token_sum, rows_group = parted(small_total, token_parts)
    out_weight_grad_t = jnp.einsum(
        "td,te->de", grad_att_all, context, preferred_element_type=jnp.float32
    )
    grad_context = jnp.einsum(
        "td,ed->te", grad_att_all, out_weight, preferred_element_type=jnp.float32
    ).astype(jnp.bfloat16)
    grad_queries, grad_keys, grad_values = attend_backward(
        queries, key_rows, value_rows, segments, log_totals, grad_context
    )
    stacked = jnp.stack([grad_queries, grad_keys, grad_values])
    qkv_weight_grad = jnp.einsum(
        "td,tq->dq",
        gathered,
        jnp.concatenate([grad_queries, grad_keys, grad_values], axis=1),
        preferred_element_type=jnp.float32,
    )
    qv_bias_grad = jnp.stack(
        [
            jnp.sum(grad_queries.astype(jnp.float32), axis=0),
            jnp.sum(grad_values.astype(jnp.float32), axis=0),
        ]
    )
    input_grad = (
        lax.psum_scatter(
            jnp.einsum(
                "kte,kde->td", stacked, qkv_weight, preferred_element_type=jnp.float32
            ).astype(jnp.bfloat16),
            "tensor",
            scatter_dimension=0,
            tiled=True,
        ).astype(jnp.float32)
        + grad_res
    ).astype(jnp.bfloat16)

    def stacked_sum(parts, dtype):
        padded = [
            jnp.pad(part.astype(dtype), ((0, 0), (0, (-part.shape[1]) % 16), (0, 0)))
            for part in parts
        ]
        flat = jnp.concatenate(padded, axis=1)
        lanes = flat.shape[2]
        summed = lax.psum_scatter(
            flat.reshape(-1, lanes), "dp", scatter_dimension=0, tiled=True
        )
        pieces = []
        begin = 0
        for part, held in zip(parts, padded):
            pieces.append(summed[begin : begin + part.shape[1]])
            begin += held.shape[1]
        return pieces

    def in_blocks(grad):
        return grad.reshape(dp_count, grad.shape[0] // dp_count, grad.shape[1])

    def copied(flat, lanes):
        rows = -(-flat.size // lanes)
        flat = jnp.pad(flat, (0, rows * lanes - flat.size)).reshape(1, rows, lanes)
        return jnp.broadcast_to(flat, (dp_count, rows, lanes))

    copied_rows = dp_count * dp_count * rows_group.size <= (1 << 20)
    out_blocks = in_blocks(out_weight_grad_t).reshape(dp_count, -1, model_width)
    early_shared = [token_sum, up_bias_grad]
    early_parts = [
        in_blocks(up_weight_grad),
        in_blocks(down_weight_grad_t),
        out_blocks,
        copied(joined(early_shared), model_width),
    ]
    if copied_rows:
        rows_slotted = lax.dynamic_update_slice(
            jnp.zeros((dp_count,) + rows_group.shape, rows_group.dtype),
            rows_group[None],
            (dp_index, 0, 0, 0),
        )
        early_parts.append(copied(rows_slotted.reshape(-1), model_width))
    else:
        rows_each = lax.all_gather(rows_group.astype(jnp.bfloat16), "dp", axis=0, tiled=False)
    early_sums = stacked_sum(early_parts, jnp.bfloat16)
    up_sum = early_sums[0].astype(jnp.float32)
    down_sum = early_sums[1].astype(jnp.float32).T
    out_sum = early_sums[2].reshape(-1, out_weight_grad_t.shape[1]).astype(jnp.float32).T
    token_grads, up_bias_total = parted(
        early_sums[3].reshape(-1).astype(jnp.float32), early_shared
    )
    if copied_rows:
        rows_each = early_sums[4].reshape(-1)[: rows_slotted.size]
    late_shared = [qv_bias_grad]
    qkv_lanes = qkv_weight_grad.shape[1]
    late_parts = [in_blocks(qkv_weight_grad), copied(joined(late_shared), qkv_lanes)]
    late_received = lax.all_to_all(
        jnp.concatenate(late_parts, axis=1), "dp", 0, 0, tiled=False
    )
    late_total = jnp.sum(late_received, axis=0)
    late_sums = [late_total[: late_parts[0].shape[1]], late_total[late_parts[0].shape[1] :]]
    qkv_sum = jnp.transpose(
        late_sums[0].reshape(late_sums[0].shape[0], 3, qkv_lanes // 3), (1, 0, 2)
    ).astype(jnp.float32)
    (qv_bias_total,) = parted(late_sums[1].reshape(-1).astype(jnp.float32), late_shared)
    rows_all = rows_each.reshape(dp_count * seq_count, 4, model_width).astype(jnp.bfloat16)
    leading_all = rows_all[:, 0]
    grad_pre_all = rows_all[:, 1]
    pooled_all = rows_all[:, 2]
    grad_logits_all = rows_all[:, 3, :classes]
    pool_weight_grad = jnp.einsum(
        "rd,re->de", leading_all, grad_pre_all, preferred_element_type=jnp.float32
    )
    pool_bias_grad = jnp.sum(grad_pre_all.astype(jnp.float32), axis=0)
    class_weight_grad = jnp.einsum(
        "rd,rc->dc", pooled_all, grad_logits_all, preferred_element_type=jnp.float32
    )
    class_bias_grad = jnp.sum(grad_logits_all.astype(jnp.float32), axis=0)

    return (
        final_norm.astype(jnp.bfloat16),
        input_grad,
        qkv_sum,
        qv_bias_total,
        out_sum,
        token_grads[0],
        token_grads[1],
        token_grads[2],
        up_sum,
        up_bias_total,
        down_sum,
        token_grads[3],
        token_grads[4],
        token_grads[5],
        pool_weight_grad,
        pool_bias_grad,
        class_weight_grad,
        class_bias_grad,
    )


def solution(mesh):
    placed = (
        P(("dp", "tensor"), None),
        P("dp", None),
        P("dp"),
        P(None, None, "tensor"),
        P(None, "tensor"),
        P("tensor", None),
        P(),
        P(),
        P(),
        P(None, "tensor"),
        P("tensor"),
        P("tensor", None),
        P(),
        P(),
        P(),
        P(),
        P(),
        P(),
        P(),
        P(("dp", "tensor"), None),
    )
    return jax.shard_map(
        body,
        mesh=mesh,
        in_specs=placed,
        out_specs=(
            P(("dp", "tensor"), None),
            P(("dp", "tensor"), None),
            P(None, "dp", "tensor"),
            P(None, "tensor"),
            P("tensor", "dp"),
            P(),
            P(),
            P(),
            P("dp", "tensor"),
            P("tensor"),
            P("tensor", "dp"),
            P(),
            P(),
            P(),
            P(),
            P(),
            P(),
            P(),
        ),
        check_vma=False,
    )
```

```python
from functools import partial

import jax
import jax.numpy as jnp
from jax import lax
from jax.sharding import PartitionSpec as P


HEAD = 64


epsilon = 1e-12
masked_value = -1e30


def norm_forward(values, norm_gain, norm_shift):
    centre = values - jnp.mean(values, axis=-1, keepdims=True)
    inverse = lax.rsqrt(jnp.mean(centre * centre, axis=-1, keepdims=True) + epsilon)
    normed = centre * inverse
    return (normed * norm_gain + norm_shift, normed, inverse)


def norm_backward(grad_out, normed, inverse, norm_gain):
    scaled = grad_out * norm_gain
    grad_in = inverse * (
        scaled
        - jnp.mean(scaled, axis=-1, keepdims=True)
        - normed * jnp.mean(scaled * normed, axis=-1, keepdims=True)
    )
    return (grad_in, jnp.sum(grad_out * normed, axis=0), jnp.sum(grad_out, axis=0))


def split_heads(rows, seq_count):
    return rows.reshape(seq_count, rows.shape[0] // seq_count, rows.shape[1] // HEAD, HEAD)


def masked_scores(query_heads, key_heads, segments):
    raw_scores = jnp.einsum(
        "rqhe,rkhe->rhqk", query_heads, key_heads, preferred_element_type=jnp.float32
    ) * HEAD ** (-0.5)
    allowed = segments[:, None, :, None] == segments[:, None, None, :]
    return (jnp.where(allowed, raw_scores, masked_value), allowed)


def attend_forward(queries, key_rows, value_rows, segments):
    seq_count = segments.shape[0]
    scores, _ = masked_scores(
        split_heads(queries, seq_count), split_heads(key_rows, seq_count), segments
    )
    largest = jnp.max(scores, axis=-1, keepdims=True)
    exponent = jnp.exp(scores - largest)
    row_total = jnp.sum(exponent, axis=-1, keepdims=True)
    soft_low = (exponent / row_total).astype(jnp.bfloat16)
    context = jnp.einsum(
        "rhqk,rkhe->rqhe",
        soft_low,
        split_heads(value_rows, seq_count),
        preferred_element_type=jnp.float32,
    )
    context = context.reshape(queries.shape).astype(jnp.bfloat16)
    return (context, largest + jnp.log(row_total))


def attend_backward(queries, key_rows, value_rows, segments, log_total, grad_context):
    seq_count = segments.shape[0]
    query_heads = split_heads(queries, seq_count)
    key_heads = split_heads(key_rows, seq_count)
    value_heads = split_heads(value_rows, seq_count)
    grad_heads = split_heads(grad_context, seq_count)
    scores, allowed = masked_scores(query_heads, key_heads, segments)
    soft_probs = jnp.exp(scores - log_total)
    grad_values = jnp.einsum(
        "rhqk,rqhe->rkhe",
        soft_probs.astype(jnp.bfloat16),
        grad_heads,
        preferred_element_type=jnp.float32,
    )
    grad_soft = jnp.einsum(
        "rqhe,rkhe->rhqk", grad_heads, value_heads, preferred_element_type=jnp.float32
    )
    grad_scores = soft_probs * (grad_soft - jnp.sum(soft_probs * grad_soft, axis=-1, keepdims=True))
    grad_low = lax.optimization_barrier(jnp.where(allowed, grad_scores, 0.0).astype(jnp.bfloat16))
    score_scale = HEAD ** (-0.5)
    grad_queries = (
        jnp.einsum("rhqk,rkhe->rqhe", grad_low, key_heads, preferred_element_type=jnp.float32)
        * score_scale
    )
    grad_keys = (
        jnp.einsum("rhqk,rqhe->rkhe", grad_low, query_heads, preferred_element_type=jnp.float32)
        * score_scale
    )
    full_shape = queries.shape
    return (
        grad_queries.reshape(full_shape).astype(jnp.bfloat16),
        grad_keys.reshape(full_shape).astype(jnp.bfloat16),
        grad_values.reshape(full_shape).astype(jnp.bfloat16),
    )


def body(
    inputs,
    segments,
    labels,
    qkv_weight,
    qv_bias,
    out_weight,
    out_bias,
    norm1_gain,
    norm1_bias,
    up_weight,
    up_bias,
    down_weight,
    down_bias,
    norm2_gain,
    norm2_bias,
    pool_weight,
    pool_bias,
    class_weight,
    class_bias,
    cotangent,
):
    share_rows = inputs.shape[0]
    seq_count, seq_length = segments.shape
    tensor_index = lax.axis_index("tensor")
    dp_index = lax.axis_index("dp")
    tensor_count = lax.axis_size("tensor")
    dp_count = lax.axis_size("dp")
    offset = tensor_index * share_rows

    gathered = lax.all_gather(inputs, "tensor", axis=0, tiled=True)
    group_rows = gathered.shape[0]

    def project(which):
        return jnp.dot(gathered, qkv_weight[which], preferred_element_type=jnp.float32)

    queries = (project(0) + qv_bias[0]).astype(jnp.bfloat16)
    key_rows = project(1).astype(jnp.bfloat16)
    value_rows = (project(2) + qv_bias[1]).astype(jnp.bfloat16)
    local_width = queries.shape[1]

    out_weight_all = lax.all_gather(out_weight, "tensor", axis=0, tiled=False)
    context, log_totals = attend_forward(queries, key_rows, value_rows, segments)
    context_own = lax.all_to_all(
        context.reshape(tensor_count, share_rows, local_width), "tensor", 0, 0, tiled=False
    )
    attended = (
        jnp.einsum(
            "itc,icd->td", context_own, out_weight_all, preferred_element_type=jnp.float32
        )
        + out_bias
    )
    first_norm, normed_one, inverse_one = norm_forward(
        inputs.astype(jnp.float32) + attended, norm1_gain, norm1_bias
    )
    first_low = first_norm.astype(jnp.bfloat16)
    first_all = lax.all_gather(first_low, "tensor", axis=0, tiled=True)
    up_pre = jnp.dot(first_all, up_weight, preferred_element_type=jnp.float32) + up_bias
    gelu_exact = partial(jax.nn.gelu, approximate=False)
    active = gelu_exact(up_pre).astype(jnp.bfloat16)
    ffn_out = (
        lax.psum_scatter(
            jnp.dot(active, down_weight, preferred_element_type=jnp.float32).astype(jnp.bfloat16),
            "tensor",
            scatter_dimension=0,
            tiled=True,
        )
        .astype(jnp.float32)
        + down_bias
    )
    final_norm, normed_two, inverse_two = norm_forward(
        first_norm + ffn_out, norm2_gain, norm2_bias
    )

    positions = offset + jnp.arange(share_rows, dtype=jnp.int32)
    row_starts = jnp.arange(seq_count, dtype=jnp.int32) * seq_length
    selector = (row_starts[:, None] == positions[None, :]).astype(jnp.float32)
    owned = jnp.sum(selector, axis=1, keepdims=True)
    leading = jnp.dot(selector, final_norm, precision=lax.Precision.HIGHEST).astype(jnp.bfloat16)
    pooled = jnp.tanh(jnp.dot(leading, pool_weight, preferred_element_type=jnp.float32) + pool_bias)
    pooled_low = pooled.astype(jnp.bfloat16)
    logits = jnp.dot(pooled_low, class_weight, preferred_element_type=jnp.float32) + class_bias
    chosen = (
        labels[:, None] == jnp.arange(class_weight.shape[1], dtype=jnp.int32)[None, :]
    ).astype(jnp.float32)
    grad_logits = jnp.where(
        owned > 0, jax.nn.softmax(logits, axis=-1) - chosen, 0.0
    ).astype(jnp.bfloat16)
    grad_pre = (
        jnp.einsum("rc,dc->rd", grad_logits, class_weight, preferred_element_type=jnp.float32)
        * (1.0 - pooled * pooled)
    ).astype(jnp.bfloat16)
    grad_leading = jnp.einsum(
        "re,de->rd", grad_pre, pool_weight, preferred_element_type=jnp.float32
    )
    grad_final = cotangent.astype(jnp.float32) + jnp.einsum(
        "rt,rd->td", selector, grad_leading, precision=lax.Precision.HIGHEST
    )
    grad_second, norm2_gain_grad, norm2_bias_grad = norm_backward(
        grad_final, normed_two, inverse_two, norm2_gain
    )
    grad_fed = grad_second.astype(jnp.bfloat16)
    down_bias_grad = jnp.sum(grad_fed.astype(jnp.float32), axis=0)
    grad_fed_all = lax.all_gather(grad_fed, "tensor", axis=0, tiled=True)
    down_weight_grad_t = jnp.einsum(
        "td,tf->df", grad_fed_all, active, preferred_element_type=jnp.float32
    )
    grad_active = jnp.einsum(
        "td,fd->tf", grad_fed_all, down_weight, preferred_element_type=jnp.float32
    )
    grad_up = jax.vjp(gelu_exact, up_pre)[1](grad_active)[0].astype(jnp.bfloat16)
    up_bias_grad = jnp.sum(grad_up.astype(jnp.float32), axis=0)
    up_weight_grad = jnp.einsum("td,tf->df", first_all, grad_up, preferred_element_type=jnp.float32)
    grad_first = (
        lax.psum_scatter(
            jnp.einsum("tf,df->td", grad_up, up_weight, preferred_element_type=jnp.float32).astype(jnp.bfloat16),
            "tensor",
            scatter_dimension=0,
            tiled=True,
        )
        .astype(jnp.float32)
        + grad_second
    )
    grad_res, norm1_gain_grad, norm1_bias_grad = norm_backward(
        grad_first, normed_one, inverse_one, norm1_gain
    )
    grad_att = grad_res.astype(jnp.bfloat16)
    out_bias_grad = jnp.sum(grad_att.astype(jnp.float32), axis=0)

    def joined(parts):
        return jnp.concatenate([part.reshape(-1) for part in parts])

    def parted(flat, parts):
        pieces = []
        begin = 0
        for part in parts:
            pieces.append(flat[begin : begin + part.size].reshape(part.shape))
            begin += part.size
        return pieces

    model_width = grad_att.shape[1]
    classes = class_weight.shape[1]
    row_block = jnp.stack(
        [
            leading.astype(jnp.float32) * owned,
            grad_pre.astype(jnp.float32),
            pooled_low.astype(jnp.float32) * owned,
            jnp.pad(grad_logits.astype(jnp.float32), ((0, 0), (0, model_width - classes))),
        ],
        axis=1,
    )
    token_parts = [
        jnp.stack(
            [
                out_bias_grad,
                norm1_gain_grad,
                norm1_bias_grad,
                down_bias_grad,
                norm2_gain_grad,
                norm2_bias_grad,
            ]
        ),
        row_block,
    ]
    small_flat = token_parts[0].reshape(-1)
    small_round = lax.reduce_precision(small_flat, exponent_bits=8, mantissa_bits=7)
    small_high = small_round.astype(jnp.bfloat16)
    small_low = (small_flat - small_round).astype(jnp.bfloat16)
    rows_low = row_block.reshape(-1).astype(jnp.bfloat16)
    riding_size = 2 * small_flat.size + rows_low.size
    small_rows = -(-riding_size // model_width)
    small_rows += (-(share_rows + small_rows)) % 16
    small_pad = small_rows * model_width - riding_size
    riding = jnp.concatenate(
        [small_high, small_low, rows_low, jnp.zeros((small_pad,), jnp.bfloat16)]
    ).reshape(small_rows, model_width)
    att_gathered = lax.all_gather(
        jnp.concatenate([grad_att, riding], axis=0), "tensor", axis=0, tiled=False
    )
    grad_att_all = att_gathered[:, :share_rows].reshape(group_rows, model_width)
    small_back = att_gathered[:, share_rows:].reshape(tensor_count, -1).astype(jnp.float32)
    token_size = small_flat.size
    token_sum = jnp.sum(
        small_back[:, :token_size] + small_back[:, token_size : 2 * token_size], axis=0
    ).reshape(token_parts[0].shape)
    rows_group = jnp.sum(
        small_back[:, 2 * token_size : 2 * token_size + rows_low.size], axis=0
    ).reshape(row_block.shape)
    out_weight_grad_t = jnp.einsum(
        "td,te->de", grad_att_all, context, preferred_element_type=jnp.float32
    )
    grad_context = jnp.einsum(
        "td,ed->te", grad_att_all, out_weight, preferred_element_type=jnp.float32
    ).astype(jnp.bfloat16)
    grad_queries, grad_keys, grad_values = attend_backward(
        queries, key_rows, value_rows, segments, log_totals, grad_context
    )
    stacked = jnp.stack([grad_queries, grad_keys, grad_values])
    qkv_weight_grad = jnp.einsum(
        "td,tq->dq",
        gathered,
        jnp.concatenate([grad_queries, grad_keys, grad_values], axis=1),
        preferred_element_type=jnp.float32,
    )
    qv_bias_grad = jnp.stack(
        [
            jnp.sum(grad_queries.astype(jnp.float32), axis=0),
            jnp.sum(grad_values.astype(jnp.float32), axis=0),
        ]
    )
    input_grad = (
        lax.psum_scatter(
            jnp.einsum(
                "kte,kde->td", stacked, qkv_weight, preferred_element_type=jnp.float32
            ).astype(jnp.bfloat16),
            "tensor",
            scatter_dimension=0,
            tiled=True,
        ).astype(jnp.float32)
        + grad_res
    ).astype(jnp.bfloat16)

    def stacked_sum(parts, dtype):
        padded = [
            jnp.pad(part.astype(dtype), ((0, 0), (0, (-part.shape[1]) % 16), (0, 0)))
            for part in parts
        ]
        flat = jnp.concatenate(padded, axis=1)
        lanes = flat.shape[2]
        summed = lax.psum_scatter(
            flat.reshape(-1, lanes), "dp", scatter_dimension=0, tiled=True
        )
        pieces = []
        begin = 0
        for part, held in zip(parts, padded):
            pieces.append(summed[begin : begin + part.shape[1]])
            begin += held.shape[1]
        return pieces

    def in_blocks(grad):
        return grad.reshape(dp_count, grad.shape[0] // dp_count, grad.shape[1])

    def copied(flat, lanes):
        rows = -(-flat.size // lanes)
        flat = jnp.pad(flat, (0, rows * lanes - flat.size)).reshape(1, rows, lanes)
        return jnp.broadcast_to(flat, (dp_count, rows, lanes))

    copied_rows = dp_count * dp_count * rows_group.size <= (1 << 20)
    out_blocks = in_blocks(out_weight_grad_t).reshape(dp_count, -1, model_width)
    early_shared = [token_sum, up_bias_grad]
    early_parts = [
        in_blocks(up_weight_grad),
        in_blocks(down_weight_grad_t),
        out_blocks,
        copied(joined(early_shared), model_width),
    ]
    if copied_rows:
        rows_slotted = lax.dynamic_update_slice(
            jnp.zeros((dp_count,) + rows_group.shape, rows_group.dtype),
            rows_group[None],
            (dp_index, 0, 0, 0),
        )
        early_parts.append(copied(rows_slotted.reshape(-1), model_width))
    else:
        rows_each = lax.all_gather(rows_group.astype(jnp.bfloat16), "dp", axis=0, tiled=False)
    early_sums = stacked_sum(early_parts, jnp.bfloat16)
    up_sum = early_sums[0].astype(jnp.float32)
    down_sum = early_sums[1].astype(jnp.float32).T
    out_sum = early_sums[2].reshape(-1, out_weight_grad_t.shape[1]).astype(jnp.float32).T
    token_grads, up_bias_total = parted(
        early_sums[3].reshape(-1).astype(jnp.float32), early_shared
    )
    if copied_rows:
        rows_each = early_sums[4].reshape(-1)[: rows_slotted.size]
    late_shared = [qv_bias_grad]
    qkv_lanes = qkv_weight_grad.shape[1]
    late_parts = [in_blocks(qkv_weight_grad), copied(joined(late_shared), qkv_lanes)]
    late_received = lax.all_to_all(
        jnp.concatenate(late_parts, axis=1), "dp", 0, 0, tiled=False
    )
    late_total = jnp.sum(late_received, axis=0)
    late_sums = [late_total[: late_parts[0].shape[1]], late_total[late_parts[0].shape[1] :]]
    qkv_sum = jnp.transpose(
        late_sums[0].reshape(late_sums[0].shape[0], 3, qkv_lanes // 3), (1, 0, 2)
    ).astype(jnp.float32)
    (qv_bias_total,) = parted(late_sums[1].reshape(-1).astype(jnp.float32), late_shared)
    rows_all = rows_each.reshape(dp_count * seq_count, 4, model_width).astype(jnp.bfloat16)
    leading_all = rows_all[:, 0]
    grad_pre_all = rows_all[:, 1]
    pooled_all = rows_all[:, 2]
    grad_logits_all = rows_all[:, 3, :classes]
    pool_weight_grad = jnp.einsum(
        "rd,re->de", leading_all, grad_pre_all, preferred_element_type=jnp.float32
    )
    pool_bias_grad = jnp.sum(grad_pre_all.astype(jnp.float32), axis=0)
    class_weight_grad = jnp.einsum(
        "rd,rc->dc", pooled_all, grad_logits_all, preferred_element_type=jnp.float32
    )
    class_bias_grad = jnp.sum(grad_logits_all.astype(jnp.float32), axis=0)

    return (
        final_norm.astype(jnp.bfloat16),
        input_grad,
        qkv_sum,
        qv_bias_total,
        out_sum,
        token_grads[0],
        token_grads[1],
        token_grads[2],
        up_sum,
        up_bias_total,
        down_sum,
        token_grads[3],
        token_grads[4],
        token_grads[5],
        pool_weight_grad,
        pool_bias_grad,
        class_weight_grad,
        class_bias_grad,
    )


def solution(mesh):
    placed = (
        P(("dp", "tensor"), None),
        P("dp", None),
        P("dp"),
        P(None, None, "tensor"),
        P(None, "tensor"),
        P("tensor", None),
        P(),
        P(),
        P(),
        P(None, "tensor"),
        P("tensor"),
        P("tensor", None),
        P(),
        P(),
        P(),
        P(),
        P(),
        P(),
        P(),
        P(("dp", "tensor"), None),
    )
    return jax.shard_map(
        body,
        mesh=mesh,
        in_specs=placed,
        out_specs=(
            P(("dp", "tensor"), None),
            P(("dp", "tensor"), None),
            P(None, "dp", "tensor"),
            P(None, "tensor"),
            P("tensor", "dp"),
            P(),
            P(),
            P(),
            P("dp", "tensor"),
            P("tensor"),
            P("tensor", "dp"),
            P(),
            P(),
            P(),
            P(),
            P(),
            P(),
            P(),
        ),
        check_vma=False,
    )
```

```python
from functools import partial

import jax
import jax.numpy as jnp
from jax import lax
from jax.sharding import PartitionSpec as P


HEAD = 64


epsilon = 1e-12
masked_value = -1e30


def norm_forward(values, norm_gain, norm_shift):
    centre = values - jnp.mean(values, axis=-1, keepdims=True)
    inverse = lax.rsqrt(jnp.mean(centre * centre, axis=-1, keepdims=True) + epsilon)
    normed = centre * inverse
    return (normed * norm_gain + norm_shift, normed, inverse)


def norm_backward(grad_out, normed, inverse, norm_gain):
    scaled = grad_out * norm_gain
    grad_in = inverse * (
        scaled
        - jnp.mean(scaled, axis=-1, keepdims=True)
        - normed * jnp.mean(scaled * normed, axis=-1, keepdims=True)
    )
    return (grad_in, jnp.sum(grad_out * normed, axis=0), jnp.sum(grad_out, axis=0))


def split_heads(rows, seq_count):
    return rows.reshape(seq_count, rows.shape[0] // seq_count, rows.shape[1] // HEAD, HEAD)


def masked_scores(query_heads, key_heads, segments):
    raw_scores = jnp.einsum(
        "rqhe,rkhe->rhqk", query_heads, key_heads, preferred_element_type=jnp.float32
    ) * HEAD ** (-0.5)
    allowed = segments[:, None, :, None] == segments[:, None, None, :]
    return (jnp.where(allowed, raw_scores, masked_value), allowed)


def attend_forward(queries, key_rows, value_rows, segments):
    seq_count = segments.shape[0]
    scores, _ = masked_scores(
        split_heads(queries, seq_count), split_heads(key_rows, seq_count), segments
    )
    largest = jnp.max(scores, axis=-1, keepdims=True)
    exponent = jnp.exp(scores - largest)
    row_total = jnp.sum(exponent, axis=-1, keepdims=True)
    soft_low = (exponent / row_total).astype(jnp.bfloat16)
    context = jnp.einsum(
        "rhqk,rkhe->rqhe",
        soft_low,
        split_heads(value_rows, seq_count),
        preferred_element_type=jnp.float32,
    )
    context = context.reshape(queries.shape).astype(jnp.bfloat16)
    return (context, largest + jnp.log(row_total))


def attend_backward(queries, key_rows, value_rows, segments, log_total, grad_context):
    seq_count = segments.shape[0]
    query_heads = split_heads(queries, seq_count)
    key_heads = split_heads(key_rows, seq_count)
    value_heads = split_heads(value_rows, seq_count)
    grad_heads = split_heads(grad_context, seq_count)
    scores, allowed = masked_scores(query_heads, key_heads, segments)
    soft_probs = jnp.exp(scores - log_total)
    grad_values = jnp.einsum(
        "rhqk,rqhe->rkhe",
        soft_probs.astype(jnp.bfloat16),
        grad_heads,
        preferred_element_type=jnp.float32,
    )
    grad_soft = jnp.einsum(
        "rqhe,rkhe->rhqk", grad_heads, value_heads, preferred_element_type=jnp.float32
    )
    grad_scores = soft_probs * (grad_soft - jnp.sum(soft_probs * grad_soft, axis=-1, keepdims=True))
    grad_low = lax.optimization_barrier(jnp.where(allowed, grad_scores, 0.0).astype(jnp.bfloat16))
    score_scale = HEAD ** (-0.5)
    grad_queries = (
        jnp.einsum("rhqk,rkhe->rqhe", grad_low, key_heads, preferred_element_type=jnp.float32)
        * score_scale
    )
    grad_keys = (
        jnp.einsum("rhqk,rqhe->rkhe", grad_low, query_heads, preferred_element_type=jnp.float32)
        * score_scale
    )
    full_shape = queries.shape
    return (
        grad_queries.reshape(full_shape).astype(jnp.bfloat16),
        grad_keys.reshape(full_shape).astype(jnp.bfloat16),
        grad_values.reshape(full_shape).astype(jnp.bfloat16),
    )


def body(
    inputs,
    segments,
    labels,
    qkv_weight,
    qv_bias,
    out_weight,
    out_bias,
    norm1_gain,
    norm1_bias,
    up_weight,
    up_bias,
    down_weight,
    down_bias,
    norm2_gain,
    norm2_bias,
    pool_weight,
    pool_bias,
    class_weight,
    class_bias,
    cotangent,
):
    share_rows = inputs.shape[0]
    seq_count, seq_length = segments.shape
    tensor_index = lax.axis_index("tensor")
    tensor_count = lax.axis_size("tensor")
    dp_count = lax.axis_size("dp")
    offset = tensor_index * share_rows

    gathered = lax.all_gather(inputs, "tensor", axis=0, tiled=True)
    group_rows = gathered.shape[0]

    def project(which):
        return jnp.dot(gathered, qkv_weight[which], preferred_element_type=jnp.float32)

    queries = (project(0) + qv_bias[0]).astype(jnp.bfloat16)
    key_rows = project(1).astype(jnp.bfloat16)
    value_rows = (project(2) + qv_bias[1]).astype(jnp.bfloat16)
    local_width = queries.shape[1]

    out_weight_all = lax.all_gather(out_weight, "tensor", axis=0, tiled=False)
    context, log_totals = attend_forward(queries, key_rows, value_rows, segments)
    context_own = lax.all_to_all(
        context.reshape(tensor_count, share_rows, local_width), "tensor", 0, 0, tiled=False
    )
    attended = (
        jnp.einsum(
            "itc,icd->td", context_own, out_weight_all, preferred_element_type=jnp.float32
        )
        + out_bias
    )
    first_norm, normed_one, inverse_one = norm_forward(
        inputs.astype(jnp.float32) + attended, norm1_gain, norm1_bias
    )
    first_low = first_norm.astype(jnp.bfloat16)
    first_all = lax.all_gather(first_low, "tensor", axis=0, tiled=True)
    up_pre = jnp.dot(first_all, up_weight, preferred_element_type=jnp.float32) + up_bias
    gelu_exact = partial(jax.nn.gelu, approximate=False)
    active = gelu_exact(up_pre).astype(jnp.bfloat16)
    ffn_out = (
        lax.psum_scatter(
            jnp.dot(active, down_weight, preferred_element_type=jnp.float32).astype(jnp.bfloat16),
            "tensor",
            scatter_dimension=0,
            tiled=True,
        )
        .astype(jnp.float32)
        + down_bias
    )
    final_norm, normed_two, inverse_two = norm_forward(
        first_norm + ffn_out, norm2_gain, norm2_bias
    )

    positions = offset + jnp.arange(share_rows, dtype=jnp.int32)
    row_starts = jnp.arange(seq_count, dtype=jnp.int32) * seq_length
    selector = (row_starts[:, None] == positions[None, :]).astype(jnp.float32)
    owned = jnp.sum(selector, axis=1, keepdims=True)
    leading = jnp.dot(selector, final_norm, precision=lax.Precision.HIGHEST).astype(jnp.bfloat16)
    pooled = jnp.tanh(jnp.dot(leading, pool_weight, preferred_element_type=jnp.float32) + pool_bias)
    pooled_low = pooled.astype(jnp.bfloat16)
    logits = jnp.dot(pooled_low, class_weight, preferred_element_type=jnp.float32) + class_bias
    chosen = (
        labels[:, None] == jnp.arange(class_weight.shape[1], dtype=jnp.int32)[None, :]
    ).astype(jnp.float32)
    grad_logits = jnp.where(
        owned > 0, jax.nn.softmax(logits, axis=-1) - chosen, 0.0
    ).astype(jnp.bfloat16)
    grad_pre = (
        jnp.einsum("rc,dc->rd", grad_logits, class_weight, preferred_element_type=jnp.float32)
        * (1.0 - pooled * pooled)
    ).astype(jnp.bfloat16)
    grad_leading = jnp.einsum(
        "re,de->rd", grad_pre, pool_weight, preferred_element_type=jnp.float32
    )
    grad_final = cotangent.astype(jnp.float32) + jnp.einsum(
        "rt,rd->td", selector, grad_leading, precision=lax.Precision.HIGHEST
    )
    grad_second, norm2_gain_grad, norm2_bias_grad = norm_backward(
        grad_final, normed_two, inverse_two, norm2_gain
    )
    grad_fed = grad_second.astype(jnp.bfloat16)
    down_bias_grad = jnp.sum(grad_fed.astype(jnp.float32), axis=0)
    grad_fed_all = lax.all_gather(grad_fed, "tensor", axis=0, tiled=True)
    down_weight_grad_t = jnp.einsum(
        "td,tf->df", grad_fed_all, active, preferred_element_type=jnp.float32
    )
    grad_active = jnp.einsum(
        "td,fd->tf", grad_fed_all, down_weight, preferred_element_type=jnp.float32
    )
    grad_up = jax.vjp(gelu_exact, up_pre)[1](grad_active)[0].astype(jnp.bfloat16)
    up_bias_grad = jnp.sum(grad_up.astype(jnp.float32), axis=0)
    up_weight_grad = jnp.einsum("td,tf->df", first_all, grad_up, preferred_element_type=jnp.float32)
    grad_first = (
        lax.psum_scatter(
            jnp.einsum("tf,df->td", grad_up, up_weight, preferred_element_type=jnp.float32).astype(jnp.bfloat16),
            "tensor",
            scatter_dimension=0,
            tiled=True,
        )
        .astype(jnp.float32)
        + grad_second
    )
    grad_res, norm1_gain_grad, norm1_bias_grad = norm_backward(
        grad_first, normed_one, inverse_one, norm1_gain
    )
    grad_att = grad_res.astype(jnp.bfloat16)
    out_bias_grad = jnp.sum(grad_att.astype(jnp.float32), axis=0)

    def joined(parts):
        return jnp.concatenate([part.reshape(-1) for part in parts])

    def parted(flat, parts):
        pieces = []
        begin = 0
        for part in parts:
            pieces.append(flat[begin : begin + part.size].reshape(part.shape))
            begin += part.size
        return pieces

    model_width = grad_att.shape[1]
    classes = class_weight.shape[1]
    row_block = jnp.stack(
        [
            leading.astype(jnp.float32) * owned,
            grad_pre.astype(jnp.float32),
            pooled_low.astype(jnp.float32) * owned,
            jnp.pad(grad_logits.astype(jnp.float32), ((0, 0), (0, model_width - classes))),
        ],
        axis=1,
    )
    token_parts = [
        jnp.stack(
            [
                out_bias_grad,
                norm1_gain_grad,
                norm1_bias_grad,
                down_bias_grad,
                norm2_gain_grad,
                norm2_bias_grad,
            ]
        ),
        row_block,
    ]
    small_flat = token_parts[0].reshape(-1)
    small_round = lax.reduce_precision(small_flat, exponent_bits=8, mantissa_bits=7)
    small_high = small_round.astype(jnp.bfloat16)
    small_low = (small_flat - small_round).astype(jnp.bfloat16)
    rows_low = row_block.reshape(-1).astype(jnp.bfloat16)
    riding_size = 2 * small_flat.size + rows_low.size
    small_rows = -(-riding_size // model_width)
    small_rows += (-(share_rows + small_rows)) % 16
    small_pad = small_rows * model_width - riding_size
    riding = jnp.concatenate(
        [small_high, small_low, rows_low, jnp.zeros((small_pad,), jnp.bfloat16)]
    ).reshape(small_rows, model_width)
    att_gathered = lax.all_gather(
        jnp.concatenate([grad_att, riding], axis=0), "tensor", axis=0, tiled=False
    )
    grad_att_all = att_gathered[:, :share_rows].reshape(group_rows, model_width)
    small_back = att_gathered[:, share_rows:].reshape(tensor_count, -1).astype(jnp.float32)
    token_size = small_flat.size
    token_sum = jnp.sum(
        small_back[:, :token_size] + small_back[:, token_size : 2 * token_size], axis=0
    ).reshape(token_parts[0].shape)
    rows_group = jnp.sum(
        small_back[:, 2 * token_size : 2 * token_size + rows_low.size], axis=0
    ).reshape(row_block.shape)
    out_weight_grad_t = jnp.einsum(
        "td,te->de", grad_att_all, context, preferred_element_type=jnp.float32
    )
    grad_context = jnp.einsum(
        "td,ed->te", grad_att_all, out_weight, preferred_element_type=jnp.float32
    ).astype(jnp.bfloat16)
    grad_queries, grad_keys, grad_values = attend_backward(
        queries, key_rows, value_rows, segments, log_totals, grad_context
    )
    stacked = jnp.stack([grad_queries, grad_keys, grad_values])
    qkv_weight_grad = jnp.einsum(
        "td,tq->dq",
        gathered,
        jnp.concatenate([grad_queries, grad_keys, grad_values], axis=1),
        preferred_element_type=jnp.float32,
    )
    qv_bias_grad = jnp.stack(
        [
            jnp.sum(grad_queries.astype(jnp.float32), axis=0),
            jnp.sum(grad_values.astype(jnp.float32), axis=0),
        ]
    )
    input_grad = (
        lax.psum_scatter(
            jnp.einsum(
                "kte,kde->td", stacked, qkv_weight, preferred_element_type=jnp.float32
            ).astype(jnp.bfloat16),
            "tensor",
            scatter_dimension=0,
            tiled=True,
        ).astype(jnp.float32)
        + grad_res
    ).astype(jnp.bfloat16)

    def stacked_sum(parts, dtype):
        padded = [
            jnp.pad(part.astype(dtype), ((0, 0), (0, (-part.shape[1]) % 16), (0, 0)))
            for part in parts
        ]
        flat = jnp.concatenate(padded, axis=1)
        lanes = flat.shape[2]
        summed = lax.psum_scatter(
            flat.reshape(-1, lanes), "dp", scatter_dimension=0, tiled=True
        )
        pieces = []
        begin = 0
        for part, held in zip(parts, padded):
            pieces.append(summed[begin : begin + part.shape[1]])
            begin += held.shape[1]
        return pieces

    def in_blocks(grad):
        return grad.reshape(dp_count, grad.shape[0] // dp_count, grad.shape[1])

    def copied(flat, lanes):
        rows = -(-flat.size // lanes)
        flat = jnp.pad(flat, (0, rows * lanes - flat.size)).reshape(1, rows, lanes)
        return jnp.broadcast_to(flat, (dp_count, rows, lanes))

    out_blocks = in_blocks(out_weight_grad_t).reshape(dp_count, -1, model_width)
    early_parts = [in_blocks(up_weight_grad), in_blocks(down_weight_grad_t), out_blocks]
    early_sums = stacked_sum(early_parts, jnp.bfloat16)
    up_sum = early_sums[0].astype(jnp.float32)
    down_sum = early_sums[1].astype(jnp.float32).T
    out_sum = early_sums[2].reshape(-1, out_weight_grad_t.shape[1]).astype(jnp.float32).T
    late_shared = [qv_bias_grad, token_sum, up_bias_grad]
    qkv_lanes = qkv_weight_grad.shape[1]

    def aligned(part):
        return jnp.pad(part, ((0, 0), (0, (-part.shape[1]) % 8), (0, 0)))

    late_parts = [
        aligned(in_blocks(qkv_weight_grad)),
        aligned(copied(joined(late_shared), qkv_lanes)),
        aligned(copied(rows_group.reshape(-1), qkv_lanes)),
    ]
    late_received = lax.all_to_all(
        jnp.concatenate(late_parts, axis=1), "dp", 0, 0, tiled=False
    )
    qkv_rows = in_blocks(qkv_weight_grad).shape[1]
    shared_begin = late_parts[0].shape[1]
    rows_begin = shared_begin + late_parts[1].shape[1]
    late_total = jnp.sum(late_received[:, :rows_begin], axis=0)
    qkv_sum = jnp.transpose(
        late_total[:qkv_rows].reshape(qkv_rows, 3, qkv_lanes // 3), (1, 0, 2)
    )
    qv_bias_total, token_grads, up_bias_total = parted(
        late_total[shared_begin:].reshape(-1), late_shared
    )
    rows_each = late_received[:, rows_begin:].reshape(dp_count, -1)[:, : rows_group.size]
    rows_all = rows_each.reshape(dp_count * seq_count, 4, model_width).astype(jnp.bfloat16)
    leading_all = rows_all[:, 0]
    grad_pre_all = rows_all[:, 1]
    pooled_all = rows_all[:, 2]
    grad_logits_all = rows_all[:, 3, :classes]
    pool_weight_grad = jnp.einsum(
        "rd,re->de", leading_all, grad_pre_all, preferred_element_type=jnp.float32
    )
    pool_bias_grad = jnp.sum(grad_pre_all.astype(jnp.float32), axis=0)
    class_weight_grad = jnp.einsum(
        "rd,rc->dc", pooled_all, grad_logits_all, preferred_element_type=jnp.float32
    )
    class_bias_grad = jnp.sum(grad_logits_all.astype(jnp.float32), axis=0)

    return (
        final_norm.astype(jnp.bfloat16),
        input_grad,
        qkv_sum,
        qv_bias_total,
        out_sum,
        token_grads[0],
        token_grads[1],
        token_grads[2],
        up_sum,
        up_bias_total,
        down_sum,
        token_grads[3],
        token_grads[4],
        token_grads[5],
        pool_weight_grad,
        pool_bias_grad,
        class_weight_grad,
        class_bias_grad,
    )


def solution(mesh):
    placed = (
        P(("dp", "tensor"), None),
        P("dp", None),
        P("dp"),
        P(None, None, "tensor"),
        P(None, "tensor"),
        P("tensor", None),
        P(),
        P(),
        P(),
        P(None, "tensor"),
        P("tensor"),
        P("tensor", None),
        P(),
        P(),
        P(),
        P(),
        P(),
        P(),
        P(),
        P(("dp", "tensor"), None),
    )
    return jax.shard_map(
        body,
        mesh=mesh,
        in_specs=placed,
        out_specs=(
            P(("dp", "tensor"), None),
            P(("dp", "tensor"), None),
            P(None, "dp", "tensor"),
            P(None, "tensor"),
            P("tensor", "dp"),
            P(),
            P(),
            P(),
            P("dp", "tensor"),
            P("tensor"),
            P("tensor", "dp"),
            P(),
            P(),
            P(),
            P(),
            P(),
            P(),
            P(),
        ),
        check_vma=False,
    )
```

```python
from functools import partial

import jax
import jax.numpy as jnp
from jax import lax
from jax.sharding import PartitionSpec as P


HEAD = 64


epsilon = 1e-12
masked_value = -1e30


def norm_forward(values, norm_gain, norm_shift):
    centre = values - jnp.mean(values, axis=-1, keepdims=True)
    inverse = lax.rsqrt(jnp.mean(centre * centre, axis=-1, keepdims=True) + epsilon)
    normed = centre * inverse
    return (normed * norm_gain + norm_shift, normed, inverse)


def norm_backward(grad_out, normed, inverse, norm_gain):
    scaled = grad_out * norm_gain
    grad_in = inverse * (
        scaled
        - jnp.mean(scaled, axis=-1, keepdims=True)
        - normed * jnp.mean(scaled * normed, axis=-1, keepdims=True)
    )
    return (grad_in, jnp.sum(grad_out * normed, axis=0), jnp.sum(grad_out, axis=0))


def split_heads(rows, seq_count):
    return rows.reshape(seq_count, rows.shape[0] // seq_count, rows.shape[1] // HEAD, HEAD)


def masked_scores(query_heads, key_heads, segments):
    raw_scores = jnp.einsum(
        "rqhe,rkhe->rhqk", query_heads, key_heads, preferred_element_type=jnp.float32
    ) * HEAD ** (-0.5)
    allowed = segments[:, None, :, None] == segments[:, None, None, :]
    return (jnp.where(allowed, raw_scores, masked_value), allowed)


def attend_forward(queries, key_rows, value_rows, segments):
    seq_count = segments.shape[0]
    scores, _ = masked_scores(
        split_heads(queries, seq_count), split_heads(key_rows, seq_count), segments
    )
    largest = jnp.max(scores, axis=-1, keepdims=True)
    exponent = jnp.exp(scores - largest)
    row_total = jnp.sum(exponent, axis=-1, keepdims=True)
    soft_low = (exponent / row_total).astype(jnp.bfloat16)
    context = jnp.einsum(
        "rhqk,rkhe->rqhe",
        soft_low,
        split_heads(value_rows, seq_count),
        preferred_element_type=jnp.float32,
    )
    context = context.reshape(queries.shape).astype(jnp.bfloat16)
    return (context, largest + jnp.log(row_total))


def attend_backward(queries, key_rows, value_rows, segments, log_total, grad_context):
    seq_count = segments.shape[0]
    query_heads = split_heads(queries, seq_count)
    key_heads = split_heads(key_rows, seq_count)
    value_heads = split_heads(value_rows, seq_count)
    grad_heads = split_heads(grad_context, seq_count)
    scores, allowed = masked_scores(query_heads, key_heads, segments)
    soft_probs = jnp.exp(scores - log_total)
    grad_values = jnp.einsum(
        "rhqk,rqhe->rkhe",
        soft_probs.astype(jnp.bfloat16),
        grad_heads,
        preferred_element_type=jnp.float32,
    )
    grad_soft = jnp.einsum(
        "rqhe,rkhe->rhqk", grad_heads, value_heads, preferred_element_type=jnp.float32
    )
    grad_scores = soft_probs * (grad_soft - jnp.sum(soft_probs * grad_soft, axis=-1, keepdims=True))
    grad_low = lax.optimization_barrier(jnp.where(allowed, grad_scores, 0.0).astype(jnp.bfloat16))
    score_scale = HEAD ** (-0.5)
    grad_queries = (
        jnp.einsum("rhqk,rkhe->rqhe", grad_low, key_heads, preferred_element_type=jnp.float32)
        * score_scale
    )
    grad_keys = (
        jnp.einsum("rhqk,rqhe->rkhe", grad_low, query_heads, preferred_element_type=jnp.float32)
        * score_scale
    )
    full_shape = queries.shape
    return (
        grad_queries.reshape(full_shape).astype(jnp.bfloat16),
        grad_keys.reshape(full_shape).astype(jnp.bfloat16),
        grad_values.reshape(full_shape).astype(jnp.bfloat16),
    )


def body(
    inputs,
    segments,
    labels,
    qkv_weight,
    qv_bias,
    out_weight,
    out_bias,
    norm1_gain,
    norm1_bias,
    up_weight,
    up_bias,
    down_weight,
    down_bias,
    norm2_gain,
    norm2_bias,
    pool_weight,
    pool_bias,
    class_weight,
    class_bias,
    cotangent,
):
    share_rows = inputs.shape[0]
    seq_count, seq_length = segments.shape
    tensor_index = lax.axis_index("tensor")
    tensor_count = lax.axis_size("tensor")
    dp_count = lax.axis_size("dp")
    offset = tensor_index * share_rows

    gathered = lax.all_gather(inputs, "tensor", axis=0, tiled=True)
    group_rows = gathered.shape[0]

    def project(which):
        return jnp.dot(gathered, qkv_weight[which], preferred_element_type=jnp.float32)

    queries = (project(0) + qv_bias[0]).astype(jnp.bfloat16)
    key_rows = project(1).astype(jnp.bfloat16)
    value_rows = (project(2) + qv_bias[1]).astype(jnp.bfloat16)
    local_width = queries.shape[1]

    out_weight_all = lax.all_gather(out_weight, "tensor", axis=0, tiled=False)
    context, log_totals = attend_forward(queries, key_rows, value_rows, segments)
    context_own = lax.all_to_all(
        context.reshape(tensor_count, share_rows, local_width), "tensor", 0, 0, tiled=False
    )
    attended = (
        jnp.einsum(
            "itc,icd->td", context_own, out_weight_all, preferred_element_type=jnp.float32
        )
        + out_bias
    )
    first_norm, normed_one, inverse_one = norm_forward(
        inputs.astype(jnp.float32) + attended, norm1_gain, norm1_bias
    )
    first_low = first_norm.astype(jnp.bfloat16)
    first_all = lax.all_gather(first_low, "tensor", axis=0, tiled=True)
    up_pre = jnp.dot(first_all, up_weight, preferred_element_type=jnp.float32) + up_bias
    gelu_exact = partial(jax.nn.gelu, approximate=False)
    active = gelu_exact(up_pre).astype(jnp.bfloat16)
    ffn_out = (
        lax.psum_scatter(
            jnp.dot(active, down_weight, preferred_element_type=jnp.float32).astype(jnp.bfloat16),
            "tensor",
            scatter_dimension=0,
            tiled=True,
        )
        .astype(jnp.float32)
        + down_bias
    )
    final_norm, normed_two, inverse_two = norm_forward(
        first_norm + ffn_out, norm2_gain, norm2_bias
    )

    positions = offset + jnp.arange(share_rows, dtype=jnp.int32)
    row_starts = jnp.arange(seq_count, dtype=jnp.int32) * seq_length
    selector = (row_starts[:, None] == positions[None, :]).astype(jnp.float32)
    owned = jnp.sum(selector, axis=1, keepdims=True)
    leading = jnp.dot(selector, final_norm, precision=lax.Precision.HIGHEST).astype(jnp.bfloat16)
    pooled = jnp.tanh(jnp.dot(leading, pool_weight, preferred_element_type=jnp.float32) + pool_bias)
    pooled_low = pooled.astype(jnp.bfloat16)
    logits = jnp.dot(pooled_low, class_weight, preferred_element_type=jnp.float32) + class_bias
    chosen = (
        labels[:, None] == jnp.arange(class_weight.shape[1], dtype=jnp.int32)[None, :]
    ).astype(jnp.float32)
    grad_logits = jnp.where(
        owned > 0, jax.nn.softmax(logits, axis=-1) - chosen, 0.0
    ).astype(jnp.bfloat16)
    grad_pre = (
        jnp.einsum("rc,dc->rd", grad_logits, class_weight, preferred_element_type=jnp.float32)
        * (1.0 - pooled * pooled)
    ).astype(jnp.bfloat16)
    grad_leading = jnp.einsum(
        "re,de->rd", grad_pre, pool_weight, preferred_element_type=jnp.float32
    )
    grad_final = cotangent.astype(jnp.float32) + jnp.einsum(
        "rt,rd->td", selector, grad_leading, precision=lax.Precision.HIGHEST
    )
    grad_second, norm2_gain_grad, norm2_bias_grad = norm_backward(
        grad_final, normed_two, inverse_two, norm2_gain
    )
    grad_fed = grad_second.astype(jnp.bfloat16)
    down_bias_grad = jnp.sum(grad_fed.astype(jnp.float32), axis=0)
    grad_fed_all = lax.all_gather(grad_fed, "tensor", axis=0, tiled=True)
    down_weight_grad_t = jnp.einsum(
        "td,tf->df", grad_fed_all, active, preferred_element_type=jnp.float32
    )
    grad_active = jnp.einsum(
        "td,fd->tf", grad_fed_all, down_weight, preferred_element_type=jnp.float32
    )
    grad_up = jax.vjp(gelu_exact, up_pre)[1](grad_active)[0].astype(jnp.bfloat16)
    up_bias_grad = jnp.sum(grad_up.astype(jnp.float32), axis=0)
    up_weight_grad = jnp.einsum("td,tf->df", first_all, grad_up, preferred_element_type=jnp.float32)
    grad_first = (
        lax.psum_scatter(
            jnp.einsum("tf,df->td", grad_up, up_weight, preferred_element_type=jnp.float32).astype(jnp.bfloat16),
            "tensor",
            scatter_dimension=0,
            tiled=True,
        )
        .astype(jnp.float32)
        + grad_second
    )
    grad_res, norm1_gain_grad, norm1_bias_grad = norm_backward(
        grad_first, normed_one, inverse_one, norm1_gain
    )
    grad_att = grad_res.astype(jnp.bfloat16)
    out_bias_grad = jnp.sum(grad_att.astype(jnp.float32), axis=0)

    def joined(parts):
        return jnp.concatenate([part.reshape(-1) for part in parts])

    def parted(flat, parts):
        pieces = []
        begin = 0
        for part in parts:
            pieces.append(flat[begin : begin + part.size].reshape(part.shape))
            begin += part.size
        return pieces

    model_width = grad_att.shape[1]
    classes = class_weight.shape[1]
    row_block = jnp.stack(
        [
            leading.astype(jnp.float32) * owned,
            grad_pre.astype(jnp.float32),
            pooled_low.astype(jnp.float32) * owned,
            jnp.pad(grad_logits.astype(jnp.float32), ((0, 0), (0, model_width - classes))),
        ],
        axis=1,
    )
    token_parts = [
        jnp.stack(
            [
                out_bias_grad,
                norm1_gain_grad,
                norm1_bias_grad,
                down_bias_grad,
                norm2_gain_grad,
                norm2_bias_grad,
            ]
        ),
        row_block,
    ]
    small_flat = token_parts[0].reshape(-1)
    small_round = lax.reduce_precision(small_flat, exponent_bits=8, mantissa_bits=7)
    small_high = small_round.astype(jnp.bfloat16)
    small_low = (small_flat - small_round).astype(jnp.bfloat16)
    rows_low = row_block.reshape(-1).astype(jnp.bfloat16)
    riding_size = 2 * small_flat.size + rows_low.size
    small_rows = -(-riding_size // model_width)
    small_rows += (-(share_rows + small_rows)) % 16
    small_pad = small_rows * model_width - riding_size
    riding = jnp.concatenate(
        [small_high, small_low, rows_low, jnp.zeros((small_pad,), jnp.bfloat16)]
    ).reshape(small_rows, model_width)
    att_gathered = lax.all_gather(
        jnp.concatenate([grad_att, riding], axis=0), "tensor", axis=0, tiled=False
    )
    grad_att_all = att_gathered[:, :share_rows].reshape(group_rows, model_width)
    small_back = att_gathered[:, share_rows:].reshape(tensor_count, -1).astype(jnp.float32)
    token_size = small_flat.size
    token_sum = jnp.sum(
        small_back[:, :token_size] + small_back[:, token_size : 2 * token_size], axis=0
    ).reshape(token_parts[0].shape)
    rows_group = jnp.sum(
        small_back[:, 2 * token_size : 2 * token_size + rows_low.size], axis=0
    ).reshape(row_block.shape)
    out_weight_grad_t = jnp.einsum(
        "td,te->de", grad_att_all, context, preferred_element_type=jnp.float32
    )
    grad_context = jnp.einsum(
        "td,ed->te", grad_att_all, out_weight, preferred_element_type=jnp.float32
    ).astype(jnp.bfloat16)
    grad_queries, grad_keys, grad_values = attend_backward(
        queries, key_rows, value_rows, segments, log_totals, grad_context
    )
    stacked = jnp.stack([grad_queries, grad_keys, grad_values])
    qkv_weight_grad = jnp.einsum(
        "td,tq->dq",
        gathered,
        jnp.concatenate([grad_queries, grad_keys, grad_values], axis=1),
        preferred_element_type=jnp.float32,
    )
    qv_bias_grad = jnp.stack(
        [
            jnp.sum(grad_queries.astype(jnp.float32), axis=0),
            jnp.sum(grad_values.astype(jnp.float32), axis=0),
        ]
    )
    input_grad = (
        lax.psum_scatter(
            jnp.einsum(
                "kte,kde->td", stacked, qkv_weight, preferred_element_type=jnp.float32
            ).astype(jnp.bfloat16),
            "tensor",
            scatter_dimension=0,
            tiled=True,
        ).astype(jnp.float32)
        + grad_res
    ).astype(jnp.bfloat16)

    def stacked_sum(parts, dtype):
        padded = [
            jnp.pad(part.astype(dtype), ((0, 0), (0, (-part.shape[1]) % 16), (0, 0)))
            for part in parts
        ]
        flat = jnp.concatenate(padded, axis=1)
        lanes = flat.shape[2]
        summed = lax.psum_scatter(
            flat.reshape(-1, lanes), "dp", scatter_dimension=0, tiled=True
        )
        pieces = []
        begin = 0
        for part, held in zip(parts, padded):
            pieces.append(summed[begin : begin + part.shape[1]])
            begin += held.shape[1]
        return pieces

    def in_blocks(grad):
        return grad.reshape(dp_count, grad.shape[0] // dp_count, grad.shape[1])

    def copied(flat, lanes):
        rows = -(-flat.size // lanes)
        flat = jnp.pad(flat, (0, rows * lanes - flat.size)).reshape(1, rows, lanes)
        return jnp.broadcast_to(flat, (dp_count, rows, lanes))

    out_blocks = in_blocks(out_weight_grad_t).reshape(dp_count, -1, model_width)
    early_parts = [in_blocks(up_weight_grad), in_blocks(down_weight_grad_t), out_blocks]
    early_sums = stacked_sum(early_parts, jnp.bfloat16)
    up_sum = early_sums[0].astype(jnp.float32)
    down_sum = early_sums[1].astype(jnp.float32).T
    out_sum = early_sums[2].reshape(-1, out_weight_grad_t.shape[1]).astype(jnp.float32).T
    late_shared = [qv_bias_grad, token_sum, up_bias_grad]
    qkv_lanes = qkv_weight_grad.shape[1]

    def aligned(part):
        return jnp.pad(part, ((0, 0), (0, (-part.shape[1]) % 16), (0, 0)))

    shared_flat = joined(late_shared)
    shared_round = lax.reduce_precision(shared_flat, exponent_bits=8, mantissa_bits=7)
    shared_pair = jnp.concatenate([shared_round, shared_flat - shared_round]).astype(jnp.bfloat16)
    late_parts = [
        aligned(in_blocks(qkv_weight_grad).astype(jnp.bfloat16)),
        aligned(copied(shared_pair, qkv_lanes)),
        aligned(copied(rows_group.reshape(-1).astype(jnp.bfloat16), qkv_lanes)),
    ]
    late_received = lax.all_to_all(
        jnp.concatenate(late_parts, axis=1), "dp", 0, 0, tiled=False
    )
    qkv_rows = in_blocks(qkv_weight_grad).shape[1]
    shared_begin = late_parts[0].shape[1]
    rows_begin = shared_begin + late_parts[1].shape[1]
    qkv_total = jnp.sum(late_received[:, :qkv_rows].astype(jnp.float32), axis=0)
    qkv_sum = jnp.transpose(qkv_total.reshape(qkv_rows, 3, qkv_lanes // 3), (1, 0, 2))
    shared_back = late_received[:, shared_begin:rows_begin].reshape(dp_count, -1)
    shared_back = shared_back.astype(jnp.float32)
    shared_total = jnp.sum(
        shared_back[:, : shared_flat.size]
        + shared_back[:, shared_flat.size : 2 * shared_flat.size],
        axis=0,
    )
    qv_bias_total, token_grads, up_bias_total = parted(shared_total, late_shared)
    rows_each = late_received[:, rows_begin:].reshape(dp_count, -1)[:, : rows_group.size]
    rows_all = rows_each.reshape(dp_count * seq_count, 4, model_width).astype(jnp.bfloat16)
    leading_all = rows_all[:, 0]
    grad_pre_all = rows_all[:, 1]
    pooled_all = rows_all[:, 2]
    grad_logits_all = rows_all[:, 3, :classes]
    pool_weight_grad = jnp.einsum(
        "rd,re->de", leading_all, grad_pre_all, preferred_element_type=jnp.float32
    )
    pool_bias_grad = jnp.sum(grad_pre_all.astype(jnp.float32), axis=0)
    class_weight_grad = jnp.einsum(
        "rd,rc->dc", pooled_all, grad_logits_all, preferred_element_type=jnp.float32
    )
    class_bias_grad = jnp.sum(grad_logits_all.astype(jnp.float32), axis=0)

    return (
        final_norm.astype(jnp.bfloat16),
        input_grad,
        qkv_sum,
        qv_bias_total,
        out_sum,
        token_grads[0],
        token_grads[1],
        token_grads[2],
        up_sum,
        up_bias_total,
        down_sum,
        token_grads[3],
        token_grads[4],
        token_grads[5],
        pool_weight_grad,
        pool_bias_grad,
        class_weight_grad,
        class_bias_grad,
    )


def solution(mesh):
    placed = (
        P(("dp", "tensor"), None),
        P("dp", None),
        P("dp"),
        P(None, None, "tensor"),
        P(None, "tensor"),
        P("tensor", None),
        P(),
        P(),
        P(),
        P(None, "tensor"),
        P("tensor"),
        P("tensor", None),
        P(),
        P(),
        P(),
        P(),
        P(),
        P(),
        P(),
        P(("dp", "tensor"), None),
    )
    return jax.shard_map(
        body,
        mesh=mesh,
        in_specs=placed,
        out_specs=(
            P(("dp", "tensor"), None),
            P(("dp", "tensor"), None),
            P(None, "dp", "tensor"),
            P(None, "tensor"),
            P("tensor", "dp"),
            P(),
            P(),
            P(),
            P("dp", "tensor"),
            P("tensor"),
            P("tensor", "dp"),
            P(),
            P(),
            P(),
            P(),
            P(),
            P(),
            P(),
        ),
        check_vma=False,
    )
```

```python
from functools import partial

import jax
import jax.numpy as jnp
from jax import lax
from jax.sharding import PartitionSpec as P


HEAD = 64


epsilon = 1e-12
masked_value = -1e30


def norm_forward(values, norm_gain, norm_shift):
    centre = values - jnp.mean(values, axis=-1, keepdims=True)
    inverse = lax.rsqrt(jnp.mean(centre * centre, axis=-1, keepdims=True) + epsilon)
    normed = centre * inverse
    return (normed * norm_gain + norm_shift, normed, inverse)


def norm_backward(grad_out, normed, inverse, norm_gain):
    scaled = grad_out * norm_gain
    grad_in = inverse * (
        scaled
        - jnp.mean(scaled, axis=-1, keepdims=True)
        - normed * jnp.mean(scaled * normed, axis=-1, keepdims=True)
    )
    return (grad_in, jnp.sum(grad_out * normed, axis=0), jnp.sum(grad_out, axis=0))


def split_heads(rows, seq_count):
    return rows.reshape(seq_count, rows.shape[0] // seq_count, rows.shape[1] // HEAD, HEAD)


def masked_scores(query_heads, key_heads, segments):
    raw_scores = jnp.einsum(
        "rqhe,rkhe->rhqk", query_heads, key_heads, preferred_element_type=jnp.float32
    ) * HEAD ** (-0.5)
    allowed = segments[:, None, :, None] == segments[:, None, None, :]
    return (jnp.where(allowed, raw_scores, masked_value), allowed)


def attend_forward(queries, key_rows, value_rows, segments):
    seq_count = segments.shape[0]
    scores, _ = masked_scores(
        split_heads(queries, seq_count), split_heads(key_rows, seq_count), segments
    )
    largest = jnp.max(scores, axis=-1, keepdims=True)
    exponent = jnp.exp(scores - largest)
    row_total = jnp.sum(exponent, axis=-1, keepdims=True)
    soft_low = (exponent / row_total).astype(jnp.bfloat16)
    context = jnp.einsum(
        "rhqk,rkhe->rqhe",
        soft_low,
        split_heads(value_rows, seq_count),
        preferred_element_type=jnp.float32,
    )
    context = context.reshape(queries.shape).astype(jnp.bfloat16)
    return (context, largest + jnp.log(row_total))


def attend_backward(queries, key_rows, value_rows, segments, log_total, grad_context):
    seq_count = segments.shape[0]
    query_heads = split_heads(queries, seq_count)
    key_heads = split_heads(key_rows, seq_count)
    value_heads = split_heads(value_rows, seq_count)
    grad_heads = split_heads(grad_context, seq_count)
    scores, allowed = masked_scores(query_heads, key_heads, segments)
    soft_probs = jnp.exp(scores - log_total)
    grad_values = jnp.einsum(
        "rhqk,rqhe->rkhe",
        soft_probs.astype(jnp.bfloat16),
        grad_heads,
        preferred_element_type=jnp.float32,
    )
    grad_soft = jnp.einsum(
        "rqhe,rkhe->rhqk", grad_heads, value_heads, preferred_element_type=jnp.float32
    )
    grad_scores = soft_probs * (grad_soft - jnp.sum(soft_probs * grad_soft, axis=-1, keepdims=True))
    grad_low = lax.optimization_barrier(jnp.where(allowed, grad_scores, 0.0).astype(jnp.bfloat16))
    score_scale = HEAD ** (-0.5)
    grad_queries = (
        jnp.einsum("rhqk,rkhe->rqhe", grad_low, key_heads, preferred_element_type=jnp.float32)
        * score_scale
    )
    grad_keys = (
        jnp.einsum("rhqk,rqhe->rkhe", grad_low, query_heads, preferred_element_type=jnp.float32)
        * score_scale
    )
    full_shape = queries.shape
    return (
        grad_queries.reshape(full_shape).astype(jnp.bfloat16),
        grad_keys.reshape(full_shape).astype(jnp.bfloat16),
        grad_values.reshape(full_shape).astype(jnp.bfloat16),
    )


def body(
    inputs,
    segments,
    labels,
    qkv_weight,
    qv_bias,
    out_weight,
    out_bias,
    norm1_gain,
    norm1_bias,
    up_weight,
    up_bias,
    down_weight,
    down_bias,
    norm2_gain,
    norm2_bias,
    pool_weight,
    pool_bias,
    class_weight,
    class_bias,
    cotangent,
):
    share_rows = inputs.shape[0]
    seq_count, seq_length = segments.shape
    tensor_index = lax.axis_index("tensor")
    tensor_count = lax.axis_size("tensor")
    dp_count = lax.axis_size("dp")
    offset = tensor_index * share_rows

    gathered = lax.all_gather(inputs, "tensor", axis=0, tiled=True)
    group_rows = gathered.shape[0]

    def project(which):
        return jnp.dot(gathered, qkv_weight[which], preferred_element_type=jnp.float32)

    queries = (project(0) + qv_bias[0]).astype(jnp.bfloat16)
    key_rows = project(1).astype(jnp.bfloat16)
    value_rows = (project(2) + qv_bias[1]).astype(jnp.bfloat16)
    local_width = queries.shape[1]

    out_weight_all = lax.all_gather(out_weight, "tensor", axis=0, tiled=False)
    context, log_totals = attend_forward(queries, key_rows, value_rows, segments)
    context_own = lax.all_to_all(
        context.reshape(tensor_count, share_rows, local_width), "tensor", 0, 0, tiled=False
    )
    attended = (
        jnp.einsum(
            "itc,icd->td", context_own, out_weight_all, preferred_element_type=jnp.float32
        )
        + out_bias
    )
    first_norm, normed_one, inverse_one = norm_forward(
        inputs.astype(jnp.float32) + attended, norm1_gain, norm1_bias
    )
    first_low = first_norm.astype(jnp.bfloat16)
    first_all = lax.all_gather(first_low, "tensor", axis=0, tiled=True)
    up_pre = jnp.dot(first_all, up_weight, preferred_element_type=jnp.float32) + up_bias
    gelu_exact = partial(jax.nn.gelu, approximate=False)
    active = gelu_exact(up_pre).astype(jnp.bfloat16)
    ffn_out = (
        lax.psum_scatter(
            jnp.dot(active, down_weight, preferred_element_type=jnp.float32).astype(jnp.bfloat16),
            "tensor",
            scatter_dimension=0,
            tiled=True,
        )
        .astype(jnp.float32)
        + down_bias
    )
    final_norm, normed_two, inverse_two = norm_forward(
        first_norm + ffn_out, norm2_gain, norm2_bias
    )

    positions = offset + jnp.arange(share_rows, dtype=jnp.int32)
    row_starts = jnp.arange(seq_count, dtype=jnp.int32) * seq_length
    selector = (row_starts[:, None] == positions[None, :]).astype(jnp.float32)
    owned = jnp.sum(selector, axis=1, keepdims=True)
    leading = jnp.dot(selector, final_norm, precision=lax.Precision.HIGHEST).astype(jnp.bfloat16)
    pooled = jnp.tanh(jnp.dot(leading, pool_weight, preferred_element_type=jnp.float32) + pool_bias)
    pooled_low = pooled.astype(jnp.bfloat16)
    logits = jnp.dot(pooled_low, class_weight, preferred_element_type=jnp.float32) + class_bias
    chosen = (
        labels[:, None] == jnp.arange(class_weight.shape[1], dtype=jnp.int32)[None, :]
    ).astype(jnp.float32)
    grad_logits = jnp.where(
        owned > 0, jax.nn.softmax(logits, axis=-1) - chosen, 0.0
    ).astype(jnp.bfloat16)
    grad_pre = (
        jnp.einsum("rc,dc->rd", grad_logits, class_weight, preferred_element_type=jnp.float32)
        * (1.0 - pooled * pooled)
    ).astype(jnp.bfloat16)
    grad_leading = jnp.einsum(
        "re,de->rd", grad_pre, pool_weight, preferred_element_type=jnp.float32
    )
    grad_final = cotangent.astype(jnp.float32) + jnp.einsum(
        "rt,rd->td", selector, grad_leading, precision=lax.Precision.HIGHEST
    )
    grad_second, norm2_gain_grad, norm2_bias_grad = norm_backward(
        grad_final, normed_two, inverse_two, norm2_gain
    )
    grad_fed = grad_second.astype(jnp.bfloat16)
    down_bias_grad = jnp.sum(grad_fed.astype(jnp.float32), axis=0)
    grad_fed_all = lax.all_gather(grad_fed, "tensor", axis=0, tiled=True)
    down_weight_grad_t = jnp.einsum(
        "td,tf->df", grad_fed_all, active, preferred_element_type=jnp.float32
    )
    grad_active = jnp.einsum(
        "td,fd->tf", grad_fed_all, down_weight, preferred_element_type=jnp.float32
    )
    grad_up = jax.vjp(gelu_exact, up_pre)[1](grad_active)[0].astype(jnp.bfloat16)
    up_bias_grad = jnp.sum(grad_up.astype(jnp.float32), axis=0)
    up_weight_grad = jnp.einsum("td,tf->df", first_all, grad_up, preferred_element_type=jnp.float32)
    grad_first = (
        lax.psum_scatter(
            jnp.einsum("tf,df->td", grad_up, up_weight, preferred_element_type=jnp.float32).astype(jnp.bfloat16),
            "tensor",
            scatter_dimension=0,
            tiled=True,
        )
        .astype(jnp.float32)
        + grad_second
    )
    grad_res, norm1_gain_grad, norm1_bias_grad = norm_backward(
        grad_first, normed_one, inverse_one, norm1_gain
    )
    grad_att = grad_res.astype(jnp.bfloat16)
    out_bias_grad = jnp.sum(grad_att.astype(jnp.float32), axis=0)

    def joined(parts):
        return jnp.concatenate([part.reshape(-1) for part in parts])

    def parted(flat, parts):
        pieces = []
        begin = 0
        for part in parts:
            pieces.append(flat[begin : begin + part.size].reshape(part.shape))
            begin += part.size
        return pieces

    model_width = grad_att.shape[1]
    classes = class_weight.shape[1]
    row_block = jnp.stack(
        [
            leading.astype(jnp.float32) * owned,
            grad_pre.astype(jnp.float32),
            pooled_low.astype(jnp.float32) * owned,
            jnp.pad(grad_logits.astype(jnp.float32), ((0, 0), (0, model_width - classes))),
        ],
        axis=1,
    )
    token_parts = [
        jnp.stack(
            [
                out_bias_grad,
                norm1_gain_grad,
                norm1_bias_grad,
                down_bias_grad,
                norm2_gain_grad,
                norm2_bias_grad,
            ]
        ),
        row_block,
    ]
    small_flat = token_parts[0].reshape(-1)
    small_round = lax.reduce_precision(small_flat, exponent_bits=8, mantissa_bits=7)
    small_high = small_round.astype(jnp.bfloat16)
    small_low = (small_flat - small_round).astype(jnp.bfloat16)
    rows_low = row_block.reshape(-1).astype(jnp.bfloat16)
    riding_size = 2 * small_flat.size + rows_low.size
    small_rows = -(-riding_size // model_width)
    small_rows += (-(share_rows + small_rows)) % 16
    small_pad = small_rows * model_width - riding_size
    riding = jnp.concatenate(
        [small_high, small_low, rows_low, jnp.zeros((small_pad,), jnp.bfloat16)]
    ).reshape(small_rows, model_width)
    att_gathered = lax.all_gather(
        jnp.concatenate([grad_att, riding], axis=0), "tensor", axis=0, tiled=False
    )
    grad_att_all = att_gathered[:, :share_rows].reshape(group_rows, model_width)
    small_back = att_gathered[:, share_rows:].reshape(tensor_count, -1).astype(jnp.float32)
    token_size = small_flat.size
    token_sum = jnp.sum(
        small_back[:, :token_size] + small_back[:, token_size : 2 * token_size], axis=0
    ).reshape(token_parts[0].shape)
    rows_group = jnp.sum(
        small_back[:, 2 * token_size : 2 * token_size + rows_low.size], axis=0
    ).reshape(row_block.shape)
    out_weight_grad_t = jnp.einsum(
        "td,te->de", grad_att_all, context, preferred_element_type=jnp.float32
    )
    grad_context = jnp.einsum(
        "td,ed->te", grad_att_all, out_weight, preferred_element_type=jnp.float32
    ).astype(jnp.bfloat16)
    grad_queries, grad_keys, grad_values = attend_backward(
        queries, key_rows, value_rows, segments, log_totals, grad_context
    )
    stacked = jnp.stack([grad_queries, grad_keys, grad_values])
    qkv_weight_grad = jnp.einsum(
        "td,tq->dq",
        gathered,
        jnp.concatenate([grad_queries, grad_keys, grad_values], axis=1),
        preferred_element_type=jnp.float32,
    )
    qv_bias_grad = jnp.stack(
        [
            jnp.sum(grad_queries.astype(jnp.float32), axis=0),
            jnp.sum(grad_values.astype(jnp.float32), axis=0),
        ]
    )
    input_part = jnp.einsum(
        "kte,kde->td", stacked, qkv_weight, preferred_element_type=jnp.float32
    ).astype(jnp.bfloat16)
    split_width = (input_part.shape[1] * 3 // 512) * 128
    summed_half = lax.psum_scatter(
        input_part[:, :split_width], "tensor", scatter_dimension=0, tiled=True
    ).astype(jnp.float32)
    swapped_half = lax.all_to_all(
        input_part[:, split_width:].reshape(tensor_count, share_rows, -1),
        "tensor",
        0,
        0,
        tiled=False,
    )
    input_sum = jnp.concatenate(
        [summed_half, jnp.sum(swapped_half.astype(jnp.float32), axis=0)], axis=1
    )
    input_grad = (input_sum + grad_res).astype(jnp.bfloat16)

    def stacked_sum(parts, dtype):
        padded = [
            jnp.pad(part.astype(dtype), ((0, 0), (0, (-part.shape[1]) % 16), (0, 0)))
            for part in parts
        ]
        flat = jnp.concatenate(padded, axis=1)
        lanes = flat.shape[2]
        summed = lax.psum_scatter(
            flat.reshape(-1, lanes), "dp", scatter_dimension=0, tiled=True
        )
        pieces = []
        begin = 0
        for part, held in zip(parts, padded):
            pieces.append(summed[begin : begin + part.shape[1]])
            begin += held.shape[1]
        return pieces

    def in_blocks(grad):
        return grad.reshape(dp_count, grad.shape[0] // dp_count, grad.shape[1])

    def copied(flat, lanes):
        rows = -(-flat.size // lanes)
        flat = jnp.pad(flat, (0, rows * lanes - flat.size)).reshape(1, rows, lanes)
        return jnp.broadcast_to(flat, (dp_count, rows, lanes))

    early_parts = [in_blocks(up_weight_grad), in_blocks(down_weight_grad_t)]
    early_sums = stacked_sum(early_parts, jnp.bfloat16)
    up_sum = early_sums[0].astype(jnp.float32)
    down_sum = early_sums[1].astype(jnp.float32).T
    late_shared = [qv_bias_grad, token_sum, up_bias_grad]
    qkv_lanes = qkv_weight_grad.shape[1]

    def aligned(part):
        return jnp.pad(part, ((0, 0), (0, (-part.shape[1]) % 16), (0, 0)))

    shared_flat = joined(late_shared)
    shared_round = lax.reduce_precision(shared_flat, exponent_bits=8, mantissa_bits=7)
    shared_pair = jnp.concatenate([shared_round, shared_flat - shared_round]).astype(jnp.bfloat16)
    qkv_lanes = qkv_weight_grad.shape[1]
    out_flat = in_blocks(out_weight_grad_t).astype(jnp.bfloat16).reshape(dp_count, -1)
    out_rows = -(-out_flat.shape[1] // qkv_lanes)
    out_blocks = jnp.pad(out_flat, ((0, 0), (0, out_rows * qkv_lanes - out_flat.shape[1])))
    late_parts = [
        aligned(in_blocks(qkv_weight_grad).astype(jnp.bfloat16)),
        aligned(out_blocks.reshape(dp_count, out_rows, qkv_lanes)),
        aligned(copied(shared_pair, qkv_lanes)),
        aligned(copied(rows_group.reshape(-1).astype(jnp.bfloat16), qkv_lanes)),
    ]
    late_received = lax.all_to_all(
        jnp.concatenate(late_parts, axis=1), "dp", 0, 0, tiled=False
    )
    qkv_rows = in_blocks(qkv_weight_grad).shape[1]
    out_begin = late_parts[0].shape[1]
    shared_begin = out_begin + late_parts[1].shape[1]
    rows_begin = shared_begin + late_parts[2].shape[1]
    qkv_total = jnp.sum(late_received[:, :qkv_rows].astype(jnp.float32), axis=0)
    out_total = jnp.sum(
        late_received[:, out_begin:shared_begin].reshape(dp_count, -1).astype(jnp.float32),
        axis=0,
    )
    out_sum = out_total[: out_flat.shape[1]].reshape(-1, out_weight_grad_t.shape[1]).T
    qkv_sum = jnp.transpose(qkv_total.reshape(qkv_rows, 3, qkv_lanes // 3), (1, 0, 2))
    shared_back = late_received[:, shared_begin:rows_begin].reshape(dp_count, -1)
    shared_back = shared_back.astype(jnp.float32)
    shared_total = jnp.sum(
        shared_back[:, : shared_flat.size]
        + shared_back[:, shared_flat.size : 2 * shared_flat.size],
        axis=0,
    )
    qv_bias_total, token_grads, up_bias_total = parted(shared_total, late_shared)
    rows_each = late_received[:, rows_begin:].reshape(dp_count, -1)[:, : rows_group.size]
    rows_all = rows_each.reshape(dp_count * seq_count, 4, model_width).astype(jnp.bfloat16)
    leading_all = rows_all[:, 0]
    grad_pre_all = rows_all[:, 1]
    pooled_all = rows_all[:, 2]
    grad_logits_all = rows_all[:, 3, :classes]
    pool_weight_grad = jnp.einsum(
        "rd,re->de", leading_all, grad_pre_all, preferred_element_type=jnp.float32
    )
    pool_bias_grad = jnp.sum(grad_pre_all.astype(jnp.float32), axis=0)
    class_weight_grad = jnp.einsum(
        "rd,rc->dc", pooled_all, grad_logits_all, preferred_element_type=jnp.float32
    )
    class_bias_grad = jnp.sum(grad_logits_all.astype(jnp.float32), axis=0)

    return (
        final_norm.astype(jnp.bfloat16),
        input_grad,
        qkv_sum,
        qv_bias_total,
        out_sum,
        token_grads[0],
        token_grads[1],
        token_grads[2],
        up_sum,
        up_bias_total,
        down_sum,
        token_grads[3],
        token_grads[4],
        token_grads[5],
        pool_weight_grad,
        pool_bias_grad,
        class_weight_grad,
        class_bias_grad,
    )


def solution(mesh):
    placed = (
        P(("dp", "tensor"), None),
        P("dp", None),
        P("dp"),
        P(None, None, "tensor"),
        P(None, "tensor"),
        P("tensor", None),
        P(),
        P(),
        P(),
        P(None, "tensor"),
        P("tensor"),
        P("tensor", None),
        P(),
        P(),
        P(),
        P(),
        P(),
        P(),
        P(),
        P(("dp", "tensor"), None),
    )
    return jax.shard_map(
        body,
        mesh=mesh,
        in_specs=placed,
        out_specs=(
            P(("dp", "tensor"), None),
            P(("dp", "tensor"), None),
            P(None, "dp", "tensor"),
            P(None, "tensor"),
            P("tensor", "dp"),
            P(),
            P(),
            P(),
            P("dp", "tensor"),
            P("tensor"),
            P("tensor", "dp"),
            P(),
            P(),
            P(),
            P(),
            P(),
            P(),
            P(),
        ),
        check_vma=False,
    )
```

```python
from functools import partial

import jax
import jax.numpy as jnp
from jax import lax
from jax.sharding import PartitionSpec as P


HEAD = 64


epsilon = 1e-12
masked_value = -1e30


def norm_forward(values, norm_gain, norm_shift):
    centre = values - jnp.mean(values, axis=-1, keepdims=True)
    inverse = lax.rsqrt(jnp.mean(centre * centre, axis=-1, keepdims=True) + epsilon)
    normed = centre * inverse
    return (normed * norm_gain + norm_shift, normed, inverse)


def norm_backward(grad_out, normed, inverse, norm_gain):
    scaled = grad_out * norm_gain
    grad_in = inverse * (
        scaled
        - jnp.mean(scaled, axis=-1, keepdims=True)
        - normed * jnp.mean(scaled * normed, axis=-1, keepdims=True)
    )
    return (grad_in, jnp.sum(grad_out * normed, axis=0), jnp.sum(grad_out, axis=0))


def split_heads(rows, seq_count):
    return rows.reshape(seq_count, rows.shape[0] // seq_count, rows.shape[1] // HEAD, HEAD)


def masked_scores(query_heads, key_heads, segments):
    raw_scores = jnp.einsum(
        "rqhe,rkhe->rhqk", query_heads, key_heads, preferred_element_type=jnp.float32
    ) * HEAD ** (-0.5)
    allowed = segments[:, None, :, None] == segments[:, None, None, :]
    return (jnp.where(allowed, raw_scores, masked_value), allowed)


def attend_forward(queries, key_rows, value_rows, segments):
    seq_count = segments.shape[0]
    scores, _ = masked_scores(
        split_heads(queries, seq_count), split_heads(key_rows, seq_count), segments
    )
    largest = jnp.max(scores, axis=-1, keepdims=True)
    exponent = jnp.exp(scores - largest)
    row_total = jnp.sum(exponent, axis=-1, keepdims=True)
    soft_low = (exponent / row_total).astype(jnp.bfloat16)
    context = jnp.einsum(
        "rhqk,rkhe->rqhe",
        soft_low,
        split_heads(value_rows, seq_count),
        preferred_element_type=jnp.float32,
    )
    context = context.reshape(queries.shape).astype(jnp.bfloat16)
    return (context, largest + jnp.log(row_total))


def attend_backward(queries, key_rows, value_rows, segments, log_total, grad_context):
    seq_count = segments.shape[0]
    query_heads = split_heads(queries, seq_count)
    key_heads = split_heads(key_rows, seq_count)
    value_heads = split_heads(value_rows, seq_count)
    grad_heads = split_heads(grad_context, seq_count)
    scores, allowed = masked_scores(query_heads, key_heads, segments)
    soft_probs = jnp.exp(scores - log_total)
    grad_values = jnp.einsum(
        "rhqk,rqhe->rkhe",
        soft_probs.astype(jnp.bfloat16),
        grad_heads,
        preferred_element_type=jnp.float32,
    )
    grad_soft = jnp.einsum(
        "rqhe,rkhe->rhqk", grad_heads, value_heads, preferred_element_type=jnp.float32
    )
    grad_scores = soft_probs * (grad_soft - jnp.sum(soft_probs * grad_soft, axis=-1, keepdims=True))
    grad_low = lax.optimization_barrier(jnp.where(allowed, grad_scores, 0.0).astype(jnp.bfloat16))
    score_scale = HEAD ** (-0.5)
    grad_queries = (
        jnp.einsum("rhqk,rkhe->rqhe", grad_low, key_heads, preferred_element_type=jnp.float32)
        * score_scale
    )
    grad_keys = (
        jnp.einsum("rhqk,rqhe->rkhe", grad_low, query_heads, preferred_element_type=jnp.float32)
        * score_scale
    )
    full_shape = queries.shape
    return (
        grad_queries.reshape(full_shape).astype(jnp.bfloat16),
        grad_keys.reshape(full_shape).astype(jnp.bfloat16),
        grad_values.reshape(full_shape).astype(jnp.bfloat16),
    )


def body(
    inputs,
    segments,
    labels,
    qkv_weight,
    qv_bias,
    out_weight,
    out_bias,
    norm1_gain,
    norm1_bias,
    up_weight,
    up_bias,
    down_weight,
    down_bias,
    norm2_gain,
    norm2_bias,
    pool_weight,
    pool_bias,
    class_weight,
    class_bias,
    cotangent,
):
    share_rows = inputs.shape[0]
    seq_count, seq_length = segments.shape
    tensor_index = lax.axis_index("tensor")
    tensor_count = lax.axis_size("tensor")
    dp_count = lax.axis_size("dp")
    offset = tensor_index * share_rows

    gathered = lax.all_gather(inputs, "tensor", axis=0, tiled=True)
    group_rows = gathered.shape[0]

    def project(which):
        return jnp.dot(gathered, qkv_weight[which], preferred_element_type=jnp.float32)

    queries = (project(0) + qv_bias[0]).astype(jnp.bfloat16)
    key_rows = project(1).astype(jnp.bfloat16)
    value_rows = (project(2) + qv_bias[1]).astype(jnp.bfloat16)
    local_width = queries.shape[1]

    out_weight_all = lax.all_gather(out_weight, "tensor", axis=0, tiled=False)
    context, log_totals = attend_forward(queries, key_rows, value_rows, segments)
    context_own = lax.all_to_all(
        context.reshape(tensor_count, share_rows, local_width), "tensor", 0, 0, tiled=False
    )
    attended = (
        jnp.einsum(
            "itc,icd->td", context_own, out_weight_all, preferred_element_type=jnp.float32
        )
        + out_bias
    )
    first_norm, normed_one, inverse_one = norm_forward(
        inputs.astype(jnp.float32) + attended, norm1_gain, norm1_bias
    )
    first_low = first_norm.astype(jnp.bfloat16)
    first_all = lax.all_gather(first_low, "tensor", axis=0, tiled=True)
    up_pre = jnp.dot(first_all, up_weight, preferred_element_type=jnp.float32) + up_bias
    gelu_exact = partial(jax.nn.gelu, approximate=False)
    active = gelu_exact(up_pre).astype(jnp.bfloat16)
    ffn_out = (
        lax.psum_scatter(
            jnp.dot(active, down_weight, preferred_element_type=jnp.float32).astype(jnp.bfloat16),
            "tensor",
            scatter_dimension=0,
            tiled=True,
        )
        .astype(jnp.float32)
        + down_bias
    )
    final_norm, normed_two, inverse_two = norm_forward(
        first_norm + ffn_out, norm2_gain, norm2_bias
    )

    positions = offset + jnp.arange(share_rows, dtype=jnp.int32)
    row_starts = jnp.arange(seq_count, dtype=jnp.int32) * seq_length
    selector = (row_starts[:, None] == positions[None, :]).astype(jnp.float32)
    owned = jnp.sum(selector, axis=1, keepdims=True)
    leading = jnp.dot(selector, final_norm, precision=lax.Precision.HIGHEST).astype(jnp.bfloat16)
    pooled = jnp.tanh(jnp.dot(leading, pool_weight, preferred_element_type=jnp.float32) + pool_bias)
    pooled_low = pooled.astype(jnp.bfloat16)
    logits = jnp.dot(pooled_low, class_weight, preferred_element_type=jnp.float32) + class_bias
    chosen = (
        labels[:, None] == jnp.arange(class_weight.shape[1], dtype=jnp.int32)[None, :]
    ).astype(jnp.float32)
    grad_logits = jnp.where(
        owned > 0, jax.nn.softmax(logits, axis=-1) - chosen, 0.0
    ).astype(jnp.bfloat16)
    grad_pre = (
        jnp.einsum("rc,dc->rd", grad_logits, class_weight, preferred_element_type=jnp.float32)
        * (1.0 - pooled * pooled)
    ).astype(jnp.bfloat16)
    grad_leading = jnp.einsum(
        "re,de->rd", grad_pre, pool_weight, preferred_element_type=jnp.float32
    )
    grad_final = cotangent.astype(jnp.float32) + jnp.einsum(
        "rt,rd->td", selector, grad_leading, precision=lax.Precision.HIGHEST
    )
    grad_second, norm2_gain_grad, norm2_bias_grad = norm_backward(
        grad_final, normed_two, inverse_two, norm2_gain
    )
    grad_fed = grad_second.astype(jnp.bfloat16)
    down_bias_grad = jnp.sum(grad_fed.astype(jnp.float32), axis=0)
    grad_fed_all = lax.all_gather(grad_fed, "tensor", axis=0, tiled=True)
    down_weight_grad_t = jnp.einsum(
        "td,tf->df", grad_fed_all, active, preferred_element_type=jnp.float32
    )
    grad_active = jnp.einsum(
        "td,fd->tf", grad_fed_all, down_weight, preferred_element_type=jnp.float32
    )
    grad_up = jax.vjp(gelu_exact, up_pre)[1](grad_active)[0].astype(jnp.bfloat16)
    up_bias_grad = jnp.sum(grad_up.astype(jnp.float32), axis=0)
    up_weight_grad = jnp.einsum("td,tf->df", first_all, grad_up, preferred_element_type=jnp.float32)
    grad_first = (
        lax.psum_scatter(
            jnp.einsum("tf,df->td", grad_up, up_weight, preferred_element_type=jnp.float32).astype(jnp.bfloat16),
            "tensor",
            scatter_dimension=0,
            tiled=True,
        )
        .astype(jnp.float32)
        + grad_second
    )
    grad_res, norm1_gain_grad, norm1_bias_grad = norm_backward(
        grad_first, normed_one, inverse_one, norm1_gain
    )
    grad_att = grad_res.astype(jnp.bfloat16)
    out_bias_grad = jnp.sum(grad_att.astype(jnp.float32), axis=0)

    def joined(parts):
        return jnp.concatenate([part.reshape(-1) for part in parts])

    def parted(flat, parts):
        pieces = []
        begin = 0
        for part in parts:
            pieces.append(flat[begin : begin + part.size].reshape(part.shape))
            begin += part.size
        return pieces

    model_width = grad_att.shape[1]
    classes = class_weight.shape[1]
    row_block = jnp.stack(
        [
            leading.astype(jnp.float32) * owned,
            grad_pre.astype(jnp.float32),
            pooled_low.astype(jnp.float32) * owned,
            jnp.pad(grad_logits.astype(jnp.float32), ((0, 0), (0, model_width - classes))),
        ],
        axis=1,
    )
    token_parts = [
        jnp.stack(
            [
                out_bias_grad,
                norm1_gain_grad,
                norm1_bias_grad,
                down_bias_grad,
                norm2_gain_grad,
                norm2_bias_grad,
            ]
        ),
        row_block,
    ]
    small_flat = token_parts[0].reshape(-1)
    small_round = lax.reduce_precision(small_flat, exponent_bits=8, mantissa_bits=7)
    small_high = small_round.astype(jnp.bfloat16)
    small_low = (small_flat - small_round).astype(jnp.bfloat16)
    rows_low = row_block.reshape(-1).astype(jnp.bfloat16)
    riding_size = 2 * small_flat.size + rows_low.size
    small_rows = -(-riding_size // model_width)
    small_rows += (-(share_rows + small_rows)) % 8
    small_pad = small_rows * model_width - riding_size
    riding = jnp.concatenate(
        [small_high, small_low, rows_low, jnp.zeros((small_pad,), jnp.bfloat16)]
    ).reshape(small_rows, model_width)
    att_gathered = lax.all_gather(
        jnp.concatenate([grad_att, riding], axis=0), "tensor", axis=0, tiled=False
    )
    grad_att_all = att_gathered[:, :share_rows].reshape(group_rows, model_width)
    small_back = att_gathered[:, share_rows:].reshape(tensor_count, -1).astype(jnp.float32)
    token_size = small_flat.size
    token_sum = jnp.sum(
        small_back[:, :token_size] + small_back[:, token_size : 2 * token_size], axis=0
    ).reshape(token_parts[0].shape)
    rows_group = jnp.sum(
        small_back[:, 2 * token_size : 2 * token_size + rows_low.size], axis=0
    ).reshape(row_block.shape)
    out_weight_grad_t = jnp.einsum(
        "td,te->de", grad_att_all, context, preferred_element_type=jnp.float32
    )
    grad_context = jnp.einsum(
        "td,ed->te", grad_att_all, out_weight, preferred_element_type=jnp.float32
    ).astype(jnp.bfloat16)
    grad_queries, grad_keys, grad_values = attend_backward(
        queries, key_rows, value_rows, segments, log_totals, grad_context
    )
    stacked = jnp.stack([grad_queries, grad_keys, grad_values])
    qkv_weight_grad = jnp.einsum(
        "td,tq->dq",
        gathered,
        jnp.concatenate([grad_queries, grad_keys, grad_values], axis=1),
        preferred_element_type=jnp.float32,
    )
    qv_bias_grad = jnp.stack(
        [
            jnp.sum(grad_queries.astype(jnp.float32), axis=0),
            jnp.sum(grad_values.astype(jnp.float32), axis=0),
        ]
    )
    input_grad = (
        lax.psum_scatter(
            jnp.einsum(
                "kte,kde->td", stacked, qkv_weight, preferred_element_type=jnp.float32
            ).astype(jnp.bfloat16),
            "tensor",
            scatter_dimension=0,
            tiled=True,
        ).astype(jnp.float32)
        + grad_res
    ).astype(jnp.bfloat16)

    def stacked_sum(parts, dtype):
        padded = [
            jnp.pad(part.astype(dtype), ((0, 0), (0, (-part.shape[1]) % 16), (0, 0)))
            for part in parts
        ]
        flat = jnp.concatenate(padded, axis=1)
        lanes = flat.shape[2]
        summed = lax.psum_scatter(
            flat.reshape(-1, lanes), "dp", scatter_dimension=0, tiled=True
        )
        pieces = []
        begin = 0
        for part, held in zip(parts, padded):
            pieces.append(summed[begin : begin + part.shape[1]])
            begin += held.shape[1]
        return pieces

    def in_blocks(grad):
        return grad.reshape(dp_count, grad.shape[0] // dp_count, grad.shape[1])

    def copied(flat, lanes):
        rows = -(-flat.size // lanes)
        flat = jnp.pad(flat, (0, rows * lanes - flat.size)).reshape(1, rows, lanes)
        return jnp.broadcast_to(flat, (dp_count, rows, lanes))

    early_parts = [in_blocks(up_weight_grad), in_blocks(down_weight_grad_t)]
    early_sums = stacked_sum(early_parts, jnp.bfloat16)
    up_sum = early_sums[0].astype(jnp.float32)
    down_sum = early_sums[1].astype(jnp.float32).T
    late_shared = [qv_bias_grad, token_sum, up_bias_grad]
    qkv_lanes = qkv_weight_grad.shape[1]

    def aligned(part):
        return jnp.pad(part, ((0, 0), (0, (-part.shape[1]) % 16), (0, 0)))

    shared_flat = joined(late_shared)
    shared_round = lax.reduce_precision(shared_flat, exponent_bits=8, mantissa_bits=7)
    shared_pair = jnp.concatenate([shared_round, shared_flat - shared_round]).astype(jnp.bfloat16)
    qkv_lanes = qkv_weight_grad.shape[1]
    out_flat = in_blocks(out_weight_grad_t).astype(jnp.bfloat16).reshape(dp_count, -1)
    out_rows = -(-out_flat.shape[1] // qkv_lanes)
    out_blocks = jnp.pad(out_flat, ((0, 0), (0, out_rows * qkv_lanes - out_flat.shape[1])))
    late_parts = [
        aligned(in_blocks(qkv_weight_grad).astype(jnp.bfloat16)),
        aligned(out_blocks.reshape(dp_count, out_rows, qkv_lanes)),
        aligned(copied(shared_pair, qkv_lanes)),
        aligned(copied(rows_group.reshape(-1).astype(jnp.bfloat16), qkv_lanes)),
    ]
    late_received = lax.all_to_all(
        jnp.concatenate(late_parts, axis=1), "dp", 0, 0, tiled=False
    )
    qkv_rows = in_blocks(qkv_weight_grad).shape[1]
    out_begin = late_parts[0].shape[1]
    shared_begin = out_begin + late_parts[1].shape[1]
    rows_begin = shared_begin + late_parts[2].shape[1]
    qkv_total = jnp.sum(late_received[:, :qkv_rows].astype(jnp.float32), axis=0)
    out_total = jnp.sum(
        late_received[:, out_begin:shared_begin].reshape(dp_count, -1).astype(jnp.float32),
        axis=0,
    )
    out_sum = out_total[: out_flat.shape[1]].reshape(-1, out_weight_grad_t.shape[1]).T
    qkv_sum = jnp.transpose(qkv_total.reshape(qkv_rows, 3, qkv_lanes // 3), (1, 0, 2))
    shared_back = late_received[:, shared_begin:rows_begin].reshape(dp_count, -1)
    shared_back = shared_back.astype(jnp.float32)
    shared_total = jnp.sum(
        shared_back[:, : shared_flat.size]
        + shared_back[:, shared_flat.size : 2 * shared_flat.size],
        axis=0,
    )
    qv_bias_total, token_grads, up_bias_total = parted(shared_total, late_shared)
    rows_each = late_received[:, rows_begin:].reshape(dp_count, -1)[:, : rows_group.size]
    rows_all = rows_each.reshape(dp_count * seq_count, 4, model_width).astype(jnp.bfloat16)
    leading_all = rows_all[:, 0]
    grad_pre_all = rows_all[:, 1]
    pooled_all = rows_all[:, 2]
    grad_logits_all = rows_all[:, 3, :classes]
    pool_weight_grad = jnp.einsum(
        "rd,re->de", leading_all, grad_pre_all, preferred_element_type=jnp.float32
    )
    pool_bias_grad = jnp.sum(grad_pre_all.astype(jnp.float32), axis=0)
    class_weight_grad = jnp.einsum(
        "rd,rc->dc", pooled_all, grad_logits_all, preferred_element_type=jnp.float32
    )
    class_bias_grad = jnp.sum(grad_logits_all.astype(jnp.float32), axis=0)

    return (
        final_norm.astype(jnp.bfloat16),
        input_grad,
        qkv_sum,
        qv_bias_total,
        out_sum,
        token_grads[0],
        token_grads[1],
        token_grads[2],
        up_sum,
        up_bias_total,
        down_sum,
        token_grads[3],
        token_grads[4],
        token_grads[5],
        pool_weight_grad,
        pool_bias_grad,
        class_weight_grad,
        class_bias_grad,
    )


def solution(mesh):
    placed = (
        P(("dp", "tensor"), None),
        P("dp", None),
        P("dp"),
        P(None, None, "tensor"),
        P(None, "tensor"),
        P("tensor", None),
        P(),
        P(),
        P(),
        P(None, "tensor"),
        P("tensor"),
        P("tensor", None),
        P(),
        P(),
        P(),
        P(),
        P(),
        P(),
        P(),
        P(("dp", "tensor"), None),
    )
    return jax.shard_map(
        body,
        mesh=mesh,
        in_specs=placed,
        out_specs=(
            P(("dp", "tensor"), None),
            P(("dp", "tensor"), None),
            P(None, "dp", "tensor"),
            P(None, "tensor"),
            P("tensor", "dp"),
            P(),
            P(),
            P(),
            P("dp", "tensor"),
            P("tensor"),
            P("tensor", "dp"),
            P(),
            P(),
            P(),
            P(),
            P(),
            P(),
            P(),
        ),
        check_vma=False,
    )
```

```python
from functools import partial

import jax
import jax.numpy as jnp
from jax import lax
from jax.sharding import PartitionSpec as P


HEAD = 64


epsilon = 1e-12
masked_value = -1e30


def norm_forward(values, norm_gain, norm_shift):
    centre = values - jnp.mean(values, axis=-1, keepdims=True)
    inverse = lax.rsqrt(jnp.mean(centre * centre, axis=-1, keepdims=True) + epsilon)
    normed = centre * inverse
    return (normed * norm_gain + norm_shift, normed, inverse)


def norm_backward(grad_out, normed, inverse, norm_gain):
    scaled = grad_out * norm_gain
    grad_in = inverse * (
        scaled
        - jnp.mean(scaled, axis=-1, keepdims=True)
        - normed * jnp.mean(scaled * normed, axis=-1, keepdims=True)
    )
    return (grad_in, jnp.sum(grad_out * normed, axis=0), jnp.sum(grad_out, axis=0))


def split_heads(rows, seq_count):
    return rows.reshape(seq_count, rows.shape[0] // seq_count, rows.shape[1] // HEAD, HEAD)


def masked_scores(query_heads, key_heads, segments):
    raw_scores = jnp.einsum(
        "rqhe,rkhe->rhqk", query_heads, key_heads, preferred_element_type=jnp.float32
    ) * HEAD ** (-0.5)
    allowed = segments[:, None, :, None] == segments[:, None, None, :]
    return (jnp.where(allowed, raw_scores, masked_value), allowed)


def attend_forward(queries, key_rows, value_rows, segments):
    seq_count = segments.shape[0]
    scores, _ = masked_scores(
        split_heads(queries, seq_count), split_heads(key_rows, seq_count), segments
    )
    largest = jnp.max(scores, axis=-1, keepdims=True)
    exponent = jnp.exp(scores - largest)
    row_total = jnp.sum(exponent, axis=-1, keepdims=True)
    soft_low = (exponent / row_total).astype(jnp.bfloat16)
    context = jnp.einsum(
        "rhqk,rkhe->rqhe",
        soft_low,
        split_heads(value_rows, seq_count),
        preferred_element_type=jnp.float32,
    )
    context = context.reshape(queries.shape).astype(jnp.bfloat16)
    return (context, largest + jnp.log(row_total))


def attend_backward(queries, key_rows, value_rows, segments, log_total, grad_context):
    seq_count = segments.shape[0]
    query_heads = split_heads(queries, seq_count)
    key_heads = split_heads(key_rows, seq_count)
    value_heads = split_heads(value_rows, seq_count)
    grad_heads = split_heads(grad_context, seq_count)
    scores, allowed = masked_scores(query_heads, key_heads, segments)
    soft_probs = jnp.exp(scores - log_total)
    grad_values = jnp.einsum(
        "rhqk,rqhe->rkhe",
        soft_probs.astype(jnp.bfloat16),
        grad_heads,
        preferred_element_type=jnp.float32,
    )
    grad_soft = jnp.einsum(
        "rqhe,rkhe->rhqk", grad_heads, value_heads, preferred_element_type=jnp.float32
    )
    grad_scores = soft_probs * (grad_soft - jnp.sum(soft_probs * grad_soft, axis=-1, keepdims=True))
    score_scale = HEAD ** (-0.5)
    grad_low = lax.optimization_barrier(
        jnp.where(allowed, grad_scores, 0.0).astype(jnp.bfloat16) * jnp.bfloat16(score_scale)
    )
    grad_queries = jnp.einsum(
        "rhqk,rkhe->rqhe", grad_low, key_heads, preferred_element_type=jnp.float32
    )
    grad_keys = jnp.einsum(
        "rhqk,rqhe->rkhe", grad_low, query_heads, preferred_element_type=jnp.float32
    )
    full_shape = queries.shape
    return (
        grad_queries.reshape(full_shape).astype(jnp.bfloat16),
        grad_keys.reshape(full_shape).astype(jnp.bfloat16),
        grad_values.reshape(full_shape).astype(jnp.bfloat16),
    )


def body(
    inputs,
    segments,
    labels,
    qkv_weight,
    qv_bias,
    out_weight,
    out_bias,
    norm1_gain,
    norm1_bias,
    up_weight,
    up_bias,
    down_weight,
    down_bias,
    norm2_gain,
    norm2_bias,
    pool_weight,
    pool_bias,
    class_weight,
    class_bias,
    cotangent,
):
    share_rows = inputs.shape[0]
    seq_count, seq_length = segments.shape
    tensor_index = lax.axis_index("tensor")
    tensor_count = lax.axis_size("tensor")
    dp_count = lax.axis_size("dp")
    offset = tensor_index * share_rows

    gathered = lax.all_gather(inputs, "tensor", axis=0, tiled=True)
    group_rows = gathered.shape[0]

    def project(which):
        return jnp.dot(gathered, qkv_weight[which], preferred_element_type=jnp.float32)

    queries = (project(0) + qv_bias[0]).astype(jnp.bfloat16)
    key_rows = project(1).astype(jnp.bfloat16)
    value_rows = (project(2) + qv_bias[1]).astype(jnp.bfloat16)
    local_width = queries.shape[1]

    out_weight_all = lax.all_gather(out_weight, "tensor", axis=0, tiled=False)
    context, log_totals = attend_forward(queries, key_rows, value_rows, segments)
    context_own = lax.all_to_all(
        context.reshape(tensor_count, share_rows, local_width), "tensor", 0, 0, tiled=False
    )
    attended = (
        jnp.einsum(
            "itc,icd->td", context_own, out_weight_all, preferred_element_type=jnp.float32
        )
        + out_bias
    )
    first_norm, normed_one, inverse_one = norm_forward(
        inputs.astype(jnp.float32) + attended, norm1_gain, norm1_bias
    )
    first_low = first_norm.astype(jnp.bfloat16)
    first_all = lax.all_gather(first_low, "tensor", axis=0, tiled=True)
    up_pre = jnp.dot(first_all, up_weight, preferred_element_type=jnp.float32) + up_bias
    gelu_exact = partial(jax.nn.gelu, approximate=False)
    active = gelu_exact(up_pre).astype(jnp.bfloat16)
    ffn_out = (
        lax.psum_scatter(
            jnp.dot(active, down_weight, preferred_element_type=jnp.float32).astype(jnp.bfloat16),
            "tensor",
            scatter_dimension=0,
            tiled=True,
        )
        .astype(jnp.float32)
        + down_bias
    )
    final_norm, normed_two, inverse_two = norm_forward(
        first_norm + ffn_out, norm2_gain, norm2_bias
    )

    positions = offset + jnp.arange(share_rows, dtype=jnp.int32)
    row_starts = jnp.arange(seq_count, dtype=jnp.int32) * seq_length
    selector = (row_starts[:, None] == positions[None, :]).astype(jnp.float32)
    owned = jnp.sum(selector, axis=1, keepdims=True)
    leading = jnp.dot(selector, final_norm, precision=lax.Precision.HIGHEST).astype(jnp.bfloat16)
    pooled = jnp.tanh(jnp.dot(leading, pool_weight, preferred_element_type=jnp.float32) + pool_bias)
    pooled_low = pooled.astype(jnp.bfloat16)
    logits = jnp.dot(pooled_low, class_weight, preferred_element_type=jnp.float32) + class_bias
    chosen = (
        labels[:, None] == jnp.arange(class_weight.shape[1], dtype=jnp.int32)[None, :]
    ).astype(jnp.float32)
    grad_logits = jnp.where(
        owned > 0, jax.nn.softmax(logits, axis=-1) - chosen, 0.0
    ).astype(jnp.bfloat16)
    grad_pre = (
        jnp.einsum("rc,dc->rd", grad_logits, class_weight, preferred_element_type=jnp.float32)
        * (1.0 - pooled * pooled)
    ).astype(jnp.bfloat16)
    grad_leading = jnp.einsum(
        "re,de->rd", grad_pre, pool_weight, preferred_element_type=jnp.float32
    )
    grad_final = cotangent.astype(jnp.float32) + jnp.einsum(
        "rt,rd->td", selector, grad_leading, precision=lax.Precision.HIGHEST
    )
    grad_second, norm2_gain_grad, norm2_bias_grad = norm_backward(
        grad_final, normed_two, inverse_two, norm2_gain
    )
    grad_fed = grad_second.astype(jnp.bfloat16)
    down_bias_grad = jnp.sum(grad_fed.astype(jnp.float32), axis=0)
    grad_fed_all = lax.all_gather(grad_fed, "tensor", axis=0, tiled=True)
    down_weight_grad_t = jnp.einsum(
        "td,tf->df", grad_fed_all, active, preferred_element_type=jnp.float32
    )
    grad_active = jnp.einsum(
        "td,fd->tf", grad_fed_all, down_weight, preferred_element_type=jnp.float32
    )
    grad_up = jax.vjp(gelu_exact, up_pre)[1](grad_active)[0].astype(jnp.bfloat16)
    up_bias_grad = jnp.sum(grad_up.astype(jnp.float32), axis=0)
    up_weight_grad = jnp.einsum("td,tf->df", first_all, grad_up, preferred_element_type=jnp.float32)
    grad_first = (
        lax.psum_scatter(
            jnp.einsum("tf,df->td", grad_up, up_weight, preferred_element_type=jnp.float32).astype(jnp.bfloat16),
            "tensor",
            scatter_dimension=0,
            tiled=True,
        )
        .astype(jnp.float32)
        + grad_second
    )
    grad_res, norm1_gain_grad, norm1_bias_grad = norm_backward(
        grad_first, normed_one, inverse_one, norm1_gain
    )
    grad_att = grad_res.astype(jnp.bfloat16)
    out_bias_grad = jnp.sum(grad_att.astype(jnp.float32), axis=0)

    def joined(parts):
        return jnp.concatenate([part.reshape(-1) for part in parts])

    def parted(flat, parts):
        pieces = []
        begin = 0
        for part in parts:
            pieces.append(flat[begin : begin + part.size].reshape(part.shape))
            begin += part.size
        return pieces

    model_width = grad_att.shape[1]
    classes = class_weight.shape[1]
    row_block = jnp.stack(
        [
            leading.astype(jnp.float32) * owned,
            grad_pre.astype(jnp.float32),
            pooled_low.astype(jnp.float32) * owned,
            jnp.pad(grad_logits.astype(jnp.float32), ((0, 0), (0, model_width - classes))),
        ],
        axis=1,
    )
    token_parts = [
        jnp.stack(
            [
                out_bias_grad,
                norm1_gain_grad,
                norm1_bias_grad,
                down_bias_grad,
                norm2_gain_grad,
                norm2_bias_grad,
            ]
        ),
        row_block,
    ]
    small_flat = token_parts[0].reshape(-1)
    small_round = lax.reduce_precision(small_flat, exponent_bits=8, mantissa_bits=7)
    small_high = small_round.astype(jnp.bfloat16)
    small_low = (small_flat - small_round).astype(jnp.bfloat16)
    rows_low = row_block.reshape(-1).astype(jnp.bfloat16)
    riding_size = 2 * small_flat.size + rows_low.size
    small_rows = -(-riding_size // model_width)
    small_rows += (-(share_rows + small_rows)) % 8
    small_pad = small_rows * model_width - riding_size
    riding = jnp.concatenate(
        [small_high, small_low, rows_low, jnp.zeros((small_pad,), jnp.bfloat16)]
    ).reshape(small_rows, model_width)
    att_gathered = lax.all_gather(
        jnp.concatenate([grad_att, riding], axis=0), "tensor", axis=0, tiled=False
    )
    grad_att_all = att_gathered[:, :share_rows].reshape(group_rows, model_width)
    small_back = att_gathered[:, share_rows:].reshape(tensor_count, -1).astype(jnp.float32)
    token_size = small_flat.size
    token_sum = jnp.sum(
        small_back[:, :token_size] + small_back[:, token_size : 2 * token_size], axis=0
    ).reshape(token_parts[0].shape)
    rows_group = jnp.sum(
        small_back[:, 2 * token_size : 2 * token_size + rows_low.size], axis=0
    ).reshape(row_block.shape)
    out_weight_grad_t = jnp.einsum(
        "td,te->de", grad_att_all, context, preferred_element_type=jnp.float32
    )
    grad_context = jnp.einsum(
        "td,ed->te", grad_att_all, out_weight, preferred_element_type=jnp.float32
    ).astype(jnp.bfloat16)
    grad_queries, grad_keys, grad_values = attend_backward(
        queries, key_rows, value_rows, segments, log_totals, grad_context
    )
    stacked = jnp.stack([grad_queries, grad_keys, grad_values])
    qkv_weight_grad = jnp.einsum(
        "td,tq->dq",
        gathered,
        jnp.concatenate([grad_queries, grad_keys, grad_values], axis=1),
        preferred_element_type=jnp.float32,
    )
    qv_bias_grad = jnp.stack(
        [
            jnp.sum(grad_queries.astype(jnp.float32), axis=0),
            jnp.sum(grad_values.astype(jnp.float32), axis=0),
        ]
    )
    input_grad = (
        lax.psum_scatter(
            jnp.einsum(
                "kte,kde->td", stacked, qkv_weight, preferred_element_type=jnp.float32
            ).astype(jnp.bfloat16),
            "tensor",
            scatter_dimension=0,
            tiled=True,
        ).astype(jnp.float32)
        + grad_res
    ).astype(jnp.bfloat16)

    def stacked_sum(parts, dtype):
        padded = [
            jnp.pad(part.astype(dtype), ((0, 0), (0, (-part.shape[1]) % 16), (0, 0)))
            for part in parts
        ]
        flat = jnp.concatenate(padded, axis=1)
        lanes = flat.shape[2]
        summed = lax.psum_scatter(
            flat.reshape(-1, lanes), "dp", scatter_dimension=0, tiled=True
        )
        pieces = []
        begin = 0
        for part, held in zip(parts, padded):
            pieces.append(summed[begin : begin + part.shape[1]])
            begin += held.shape[1]
        return pieces

    def in_blocks(grad):
        return grad.reshape(dp_count, grad.shape[0] // dp_count, grad.shape[1])

    def copied(flat, lanes):
        rows = -(-flat.size // lanes)
        flat = jnp.pad(flat, (0, rows * lanes - flat.size)).reshape(1, rows, lanes)
        return jnp.broadcast_to(flat, (dp_count, rows, lanes))

    early_parts = [in_blocks(up_weight_grad), in_blocks(down_weight_grad_t)]
    early_sums = stacked_sum(early_parts, jnp.bfloat16)
    up_sum = early_sums[0].astype(jnp.float32)
    down_sum = early_sums[1].astype(jnp.float32).T
    late_shared = [qv_bias_grad, token_sum, up_bias_grad]
    qkv_lanes = qkv_weight_grad.shape[1]

    def aligned(part):
        return jnp.pad(part, ((0, 0), (0, (-part.shape[1]) % 16), (0, 0)))

    shared_flat = joined(late_shared)
    shared_round = lax.reduce_precision(shared_flat, exponent_bits=8, mantissa_bits=7)
    shared_pair = jnp.concatenate([shared_round, shared_flat - shared_round]).astype(jnp.bfloat16)
    qkv_lanes = qkv_weight_grad.shape[1]
    out_flat = in_blocks(out_weight_grad_t).astype(jnp.bfloat16).reshape(dp_count, -1)
    out_rows = -(-out_flat.shape[1] // qkv_lanes)
    out_blocks = jnp.pad(out_flat, ((0, 0), (0, out_rows * qkv_lanes - out_flat.shape[1])))
    late_parts = [
        aligned(in_blocks(qkv_weight_grad).astype(jnp.bfloat16)),
        aligned(out_blocks.reshape(dp_count, out_rows, qkv_lanes)),
        aligned(copied(shared_pair, qkv_lanes)),
        aligned(copied(rows_group.reshape(-1).astype(jnp.bfloat16), qkv_lanes)),
    ]
    late_received = lax.all_to_all(
        jnp.concatenate(late_parts, axis=1), "dp", 0, 0, tiled=False
    )
    qkv_rows = in_blocks(qkv_weight_grad).shape[1]
    out_begin = late_parts[0].shape[1]
    shared_begin = out_begin + late_parts[1].shape[1]
    rows_begin = shared_begin + late_parts[2].shape[1]
    qkv_total = jnp.sum(late_received[:, :qkv_rows].astype(jnp.float32), axis=0)
    out_total = jnp.sum(
        late_received[:, out_begin:shared_begin].reshape(dp_count, -1).astype(jnp.float32),
        axis=0,
    )
    out_sum = out_total[: out_flat.shape[1]].reshape(-1, out_weight_grad_t.shape[1]).T
    qkv_sum = jnp.transpose(qkv_total.reshape(qkv_rows, 3, qkv_lanes // 3), (1, 0, 2))
    shared_back = late_received[:, shared_begin:rows_begin].reshape(dp_count, -1)
    shared_back = shared_back.astype(jnp.float32)
    shared_total = jnp.sum(
        shared_back[:, : shared_flat.size]
        + shared_back[:, shared_flat.size : 2 * shared_flat.size],
        axis=0,
    )
    qv_bias_total, token_grads, up_bias_total = parted(shared_total, late_shared)
    rows_each = late_received[:, rows_begin:].reshape(dp_count, -1)[:, : rows_group.size]
    rows_all = rows_each.reshape(dp_count * seq_count, 4, model_width).astype(jnp.bfloat16)
    leading_all = rows_all[:, 0]
    grad_pre_all = rows_all[:, 1]
    pooled_all = rows_all[:, 2]
    grad_logits_all = rows_all[:, 3, :classes]
    pool_weight_grad = jnp.einsum(
        "rd,re->de", leading_all, grad_pre_all, preferred_element_type=jnp.float32
    )
    pool_bias_grad = jnp.sum(grad_pre_all.astype(jnp.float32), axis=0)
    class_weight_grad = jnp.einsum(
        "rd,rc->dc", pooled_all, grad_logits_all, preferred_element_type=jnp.float32
    )
    class_bias_grad = jnp.sum(grad_logits_all.astype(jnp.float32), axis=0)

    return (
        final_norm.astype(jnp.bfloat16),
        input_grad,
        qkv_sum,
        qv_bias_total,
        out_sum,
        token_grads[0],
        token_grads[1],
        token_grads[2],
        up_sum,
        up_bias_total,
        down_sum,
        token_grads[3],
        token_grads[4],
        token_grads[5],
        pool_weight_grad,
        pool_bias_grad,
        class_weight_grad,
        class_bias_grad,
    )


def solution(mesh):
    placed = (
        P(("dp", "tensor"), None),
        P("dp", None),
        P("dp"),
        P(None, None, "tensor"),
        P(None, "tensor"),
        P("tensor", None),
        P(),
        P(),
        P(),
        P(None, "tensor"),
        P("tensor"),
        P("tensor", None),
        P(),
        P(),
        P(),
        P(),
        P(),
        P(),
        P(),
        P(("dp", "tensor"), None),
    )
    return jax.shard_map(
        body,
        mesh=mesh,
        in_specs=placed,
        out_specs=(
            P(("dp", "tensor"), None),
            P(("dp", "tensor"), None),
            P(None, "dp", "tensor"),
            P(None, "tensor"),
            P("tensor", "dp"),
            P(),
            P(),
            P(),
            P("dp", "tensor"),
            P("tensor"),
            P("tensor", "dp"),
            P(),
            P(),
            P(),
            P(),
            P(),
            P(),
            P(),
        ),
        check_vma=False,
    )
```
